256 devices in a mesh: shot: 2 (over z), gy: 128 (over x, y, core).
Axes of the slice: x: 8, y: 8, z: 2, core: 2. Of those that a mesh axis runs over, the one named last changes fastest.
The devices are a block of a 8x8x16 slice.
Arguments:
- source_now: float32 [32, 1024, 256], P('shot', 'gy'), parts along dimension 0, may hold values from -4 to 4
- source_before: float32 [32, 1024, 256], P('shot', 'gy'), parts along dimension 0, may hold values from -4 to 4
- receiver_now: float32 [32, 1024, 256], P('shot', 'gy'), parts along dimension 0, may hold values from -4 to 4
- receiver_before: float32 [32, 1024, 256], P('shot', 'gy'), parts along dimension 0, may hold values from -4 to 4
- speed_term: float32 [16, 1024, 256], P(None, 'gy'), may hold values from 0.03 to 0.12
- aniso_field: float32 [16, 1024, 256], P(None, 'gy'), may hold values from 0 to 0.3
- tilt_field: float32 [16, 1024, 256], P(None, 'gy'), may hold values from -0.5 to 0.5
- angle_bins: int32 [16, 1024, 256], P(None, 'gy'), may hold values from 0 to 7
- weight_table: bfloat16 [24, 8, 4], replicated, may hold values from -1.25 to 1.25
- offset_lags: int32 [24], replicated, may hold values from -16 to 16, as said below
- source_cells: int32 [16], P('shot'), parts along dimension 0, may hold values from 0 to 262143
- source_wavelet: float32 [4, 8], P('shot'), parts along dimension 0, may hold values from -24 to 24
- receiver_cells: int32 [4096], P('shot'), parts along dimension 0, may hold values from 0 to 262143
- receiver_traces: float32 [4, 2048], P('shot'), parts along dimension 0, may hold values from -18 to 18
Outputs:
- angle_images: bfloat16 [8, 16, 1024, 256], P('shot', None, 'gy'), parts along dimension 0
The draws below stay inside these ranges and needn't reach their ends.
There are 2 independent parts, one for each index of `shot`. The reference program is written for one: setup_inputs(seed, part) draws one part's arguments, and reference() takes and returns one part's arrays. A program takes and returns all parts, laid end to end along the dimension named above; an argument that names none is the same for every part. Nothing has to cross between parts.
Inputs may be any that keep to these rules, and one draw needn't show every extreme that they name: `offset_lags`: 24 distinct lags; -16 and 16 are among them.
All inputs are finite; a program needn't handle non-finite values.
Results may differ from the reference program's by a relative error of at most 0.0051.
Values may be sent and summed in bfloat16 or wider, within the bound.
A program may use at most 64 MiB of HBM per device.

```python
import math
import jax
import jax.numpy as jnp
from jax import lax

NX = 256
CY = 8
Z = 16
ITERS = 2
NOFF = 24
NANG = 4
NBIN = 8
NSRC = 8
NREC = 2048
NY = 1024
LMAX = 16


def draw_offset_lags(key, part):
    reach = 2 * CY
    inner = jax.random.permutation(jax.random.fold_in(key, 11), 2 * reach - 1) - (reach - 1)
    chosen = jnp.concatenate([jnp.array([-reach, reach], jnp.int32), inner[:NOFF - 2].astype(jnp.int32)])
    return jax.random.permutation(jax.random.fold_in(key, 12), chosen)


def with_ends(drawn, stream_key, least, high):
    longest = drawn.shape.index(max(drawn.shape))
    spots = []
    for shift in (0, 1):
        where = [jax.random.randint(jax.random.fold_in(stream_key, axis), (), 0, length) for axis, length in enumerate(drawn.shape)]
        where[longest] = (where[longest] + shift) % drawn.shape[longest]
        spots.append(tuple(where))
    return drawn.at[spots[0]].set(least).at[spots[1]].set(high)


def shard_levels(key, extent, split, smallest, top_value):
    gain = 1.0
    for position, shards_of in split:
        steps = jax.random.uniform(jax.random.fold_in(jax.random.fold_in(key, 6), position), (shards_of,), jnp.float32, smallest / len(split), top_value / len(split))
        gain = gain * jnp.repeat(jnp.exp(steps), extent[position] // shards_of).reshape((-1,) + (1,) * (len(extent) - 1 - position))
    return gain


def noise(rng, extent, deviation, most, shards=(), held_as=jnp.bfloat16):
    factor_of = shard_levels(rng, extent, shards, -0.22, 0.18) if shards else 1.0
    values = jax.random.normal(rng, extent, jnp.float32) * deviation * factor_of
    return jnp.minimum(jnp.maximum(values, -most), most).astype(held_as)


def setup_inputs(seed: int = 0, part: int = 0) -> dict:
    key_of = jax.random.split(jax.random.key(seed), 15)
    own_keys = jax.random.split(jax.random.fold_in(key_of[14], part), 15)
    return {
        "source_now": noise(own_keys[0], (Z, NY, NX), 0.5, 4.0, ((1, 128),), jnp.float32),
        "source_before": noise(own_keys[1], (Z, NY, NX), 0.5, 4.0, ((1, 128),), jnp.float32),
        "receiver_now": noise(own_keys[2], (Z, NY, NX), 0.5, 4.0, ((1, 128),), jnp.float32),
        "receiver_before": noise(own_keys[3], (Z, NY, NX), 0.5, 4.0, ((1, 128),), jnp.float32),
        "speed_term": jnp.clip(jnp.exp(math.log(0.12) - 1.3862944 * jax.random.uniform(key_of[4], (Z, NY, NX), jnp.float32) ** shard_levels(key_of[4], (Z, NY, NX), ((1, 128),), -0.2, 0.2)), 0.03, 0.12),
        "aniso_field": jnp.clip(0.3 * jax.random.uniform(key_of[5], (Z, NY, NX), jnp.float32) ** shard_levels(key_of[5], (Z, NY, NX), ((1, 128),), -0.2, 0.2), 0.0, 0.3),
        "tilt_field": jnp.clip(jax.random.uniform(key_of[6], (Z, NY, NX), jnp.float32, -0.5, 0.5) * shard_levels(key_of[6], (Z, NY, NX), ((1, 128),), -0.4, 0.0), -0.5, 0.5),
        "angle_bins": with_ends(jax.random.randint(key_of[7], (Z, NY, NX), 0, NBIN), jax.random.fold_in(key_of[7], 1), 0, NBIN - 1).astype(jnp.int32),
        "weight_table": noise(key_of[8], (NOFF, NBIN, NANG), NOFF ** -0.5, 1.25),
        "offset_lags": draw_offset_lags(jax.random.fold_in(key_of[14], 71), part),
        "source_cells": with_ends(jax.random.randint(own_keys[10], (NSRC,), 0, NX * NY), jax.random.fold_in(own_keys[10], 1), 0, (NX * NY) - 1).astype(jnp.int32),
        "source_wavelet": noise(own_keys[11], (ITERS, NSRC), 4.0, 24.0, (), jnp.float32),
        "receiver_cells": with_ends(jax.random.randint(own_keys[12], (NREC,), 0, NX * NY), jax.random.fold_in(own_keys[12], 1), 0, (NX * NY) - 1).astype(jnp.int32),
        "receiver_traces": noise(own_keys[13], (ITERS, NREC), 3.0, 18.0, (), jnp.float32),
    }


SECOND_COEF = (-205.0 / 72.0, 8.0 / 5.0, -1.0 / 5.0, 8.0 / 315.0, -1.0 / 560.0)
FIRST_COEF = (4.0 / 5.0, -1.0 / 5.0, 4.0 / 105.0, -1.0 / 280.0)


def derivs(padded, dimension, length):
    middle = lax.slice_in_dim(padded, 4, 4 + length, axis=dimension)
    second = SECOND_COEF[0] * middle
    first_deriv = jnp.zeros_like(middle)
    for distance in range(1, 5):
        above_cells = lax.slice_in_dim(padded, 4 + distance, 4 + distance + length, axis=dimension)
        below_cells = lax.slice_in_dim(padded, 4 - distance, 4 - distance + length, axis=dimension)
        second = second + SECOND_COEF[distance] * (above_cells + below_cells)
        first_deriv = first_deriv + FIRST_COEF[distance - 1] * (above_cells - below_cells)
    return second, first_deriv


def pad_axis(array_in, dimension):
    widths = [(0, 0)] * array_in.ndim
    widths[dimension] = (4, 4)
    return jnp.pad(array_in, widths)


def operate(extended, aniso_field, tilt_field):
    row_count = extended.shape[2] - 8
    core_part = extended[:, :, 4:4 + row_count, :]
    second_y, first_y = derivs(extended, 2, row_count)
    second_x, first_x = derivs(pad_axis(core_part, 3), 3, core_part.shape[3])
    second_z, unused = derivs(pad_axis(core_part, 1), 1, core_part.shape[1])
    unused_two, mixed_term = derivs(pad_axis(first_x + first_y, 1), 1, core_part.shape[1])
    return (1.0 + 2.0 * aniso_field) * (second_x + second_y) + second_z + tilt_field * mixed_term


def inject(fields, step_index, positions, amounts, member, grid_width, first_row):
    row_local = positions // grid_width - first_row
    inside = (row_local >= 0) & (row_local < fields.shape[2])
    clipped = jnp.clip(row_local, 0, fields.shape[2] - 1)
    added = jnp.where(inside, amounts[step_index], jnp.zeros_like(amounts[step_index]))
    return fields.at[member, 0, clipped, positions % grid_width].add(added)


def lag_products(source_win, receiver_win, offset_lags, center, row_count):
    def single(lag_value):
        source_part = lax.dynamic_slice_in_dim(source_win, center - lag_value, row_count, 1).astype(jnp.float32)
        receiver_part = lax.dynamic_slice_in_dim(receiver_win, center + lag_value, row_count, 1).astype(jnp.float32)
        return (source_part * receiver_part).reshape(-1)
    return jax.vmap(single)(offset_lags)


def combine(products, bin_ids, weights):
    flat_weights = weights.astype(jnp.float32).reshape(weights.shape[0], -1)
    mixed_term = jnp.dot(flat_weights.T, products, precision=lax.Precision.HIGHEST, preferred_element_type=jnp.float32)
    mixed_term = mixed_term.reshape(weights.shape[1], weights.shape[2], -1)
    chosen = (bin_ids[None, :] == jnp.arange(weights.shape[1], dtype=jnp.int32)[:, None]).astype(jnp.float32)
    return jnp.sum(chosen[:, None, :] * mixed_term, axis=0)


def reference(source_now, source_before, receiver_now, receiver_before, speed_term, aniso_field, tilt_field, angle_bins, weight_table, offset_lags, source_cells, source_wavelet, receiver_cells, receiver_traces):
    now_fields = jnp.stack([source_now, receiver_now])
    prev_fields = jnp.stack([source_before, receiver_before])
    image_sum = jnp.zeros((NANG, Z, NY, NX), jnp.float32)
    for step_index in range(ITERS):
        extended = jnp.pad(now_fields, ((0, 0), (0, 0), (4, 4), (0, 0)), mode="wrap")
        next_fields = 2.0 * now_fields - prev_fields + speed_term * operate(extended, aniso_field, tilt_field)
        next_fields = inject(next_fields, step_index, source_cells, source_wavelet, 0, NX, 0)
        next_fields = inject(next_fields, step_index, receiver_cells, receiver_traces, 1, NX, 0)
        prev_fields, now_fields = now_fields, next_fields
        rounded = now_fields.astype(jnp.bfloat16)
        padded = jnp.pad(rounded, ((0, 0), (0, 0), (LMAX, LMAX), (0, 0)), mode="wrap")
        moved = jnp.moveaxis(padded, 1, 0)

        def plane_image(pieces):
            planes, bin_plane = pieces
            products = lag_products(planes[0][None], planes[1][None], offset_lags, LMAX, NY)
            return combine(products, bin_plane.reshape(-1), weight_table).reshape(NANG, NY, NX)

        images = lax.map(plane_image, (moved, angle_bins))
        image_sum = image_sum + jnp.moveaxis(images, 0, 1)
    return image_sum.astype(jnp.bfloat16)
```

```python
import functools

import jax
import jax.numpy as jnp
from jax import lax
from jax.experimental import pallas as pl
from jax.experimental.pallas import tpu as pltpu
from jax.sharding import PartitionSpec as P

SECOND_COEF = (-205.0 / 72.0, 8.0 / 5.0, -1.0 / 5.0, 8.0 / 315.0, -1.0 / 560.0)
FIRST_COEF = (4.0 / 5.0, -1.0 / 5.0, 4.0 / 105.0, -1.0 / 280.0)
MESH = pl.DeviceIdType.MESH
F32 = jnp.float32
BF16 = jnp.bfloat16
LANES = 128
ROWS = 8
PAD = 4
LO, HI = 0, 1
OFFSETS = (-2, -1, 1, 2)


def kernel(
    sn_hbm, sb_hbm, rn_hbm, rb_hbm, speed_hbm, aniso_hbm, tilt_hbm, bins_hbm, wt_hbm,
    lags, scells, swave, rcells_hbm, rtraces_hbm,
    out_hbm,
    pw, qv, speed, a1, a2, bins, wt, rcells, rtraces, table, inj, base, grad,
    send0, send1, send2, recv0, recv1, recv2, win, acc, outv,
    in_sem, out_sem, send_sem0, recv_sem0, send_sem1, recv_sem1, send_sem2, recv_sem2,
):
    n = lax.axis_size("gy")
    me = lax.axis_index("gy")
    peer = {d: lax.rem(me + (d + n), n) for d in OFFSETS}
    zs = sn_hbm.shape[0]
    halves = sn_hbm.shape[2] // LANES
    n_off, n_bin, n_ang = wt_hbm.shape
    steps = swave.shape[0]
    n_src = scells.shape[0]
    rec_rows = rcells_hbm.shape[0]
    own = pl.ds(ROWS, ROWS)
    inner = pl.ds(PAD, zs)

    barrier = pltpu.get_barrier_semaphore()
    for d in OFFSETS:
        pl.semaphore_signal(barrier, inc=1, device_id={"gy": peer[d]}, device_id_type=MESH)

    copies = {}

    def fetch(name, index, src, dst):
        copy = pltpu.make_async_copy(src, dst, in_sem.at[index])
        copy.start()
        copies[name] = copy

    count = 0
    for m, ref in enumerate((sn_hbm, rn_hbm)):
        for x in range(halves):
            fetch(("now", m, x), count, ref.at[:, :, pl.ds(x * LANES, LANES)], pw.at[0, m, x, inner, own, :])
            count += 1
    for m, ref in enumerate((sb_hbm, rb_hbm)):
        for x in range(halves):
            fetch(("before", m, x), count, ref.at[:, :, pl.ds(x * LANES, LANES)], qv.at[m, x])
            count += 1
    for name, ref, dst in (("speed", speed_hbm, speed), ("aniso", aniso_hbm, a1), ("tilt", tilt_hbm, a2), ("bins", bins_hbm, bins)):
        for x in range(halves):
            fetch((name, x), count, ref.at[:, :, pl.ds(x * LANES, LANES)], dst.at[x])
            count += 1
    fetch("rcells", count, rcells_hbm, rcells)
    fetch("rtraces", count + 1, rtraces_hbm, rtraces)
    fetch("wt", count + 2, wt_hbm, wt)

    sub = lax.broadcasted_iota(jnp.int32, (ROWS, LANES), 0)
    lane = lax.broadcasted_iota(jnp.int32, (ROWS, LANES), 1)
    low_rows = sub < PAD

    def turn(v):
        return pltpu.roll(v, PAD, axis=v.ndim - 2)

    def pack(source, receiver, send, x, where_z):
        send[LO, x, where_z] = jnp.where(low_rows, source, turn(receiver)).astype(BF16)
        send[HI, x, where_z] = jnp.where(low_rows, turn(source), receiver).astype(BF16)

    def remote(src, dst, ssem, rsem, d):
        return pltpu.make_async_remote_copy(
            src_ref=src, dst_ref=dst, send_sem=ssem, recv_sem=rsem, device_id={"gy": peer[d]}, device_id_type=MESH
        )

    edge = jnp.zeros((PAD, ROWS, LANES), F32)
    for x in range(halves):
        for m in range(2):
            for s in range(steps):
                pw[s, m, x, pl.ds(0, PAD), own, :] = edge
                pw[s, m, x, pl.ds(PAD + zs, PAD), own, :] = edge
            grad[m, x, pl.ds(0, PAD)] = edge
            grad[m, x, pl.ds(PAD + zs, PAD)] = edge

    for m in range(2):
        for x in range(halves):
            copies[("now", m, x)].wait()
    for x in range(halves):
        pack(pw[0, 0, x, inner, own, :], pw[0, 1, x, inner, own, :], send0, x, pl.ds(0, zs))

    pl.semaphore_wait(barrier, len(OFFSETS))

    halo = [
        remote(send0.at[HI], recv0.at[0], send_sem0.at[0], recv_sem0.at[0], 1),
        remote(send0.at[LO], recv0.at[1], send_sem0.at[1], recv_sem0.at[1], -1),
    ]
    for copy in halo:
        copy.start()

    for x in range(halves):
        copies[("speed", x)].wait()
        copies[("aniso", x)].wait()
        copies[("tilt", x)].wait()
        a1[x] = speed[x] * (1.0 + 2.0 * a1[x])
        a2[x] = speed[x] * a2[x]

    def local_part(step):
        chunk = 2

        def part(i, carry):
            z = i * chunk
            for m in range(2):
                f = [pw[step, m, x, pl.ds(PAD + z, chunk), own, :] for x in range(halves)]
                first = [jnp.zeros_like(v) for v in f]
                second = [SECOND_COEF[0] * v for v in f]
                for k in range(1, PAD + 1):
                    up = [pltpu.roll(v, LANES - k, axis=2) for v in f] + [jnp.zeros_like(f[0])]
                    down = [jnp.zeros_like(f[0])] + [pltpu.roll(v, k, axis=2) for v in f]
                    for x in range(halves):
                        above = jnp.where(lane < LANES - k, up[x], up[x + 1])
                        below = jnp.where(lane >= k, down[x + 1], down[x])
                        second[x] = second[x] + SECOND_COEF[k] * (above + below)
                        first[x] = first[x] + FIRST_COEF[k - 1] * (above - below)
                for x in range(halves):
                    grad[m, x, pl.ds(PAD + z, chunk)] = first[x]
                    along_z = SECOND_COEF[0] * f[x]
                    for k in range(1, PAD + 1):
                        along_z = along_z + SECOND_COEF[k] * (
                            pw[step, m, x, pl.ds(PAD + z + k, chunk), own, :]
                            + pw[step, m, x, pl.ds(PAD + z - k, chunk), own, :]
                        )
                    before = qv[m, x, pl.ds(z, chunk)] if step == 0 else pw[step - 1, m, x, pl.ds(PAD + z, chunk), own, :]
                    base[m, x, pl.ds(z, chunk)] = (
                        2.0 * f[x]
                        - before
                        + a1[x, pl.ds(z, chunk)] * second[x]
                        + speed[x, pl.ds(z, chunk)] * along_z
                    )
            return carry

        lax.fori_loop(0, zs // chunk, part, 0)
        for m in range(2):
            for x in range(halves):
                base[m, x, 0] = base[m, x, 0] + inj[step, m, x]

    def injections():
        first_row = me * ROWS
        copies["rcells"].wait()
        copies["rtraces"].wait()
        left, right = [], []
        col_iota = lax.broadcasted_iota(jnp.int32, (halves * LANES, LANES), 0)
        for c in range(rec_rows):
            cell = rcells[c : c + 1, :]
            row = lax.shift_right_logical(cell, shift_bits) - first_row
            col = jnp.bitwise_and(cell, halves * LANES - 1)
            hit = jnp.broadcast_to(row, (ROWS, LANES)) == sub
            parts = []
            for s in range(steps):
                amount = jnp.broadcast_to(rtraces[s : s + 1, c * LANES : (c + 1) * LANES], (ROWS, LANES))
                amount = jnp.where(hit, amount, 0.0)
                coarse = amount.astype(BF16).astype(F32)
                parts += [coarse, amount - coarse]
            left.append(jnp.concatenate(parts, axis=0).astype(BF16))
            right.append(jnp.where(jnp.broadcast_to(col, col_iota.shape) == col_iota, 1.0, 0.0).astype(BF16))
        spread = lax.dot_general(
            jnp.concatenate(left, axis=1),
            jnp.concatenate(right, axis=1),
            (((1,), (1,)), ((), ())),
            preferred_element_type=F32,
        )
        for s in range(steps):
            total = spread[2 * s * ROWS : (2 * s + 1) * ROWS] + spread[(2 * s + 1) * ROWS : (2 * s + 2) * ROWS]
            for x in range(halves):
                inj[s, 1, x] = total[:, x * LANES : (x + 1) * LANES]
        for s in range(steps):
            for x in range(halves):
                total = jnp.zeros((ROWS, LANES), F32)
                for i in range(n_src):
                    cell = scells[i]
                    row = lax.shift_right_logical(cell, shift_bits) - first_row
                    col = jnp.bitwise_and(cell, halves * LANES - 1) - x * LANES
                    total = total + jnp.where((sub == row) & (lane == col), swave[s, i], 0.0)
                inj[s, 0, x] = total

    shift_bits = (halves * LANES).bit_length() - 1

    def halo_rows(step, below, above):
        for x in range(halves):
            low = below[x].astype(F32)
            high = above[x].astype(F32)
            pw[step, 0, x, inner, pl.ds(0, ROWS), :] = turn(low)
            pw[step, 1, x, inner, pl.ds(0, ROWS), :] = low
            pw[step, 0, x, inner, pl.ds(2 * ROWS, ROWS), :] = high
            pw[step, 1, x, inner, pl.ds(2 * ROWS, ROWS), :] = turn(high)

    def y_part(step, send):
        chunk = 4

        def along_y(i, carry):
            z = i * chunk
            for m in range(2):
                for x in range(halves):
                    def rows(k):
                        return pw[step, m, x, pl.ds(PAD + z, chunk), pl.ds(ROWS + k, ROWS), :]

                    second = SECOND_COEF[0] * rows(0)
                    first = grad[m, x, pl.ds(PAD + z, chunk)]
                    for k in range(1, PAD + 1):
                        above, below = rows(k), rows(-k)
                        second = second + SECOND_COEF[k] * (above + below)
                        first = first + FIRST_COEF[k - 1] * (above - below)
                    grad[m, x, pl.ds(PAD + z, chunk)] = first
                    base[m, x, pl.ds(z, chunk)] = base[m, x, pl.ds(z, chunk)] + a1[x, pl.ds(z, chunk)] * second
            return carry

        lax.fori_loop(0, zs // chunk, along_y, 0)

        def finish(i, carry):
            z = i * chunk
            for x in range(halves):
                new = []
                for m in range(2):
                    mixed = jnp.zeros((chunk, ROWS, LANES), F32)
                    for k in range(1, PAD + 1):
                        mixed = mixed + FIRST_COEF[k - 1] * (
                            grad[m, x, pl.ds(PAD + z + k, chunk)] - grad[m, x, pl.ds(PAD + z - k, chunk)]
                        )
                    value = base[m, x, pl.ds(z, chunk)] + a2[x, pl.ds(z, chunk)] * mixed
                    new.append(value)
                    if step + 1 < steps:
                        pw[step + 1, m, x, pl.ds(PAD + z, chunk), own, :] = value
                    win[step, m, x, pl.ds(z, chunk), pl.ds(2 * ROWS, ROWS), :] = value.astype(BF16).astype(F32)
                pack(new[0], new[1], send, x, pl.ds(z, chunk))
            return carry

        lax.fori_loop(0, zs // chunk, finish, 0)

    def open_block(step, d, recv):
        slot = OFFSETS.index(d)
        rows = pl.ds((2 + d) * ROWS, ROWS)
        for x in range(halves):
            low = recv[slot, LO, x].astype(F32)
            high = recv[slot, HI, x].astype(F32)
            win[step, 0, x, :, rows, :] = jnp.where(low_rows, low, turn(high))
            win[step, 1, x, :, rows, :] = jnp.where(low_rows, turn(low), high)

    chunk = 4
    groups = zs // chunk

    def image(step, last):
        def part(i, carry):
            x = i // groups
            z = lax.rem(i, groups) * chunk
            bin_ids = [bins[x, z + j] for j in range(chunk)]
            if step == 0:
                total = [[jnp.zeros((ROWS, LANES), F32)] * chunk for a in range(n_ang)]
            else:
                total = [[acc[a, x, z + j] for j in range(chunk)] for a in range(n_ang)]
            for h in range(n_off):
                lag = lags[h]
                product = (
                    win[step, 0, x, pl.ds(z, chunk), pl.ds(2 * ROWS - lag, ROWS), :]
                    * win[step, 1, x, pl.ds(z, chunk), pl.ds(2 * ROWS + lag, ROWS), :]
                )
                for a in range(n_ang):
                    weights = table[h, a]
                    for j in range(chunk):
                        weight = jnp.take_along_axis(weights, bin_ids[j], axis=0)
                        total[a][j] = total[a][j] + weight * product[j]
            for a in range(n_ang):
                for j in range(chunk):
                    if last:
                        outv[x, a, z + j] = total[a][j].astype(BF16)
                    else:
                        acc[a, x, z + j] = total[a][j]
            return carry

        lax.fori_loop(0, halves * groups, part, 0)

    injections()
    for m in range(2):
        for x in range(halves):
            copies[("before", m, x)].wait()
    local_part(0)
    copies["wt"].wait()
    for h in range(n_off):
        weights = wt[h].astype(F32)
        for a in range(n_ang):
            table[h, a] = jnp.broadcast_to(weights[:, a : a + 1], (n_bin, LANES))
    for x in range(halves):
        copies[("bins", x)].wait()

    for copy in halo:
        copy.wait_recv()
    halo_rows(0, recv0.at[0], recv0.at[1])
    y_part(0, send1)

    first = {}
    for index, (half, d) in enumerate(((HI, 1), (LO, -1), (LO, 1), (HI, -1))):
        slot = OFFSETS.index(-d)
        first[(half, d)] = remote(
            send1.at[half], recv1.at[slot, half], send_sem1.at[index], recv_sem1.at[index], d
        )
        first[(half, d)].start()
    for index, d in ((4, 2), (5, -2)):
        first[d] = remote(send1, recv1.at[OFFSETS.index(-d)], send_sem1.at[index], recv_sem1.at[index], d)
        first[d].start()

    local_part(1)
    first[(HI, 1)].wait_recv()
    first[(LO, -1)].wait_recv()
    halo_rows(1, recv1.at[OFFSETS.index(-1), HI], recv1.at[OFFSETS.index(1), LO])
    y_part(1, send2)

    second = {}
    for index, d in enumerate((2, -2, 1, -1)):
        second[d] = remote(send2, recv2.at[OFFSETS.index(-d)], send_sem2.at[index], recv_sem2.at[index], d)
        second[d].start()

    first[(LO, 1)].wait_recv()
    first[(HI, -1)].wait_recv()
    first[2].wait_recv()
    first[-2].wait_recv()
    for d in OFFSETS:
        open_block(0, d, recv1)
    image(0, False)

    for d in (1, -1, 2, -2):
        second[d].wait_recv()
        open_block(1, -d, recv2)
    image(1, True)

    writes = [
        pltpu.make_async_copy(outv.at[x], out_hbm.at[:, :, :, pl.ds(x * LANES, LANES)], out_sem.at[x])
        for x in range(halves)
    ]
    for copy in writes:
        copy.start()
    for copy in writes:
        copy.wait()
    for copy in halo + list(first.values()) + list(second.values()):
        copy.wait_send()


def per_device(
    source_now, source_before, receiver_now, receiver_before, speed_term, aniso_field, tilt_field,
    angle_bins, weight_table, offset_lags, source_cells, source_wavelet, receiver_cells, receiver_traces,
):
    zs, rows, width = source_now.shape
    halves = width // LANES
    steps = source_wavelet.shape[0]
    n_off, n_bin, n_ang = weight_table.shape
    receivers = receiver_cells.shape[0]
    assert rows == ROWS and n_bin == ROWS and width & (width - 1) == 0
    half = (halves, zs, ROWS, LANES)
    any_space = pl.BlockSpec(memory_space=pl.ANY)
    smem = pl.BlockSpec(memory_space=pltpu.SMEM)
    dma = pltpu.SemaphoreType.DMA
    in_specs = [any_space] * 9 + [smem] * 3 + [any_space] * 2
    return pl.pallas_call(
        kernel,
        out_shape=jax.ShapeDtypeStruct((n_ang, zs, rows, width), BF16),
        in_specs=in_specs,
        out_specs=any_space,
        scratch_shapes=[
            pltpu.VMEM((steps, 2, halves, zs + 2 * PAD, 3 * ROWS, LANES), F32),
            pltpu.VMEM((2,) + half, F32),
            pltpu.VMEM(half, F32),
            pltpu.VMEM(half, F32),
            pltpu.VMEM(half, F32),
            pltpu.VMEM(half, jnp.int32),
            pltpu.VMEM((n_off, n_bin, n_ang), BF16),
            pltpu.VMEM((receivers // LANES, LANES), jnp.int32),
            pltpu.VMEM((steps, receivers), F32),
            pltpu.VMEM((n_off, n_ang, n_bin, LANES), F32),
            pltpu.VMEM((steps, 2, halves, ROWS, LANES), F32),
            pltpu.VMEM((2,) + half, F32),
            pltpu.VMEM((2, halves, zs + 2 * PAD, ROWS, LANES), F32),
            pltpu.VMEM((2,) + half, BF16),
            pltpu.VMEM((2,) + half, BF16),
            pltpu.VMEM((2,) + half, BF16),
            pltpu.VMEM((2,) + half, BF16),
            pltpu.VMEM((len(OFFSETS), 2) + half, BF16),
            pltpu.VMEM((len(OFFSETS), 2) + half, BF16),
            pltpu.VMEM((steps, 2, halves, zs, 5 * ROWS, LANES), F32),
            pltpu.VMEM((n_ang,) + half, F32),
            pltpu.VMEM((halves, n_ang, zs, ROWS, LANES), BF16),
            dma((8 * halves + 3,)),
            dma((halves,)),
            dma((2,)),
            dma((2,)),
            dma((6,)),
            dma((6,)),
            dma((4,)),
            dma((4,)),
        ],
        compiler_params=pltpu.CompilerParams(collective_id=0, has_side_effects=True),
    )(
        source_now, source_before, receiver_now, receiver_before, speed_term, aniso_field, tilt_field,
        angle_bins, weight_table, offset_lags, source_cells, source_wavelet,
        receiver_cells.reshape(receivers // LANES, LANES), receiver_traces,
    )


def solution(mesh):
    return jax.shard_map(
        per_device,
        mesh=mesh,
        in_specs=(
            P("shot", "gy", None),
            P("shot", "gy", None),
            P("shot", "gy", None),
            P("shot", "gy", None),
            P(None, "gy", None),
            P(None, "gy", None),
            P(None, "gy", None),
            P(None, "gy", None),
            P(),
            P(),
            P("shot"),
            P("shot", None),
            P("shot"),
            P("shot", None),
        ),
        out_specs=P("shot", None, "gy", None),
        check_vma=False,
    )
```

```python
import functools

import jax
import jax.numpy as jnp
from jax import lax
from jax.experimental import pallas as pl
from jax.experimental.pallas import tpu as pltpu
from jax.sharding import PartitionSpec as P

SECOND_COEF = (-205.0 / 72.0, 8.0 / 5.0, -1.0 / 5.0, 8.0 / 315.0, -1.0 / 560.0)
FIRST_COEF = (4.0 / 5.0, -1.0 / 5.0, 4.0 / 105.0, -1.0 / 280.0)
MESH = pl.DeviceIdType.MESH
F32 = jnp.float32
BF16 = jnp.bfloat16
LANES = 128
ROWS = 8
PAD = 4
LO, HI = 0, 1
OFFSETS = (-2, -1, 1, 2)


def kernel(
    sn_hbm, sb_hbm, rn_hbm, rb_hbm, speed_hbm, aniso_hbm, tilt_hbm, bins_hbm, wt_hbm,
    lags_hbm, scells_hbm, swave_hbm, rcells_hbm, rtraces_hbm,
    out,
    pw, qv, speed, a1, a2, bins, wt, lags, scells, swave, rcells, rtraces, table, cache, inj, base, grad,
    send0, send1, send2, recv0, recv1, recv2, win, acc,
    in_sem, send_sem0, recv_sem0, send_sem1, recv_sem1, send_sem2, recv_sem2,
):
    n = lax.axis_size("gy")
    me = lax.axis_index("gy")
    peer = {d: lax.rem(me + (d + n), n) for d in OFFSETS}
    zs = sn_hbm.shape[0]
    halves = sn_hbm.shape[2] // LANES
    n_bin, n_ang, n_off = wt_hbm.shape
    steps = swave.shape[0]
    n_src = scells.shape[0]
    rec_rows = rcells_hbm.shape[0]
    own = pl.ds(ROWS, ROWS)
    inner = pl.ds(PAD, zs)

    barrier = pltpu.get_barrier_semaphore()
    for d in OFFSETS:
        pl.semaphore_signal(barrier, inc=1, device_id={"gy": peer[d]}, device_id_type=MESH)

    copies = {}

    def fetch(name, index, src, dst):
        copy = pltpu.make_async_copy(src, dst, in_sem.at[index])
        copy.start()
        copies[name] = copy

    count = 0
    for m, ref in enumerate((sn_hbm, rn_hbm)):
        for x in range(halves):
            fetch(("now", m, x), count, ref.at[:, :, pl.ds(x * LANES, LANES)], pw.at[0, m, x, inner, own, :])
            count += 1
    for m, ref in enumerate((sb_hbm, rb_hbm)):
        for x in range(halves):
            fetch(("before", m, x), count, ref.at[:, :, pl.ds(x * LANES, LANES)], qv.at[m, x])
            count += 1
    for name, ref, dst in (("speed", speed_hbm, speed), ("aniso", aniso_hbm, a1), ("tilt", tilt_hbm, a2), ("bins", bins_hbm, bins)):
        for x in range(halves):
            fetch((name, x), count, ref.at[:, :, pl.ds(x * LANES, LANES)], dst.at[x])
            count += 1
    fetch("rcells", count, rcells_hbm, rcells)
    fetch("rtraces", count + 1, rtraces_hbm, rtraces)
    fetch("wt", count + 2, wt_hbm, wt)
    fetch("lags", count + 3, lags_hbm, lags)
    fetch("scells", count + 4, scells_hbm, scells)
    fetch("swave", count + 5, swave_hbm, swave)

    sub = lax.broadcasted_iota(jnp.int32, (ROWS, LANES), 0)
    lane = lax.broadcasted_iota(jnp.int32, (ROWS, LANES), 1)
    low_rows = sub < PAD

    def turn(v):
        return pltpu.roll(v, PAD, axis=v.ndim - 2)

    def pack(source, receiver, send, x, where_z):
        send[x, LO, where_z] = jnp.where(low_rows, source, turn(receiver)).astype(BF16)
        send[x, HI, where_z] = jnp.where(low_rows, turn(source), receiver).astype(BF16)

    def remote(src, dst, ssem, rsem, d):
        return pltpu.make_async_remote_copy(
            src_ref=src, dst_ref=dst, send_sem=ssem, recv_sem=rsem, device_id={"gy": peer[d]}, device_id_type=MESH
        )

    halo = [
        (
            remote(send0.at[x, HI], recv0.at[x, 0], send_sem0.at[2 * x], recv_sem0.at[2 * x], 1),
            remote(send0.at[x, LO], recv0.at[x, 1], send_sem0.at[2 * x + 1], recv_sem0.at[2 * x + 1], -1),
        )
        for x in range(halves)
    ]
    for x in range(halves):
        for m in range(2):
            copies[("now", m, x)].wait()
        pack(pw[0, 0, x, inner, own, :], pw[0, 1, x, inner, own, :], send0, x, pl.ds(0, zs))
        if x == 0:
            pl.semaphore_wait(barrier, len(OFFSETS))
        for copy in halo[x]:
            copy.start()

    edge = jnp.zeros((PAD, ROWS, LANES), F32)
    for x in range(halves):
        for m in range(2):
            for s in range(steps):
                pw[s, m, x, pl.ds(0, PAD), own, :] = edge
                pw[s, m, x, pl.ds(PAD + zs, PAD), own, :] = edge
            grad[m, x, pl.ds(0, PAD)] = edge
            grad[m, x, pl.ds(PAD + zs, PAD)] = edge

    for x in range(halves):
        copies[("speed", x)].wait()
        copies[("aniso", x)].wait()
        copies[("tilt", x)].wait()
        a1[x] = speed[x] * (1.0 + 2.0 * a1[x])
        a2[x] = speed[x] * a2[x]

    def local_part(step):
        chunk = 2

        def part(i, carry):
            z = i * chunk
            for m in range(2):
                f = [pw[step, m, x, pl.ds(PAD + z, chunk), own, :] for x in range(halves)]
                first = [jnp.zeros_like(v) for v in f]
                second = [SECOND_COEF[0] * v for v in f]
                for k in range(1, PAD + 1):
                    up = [pltpu.roll(v, LANES - k, axis=2) for v in f] + [jnp.zeros_like(f[0])]
                    down = [jnp.zeros_like(f[0])] + [pltpu.roll(v, k, axis=2) for v in f]
                    for x in range(halves):
                        above = jnp.where(lane < LANES - k, up[x], up[x + 1])
                        below = jnp.where(lane >= k, down[x + 1], down[x])
                        second[x] = second[x] + SECOND_COEF[k] * (above + below)
                        first[x] = first[x] + FIRST_COEF[k - 1] * (above - below)
                for x in range(halves):
                    grad[m, x, pl.ds(PAD + z, chunk)] = first[x]
                    along_z = SECOND_COEF[0] * f[x]
                    for k in range(1, PAD + 1):
                        along_z = along_z + SECOND_COEF[k] * (
                            pw[step, m, x, pl.ds(PAD + z + k, chunk), own, :]
                            + pw[step, m, x, pl.ds(PAD + z - k, chunk), own, :]
                        )
                    before = qv[m, x, pl.ds(z, chunk)] if step == 0 else pw[step - 1, m, x, pl.ds(PAD + z, chunk), own, :]
                    base[m, x, pl.ds(z, chunk)] = (
                        2.0 * f[x]
                        - before
                        + a1[x, pl.ds(z, chunk)] * second[x]
                        + speed[x, pl.ds(z, chunk)] * along_z
                    )
            return carry

        lax.fori_loop(0, zs // chunk, part, 0)
        for m in range(2):
            for x in range(halves):
                base[m, x, 0] = base[m, x, 0] + inj[step, m, x]

    def injections():
        first_row = me * ROWS
        for name in ("rcells", "rtraces", "scells", "swave"):
            copies[name].wait()
        left, right = [], []
        col_iota = lax.broadcasted_iota(jnp.int32, (halves * LANES, LANES), 0)
        for c in range(rec_rows):
            cell = rcells[c : c + 1, :]
            row = lax.shift_right_logical(cell, shift_bits) - first_row
            col = jnp.bitwise_and(cell, halves * LANES - 1)
            hit = jnp.broadcast_to(row, (ROWS, LANES)) == sub
            parts = []
            for s in range(steps):
                amount = jnp.broadcast_to(rtraces[s : s + 1, c * LANES : (c + 1) * LANES], (ROWS, LANES))
                amount = jnp.where(hit, amount, 0.0)
                coarse = amount.astype(BF16).astype(F32)
                parts += [coarse, amount - coarse]
            left.append(jnp.concatenate(parts, axis=0).astype(BF16))
            right.append(jnp.where(jnp.broadcast_to(col, col_iota.shape) == col_iota, 1.0, 0.0).astype(BF16))
        spread = lax.dot_general(
            jnp.concatenate(left, axis=1),
            jnp.concatenate(right, axis=1),
            (((1,), (1,)), ((), ())),
            preferred_element_type=F32,
        )
        for s in range(steps):
            total = spread[2 * s * ROWS : (2 * s + 1) * ROWS] + spread[(2 * s + 1) * ROWS : (2 * s + 2) * ROWS]
            for x in range(halves):
                inj[s, 1, x] = total[:, x * LANES : (x + 1) * LANES]
        for s in range(steps):
            for x in range(halves):
                total = jnp.zeros((ROWS, LANES), F32)
                for i in range(n_src):
                    cell = scells[i]
                    row = lax.shift_right_logical(cell, shift_bits) - first_row
                    col = jnp.bitwise_and(cell, halves * LANES - 1) - x * LANES
                    total = total + jnp.where((sub == row) & (lane == col), swave[s, i], 0.0)
                inj[s, 0, x] = total

    shift_bits = (halves * LANES).bit_length() - 1

    def halo_rows(step, x, below, above):
        low = below[...].astype(F32)
        high = above[...].astype(F32)
        pw[step, 0, x, inner, pl.ds(0, ROWS), :] = turn(low)
        pw[step, 1, x, inner, pl.ds(0, ROWS), :] = low
        pw[step, 0, x, inner, pl.ds(2 * ROWS, ROWS), :] = high
        pw[step, 1, x, inner, pl.ds(2 * ROWS, ROWS), :] = turn(high)

    def y_part(step, x, send):
        chunk = 4

        def along_y(i, carry):
            z = i * chunk
            for m in range(2):

                def rows(k):
                    return pw[step, m, x, pl.ds(PAD + z, chunk), pl.ds(ROWS + k, ROWS), :]

                second = SECOND_COEF[0] * rows(0)
                first = grad[m, x, pl.ds(PAD + z, chunk)]
                for k in range(1, PAD + 1):
                    above, below = rows(k), rows(-k)
                    second = second + SECOND_COEF[k] * (above + below)
                    first = first + FIRST_COEF[k - 1] * (above - below)
                grad[m, x, pl.ds(PAD + z, chunk)] = first
                base[m, x, pl.ds(z, chunk)] = base[m, x, pl.ds(z, chunk)] + a1[x, pl.ds(z, chunk)] * second
            return carry

        lax.fori_loop(0, zs // chunk, along_y, 0)

        def finish(i, carry):
            z = i * chunk
            new = []
            for m in range(2):
                mixed = jnp.zeros((chunk, ROWS, LANES), F32)
                for k in range(1, PAD + 1):
                    mixed = mixed + FIRST_COEF[k - 1] * (
                        grad[m, x, pl.ds(PAD + z + k, chunk)] - grad[m, x, pl.ds(PAD + z - k, chunk)]
                    )
                value = base[m, x, pl.ds(z, chunk)] + a2[x, pl.ds(z, chunk)] * mixed
                new.append(value)
                if step + 1 < steps:
                    pw[step + 1, m, x, pl.ds(PAD + z, chunk), own, :] = value
                win[step, m, x, pl.ds(z, chunk), pl.ds(2 * ROWS, ROWS), :] = value.astype(BF16).astype(F32)
            pack(new[0], new[1], send, x, pl.ds(z, chunk))
            return carry

        lax.fori_loop(0, zs // chunk, finish, 0)

    def open_block(step, x, d, recv):
        slot = OFFSETS.index(d)
        rows = pl.ds((2 + d) * ROWS, ROWS)
        low = recv[slot, x, LO].astype(F32)
        high = recv[slot, x, HI].astype(F32)
        win[step, 0, x, :, rows, :] = jnp.where(low_rows, low, turn(high))
        win[step, 1, x, :, rows, :] = jnp.where(low_rows, turn(low), high)

    chunk = 4
    groups = zs // chunk

    def image(step, x):
        def part(i, carry):
            z = i * chunk
            if step == 0:
                bin_ids = [bins[x, z + j] for j in range(chunk)]
                total = [jnp.zeros((chunk, ROWS, LANES), F32)] * n_ang
            else:
                total = [acc[a, x, pl.ds(z, chunk)] for a in range(n_ang)]
            for h in range(n_off):
                lag = lags[h]
                product = (
                    win[step, 0, x, pl.ds(z, chunk), pl.ds(2 * ROWS - lag, ROWS), :]
                    * win[step, 1, x, pl.ds(z, chunk), pl.ds(2 * ROWS + lag, ROWS), :]
                )
                for a in range(n_ang):
                    if step == 0:
                        row = table[h, a]
                        weight = jnp.stack([jnp.take_along_axis(row, bin_ids[j], axis=0) for j in range(chunk)])
                        cache[h, a, x, pl.ds(z, chunk)] = weight
                    else:
                        weight = cache[h, a, x, pl.ds(z, chunk)]
                    total[a] = total[a] + weight * product
            for a in range(n_ang):
                if step + 1 == steps:
                    out[a, pl.ds(z, chunk), :, x * LANES : (x + 1) * LANES] = total[a].astype(BF16)
                else:
                    acc[a, x, pl.ds(z, chunk)] = total[a]
            return carry

        lax.fori_loop(0, groups, part, 0)

    for m in range(2):
        for x in range(halves):
            copies[("before", m, x)].wait()
    injections()
    local_part(0)
    copies["wt"].wait()
    copies["lags"].wait()
    by_bin = [wt[b].astype(F32) for b in range(n_bin)]
    for a in range(n_ang):
        rows = jnp.concatenate([v[a : a + 1] for v in by_bin], axis=0)
        for h in range(n_off):
            table[h, a] = jnp.broadcast_to(rows[:, h : h + 1], (n_bin, LANES))
    for x in range(halves):
        copies[("bins", x)].wait()

    slot_of = {d: OFFSETS.index(-d) for d in OFFSETS}
    border = []
    for x in range(halves):
        for copy in halo[x]:
            copy.wait_recv()
        halo_rows(0, x, recv0.at[x, 0], recv0.at[x, 1])
        y_part(0, x, send1)
        border.append(
            [
                remote(send1.at[x, half], recv1.at[slot_of[d], x, half], send_sem1.at[2 * x + i], recv_sem1.at[2 * x + i], d)
                for i, (half, d) in enumerate(((HI, 1), (LO, -1)))
            ]
        )
        for copy in border[x]:
            copy.start()
    rest = [
        remote(send1.at[:, half], recv1.at[slot_of[d], :, half], send_sem1.at[2 * halves + i], recv_sem1.at[2 * halves + i], d)
        for i, (half, d) in enumerate(((LO, 1), (HI, -1)))
    ] + [
        remote(send1, recv1.at[slot_of[d]], send_sem1.at[2 * halves + 2 + i], recv_sem1.at[2 * halves + 2 + i], d)
        for i, d in enumerate((2, -2))
    ]
    for copy in rest:
        copy.start()

    local_part(1)
    final = []
    for x in range(halves):
        for copy in border[x]:
            copy.wait_recv()
        halo_rows(1, x, recv1.at[slot_of[1], x, HI], recv1.at[slot_of[-1], x, LO])
        y_part(1, x, send2)
        final.append(
            [
                remote(send2.at[x], recv2.at[slot_of[d], x], send_sem2.at[4 * x + i], recv_sem2.at[4 * x + i], d)
                for i, d in enumerate((2, -2, 1, -1))
            ]
        )
        for copy in final[x]:
            copy.start()

    for copy in rest:
        copy.wait_recv()
    for x in range(halves):
        for d in OFFSETS:
            open_block(0, x, d, recv1)
        image(0, x)

    for x in range(halves):
        for copy in final[x]:
            copy.wait_recv()
        for d in OFFSETS:
            open_block(1, x, d, recv2)
        image(1, x)

    for copy in sum([list(c) for c in halo + border + final], []) + rest:
        copy.wait_send()


def per_device(
    source_now, source_before, receiver_now, receiver_before, speed_term, aniso_field, tilt_field,
    angle_bins, weight_table, offset_lags, source_cells, source_wavelet, receiver_cells, receiver_traces,
):
    zs, rows, width = source_now.shape
    halves = width // LANES
    steps = source_wavelet.shape[0]
    n_off, n_bin, n_ang = weight_table.shape
    n_src = source_cells.shape[0]
    receivers = receiver_cells.shape[0]
    assert rows == ROWS and n_bin == ROWS and width & (width - 1) == 0
    half = (halves, zs, ROWS, LANES)
    block = (halves, 2, zs, ROWS, LANES)
    any_space = pl.BlockSpec(memory_space=pl.ANY)
    dma = pltpu.SemaphoreType.DMA
    in_specs = [any_space] * 14
    return pl.pallas_call(
        kernel,
        out_shape=pltpu.VMEM((n_ang, zs, rows, width), BF16),
        in_specs=in_specs,
        out_specs=pl.BlockSpec(memory_space=pltpu.VMEM),
        scratch_shapes=[
            pltpu.VMEM((steps, 2, halves, zs + 2 * PAD, 3 * ROWS, LANES), F32),
            pltpu.VMEM((2,) + half, F32),
            pltpu.VMEM(half, F32),
            pltpu.VMEM(half, F32),
            pltpu.VMEM(half, F32),
            pltpu.VMEM(half, jnp.int32),
            pltpu.VMEM((n_bin, n_ang, n_off), BF16),
            pltpu.SMEM((n_off,), jnp.int32),
            pltpu.SMEM((n_src,), jnp.int32),
            pltpu.SMEM((steps, n_src), F32),
            pltpu.VMEM((receivers // LANES, LANES), jnp.int32),
            pltpu.VMEM((steps, receivers), F32),
            pltpu.VMEM((n_off, n_ang, n_bin, LANES), F32),
            pltpu.VMEM((n_off, n_ang) + half, F32),
            pltpu.VMEM((steps, 2, halves, ROWS, LANES), F32),
            pltpu.VMEM((2,) + half, F32),
            pltpu.VMEM((2, halves, zs + 2 * PAD, ROWS, LANES), F32),
            pltpu.VMEM(block, BF16),
            pltpu.VMEM(block, BF16),
            pltpu.VMEM(block, BF16),
            pltpu.VMEM(block, BF16),
            pltpu.VMEM((len(OFFSETS),) + block, BF16),
            pltpu.VMEM((len(OFFSETS),) + block, BF16),
            pltpu.VMEM((steps, 2, halves, zs, 5 * ROWS, LANES), F32),
            pltpu.VMEM((n_ang,) + half, F32),
            dma((8 * halves + 6,)),
            dma((2 * halves,)),
            dma((2 * halves,)),
            dma((2 * halves + 4,)),
            dma((2 * halves + 4,)),
            dma((4 * halves,)),
            dma((4 * halves,)),
        ],
        compiler_params=pltpu.CompilerParams(collective_id=0, has_side_effects=True),
    )(
        source_now, source_before, receiver_now, receiver_before, speed_term, aniso_field, tilt_field,
        angle_bins, jnp.transpose(weight_table, (1, 2, 0)), offset_lags, source_cells, source_wavelet,
        receiver_cells.reshape(receivers // LANES, LANES), receiver_traces,
    )


def solution(mesh):
    return jax.shard_map(
        per_device,
        mesh=mesh,
        in_specs=(
            P("shot", "gy", None),
            P("shot", "gy", None),
            P("shot", "gy", None),
            P("shot", "gy", None),
            P(None, "gy", None),
            P(None, "gy", None),
            P(None, "gy", None),
            P(None, "gy", None),
            P(),
            P(),
            P("shot"),
            P("shot", None),
            P("shot"),
            P("shot", None),
        ),
        out_specs=P("shot", None, "gy", None),
        check_vma=False,
    )
```

```python
import functools

import jax
import jax.numpy as jnp
from jax import lax
from jax.experimental import pallas as pl
from jax.experimental.pallas import tpu as pltpu
from jax.sharding import PartitionSpec as P

SECOND_COEF = (-205.0 / 72.0, 8.0 / 5.0, -1.0 / 5.0, 8.0 / 315.0, -1.0 / 560.0)
FIRST_COEF = (4.0 / 5.0, -1.0 / 5.0, 4.0 / 105.0, -1.0 / 280.0)
MESH = pl.DeviceIdType.MESH
F32 = jnp.float32
BF16 = jnp.bfloat16
LANES = 128
ROWS = 8
PAD = 4
LO, HI = 0, 1
OFFSETS = (-2, -1, 1, 2)


def kernel(
    sn_hbm, sb_hbm, rn_hbm, rb_hbm, speed_hbm, aniso_hbm, tilt_hbm, bins_hbm, wt_hbm,
    lags_hbm, scells_hbm, swave_hbm, rcells_hbm, rtraces_hbm,
    out,
    pw, qv, speed, a1, a2, bins, wt, lags, scells, swave, rcells, rtraces, table, cache, inj, base, grad,
    hw, share2, share1, send0, sendc, sendp, send1, send2, recv0, recvc, recvp, recv1, recv2, win, acc,
    in_sem, send_sem0, recv_sem0, send_semc, recv_semc, send_semp, recv_semp, send_sem1, recv_sem1, send_sem2, recv_sem2,
):
    n = lax.axis_size("gy")
    me = lax.axis_index("gy")
    peer = {d: lax.rem(me + (d + n), n) for d in OFFSETS}
    zs = sn_hbm.shape[0]
    halves = sn_hbm.shape[2] // LANES
    n_bin, n_ang, n_off = wt_hbm.shape
    steps = swave.shape[0]
    n_src = scells.shape[0]
    rec_rows = rcells_hbm.shape[0]
    own = pl.ds(ROWS, ROWS)
    inner = pl.ds(PAD, zs)

    barrier = pltpu.get_barrier_semaphore()
    for d in OFFSETS:
        pl.semaphore_signal(barrier, inc=1, device_id={"gy": peer[d]}, device_id_type=MESH)

    copies = {}

    def fetch(name, index, src, dst):
        copy = pltpu.make_async_copy(src, dst, in_sem.at[index])
        copy.start()
        copies[name] = copy

    wanted = [
        (("now", m, x), ref.at[:, :, pl.ds(x * LANES, LANES)], pw.at[0, m, x, inner, own, :])
        for x in range(halves)
        for m, ref in enumerate((sn_hbm, rn_hbm))
    ]
    wanted += [("rcells", rcells_hbm, rcells), ("rtraces", rtraces_hbm, rtraces)]
    wanted += [("scells", scells_hbm, scells), ("swave", swave_hbm, swave)]
    for name, ref, dst in (("speed", speed_hbm, speed), ("aniso", aniso_hbm, a1), ("tilt", tilt_hbm, a2)):
        wanted += [((name, x), ref.at[:, :, pl.ds(x * LANES, LANES)], dst.at[x]) for x in range(halves)]
    for m, ref in enumerate((sb_hbm, rb_hbm)):
        wanted += [(("before", m, x), ref.at[:, :, pl.ds(x * LANES, LANES)], qv.at[m, x]) for x in range(halves)]
    wanted += [(("bins", x), bins_hbm.at[:, :, pl.ds(x * LANES, LANES)], bins.at[x]) for x in range(halves)]
    wanted += [("wt", wt_hbm, wt), ("lags", lags_hbm, lags)]
    for index, (name, src, dst) in enumerate(wanted):
        fetch(name, index, src, dst)

    edge = jnp.zeros((PAD, ROWS, LANES), F32)
    plane = jnp.zeros((zs, ROWS, LANES), F32)
    for x in range(halves):
        for m in range(2):
            for s in range(steps):
                pw[s, m, x, pl.ds(0, PAD), own, :] = edge
                pw[s, m, x, pl.ds(PAD + zs, PAD), own, :] = edge
            pw[0, m, x, inner, pl.ds(0, ROWS), :] = plane
            pw[0, m, x, inner, pl.ds(2 * ROWS, ROWS), :] = plane
            hw[m, x, :, own, :] = plane
            for padded in (grad, share1):
                padded[m, x, pl.ds(0, PAD)] = edge
                padded[m, x, pl.ds(PAD + zs, PAD)] = edge

    sub = lax.broadcasted_iota(jnp.int32, (ROWS, LANES), 0)
    lane = lax.broadcasted_iota(jnp.int32, (ROWS, LANES), 1)
    low_rows = sub < PAD

    def turn(v):
        return pltpu.roll(v, PAD, axis=v.ndim - 2)

    def pack(source, receiver, send, x, where_z):
        send[x, LO, where_z] = jnp.where(low_rows, source, turn(receiver)).astype(BF16)
        send[x, HI, where_z] = jnp.where(low_rows, turn(source), receiver).astype(BF16)

    def remote(src, dst, ssem, rsem, d):
        return pltpu.make_async_remote_copy(
            src_ref=src, dst_ref=dst, send_sem=ssem, recv_sem=rsem, device_id={"gy": peer[d]}, device_id_type=MESH
        )

    halo = [
        (
            remote(send0.at[x, HI], recv0.at[x, 0], send_sem0.at[2 * x], recv_sem0.at[2 * x], 1),
            remote(send0.at[x, LO], recv0.at[x, 1], send_sem0.at[2 * x + 1], recv_sem0.at[2 * x + 1], -1),
        )
        for x in range(halves)
    ]
    for x in range(halves):
        for m in range(2):
            copies[("now", m, x)].wait()
        pack(pw[0, 0, x, inner, own, :], pw[0, 1, x, inner, own, :], send0, x, pl.ds(0, zs))
        if x == 0:
            pl.semaphore_wait(barrier, len(OFFSETS))
        for copy in halo[x]:
            copy.start()

    def local_part(step):
        chunk = 4

        def part(i, carry):
            z = i * chunk
            for m in range(2):
                f = [pw[step, m, x, pl.ds(PAD + z, chunk), own, :] for x in range(halves)]
                first = [jnp.zeros_like(v) for v in f]
                second = [SECOND_COEF[0] * v for v in f]
                for k in range(1, PAD + 1):
                    up = [pltpu.roll(v, LANES - k, axis=2) for v in f] + [jnp.zeros_like(f[0])]
                    down = [jnp.zeros_like(f[0])] + [pltpu.roll(v, k, axis=2) for v in f]
                    for x in range(halves):
                        above = jnp.where(lane < LANES - k, up[x], up[x + 1])
                        below = jnp.where(lane >= k, down[x + 1], down[x])
                        second[x] = second[x] + SECOND_COEF[k] * (above + below)
                        first[x] = first[x] + FIRST_COEF[k - 1] * (above - below)
                for x in range(halves):
                    grad[m, x, pl.ds(PAD + z, chunk)] = first[x]
                    along_z = SECOND_COEF[0] * f[x]
                    for k in range(1, PAD + 1):
                        along_z = along_z + SECOND_COEF[k] * (
                            pw[step, m, x, pl.ds(PAD + z + k, chunk), own, :]
                            + pw[step, m, x, pl.ds(PAD + z - k, chunk), own, :]
                        )
                    before = qv[m, x, pl.ds(z, chunk)] if step == 0 else pw[step - 1, m, x, pl.ds(PAD + z, chunk), own, :]
                    base[m, x, pl.ds(z, chunk)] = (
                        2.0 * f[x]
                        - before
                        + a1[x, pl.ds(z, chunk)] * second[x]
                        + speed[x, pl.ds(z, chunk)] * along_z
                    )
            return carry

        lax.fori_loop(0, zs // chunk, part, 0)
        for m in range(2):
            for x in range(halves):
                base[m, x, 0] = base[m, x, 0] + inj[step, m, x]

    def injections():
        first_row = me * ROWS
        for name in ("rcells", "rtraces", "scells", "swave"):
            copies[name].wait()
        left, right = [], []
        col_iota = lax.broadcasted_iota(jnp.int32, (halves * LANES, LANES), 0)
        for c in range(rec_rows):
            cell = rcells[c : c + 1, :]
            row = lax.shift_right_logical(cell, shift_bits) - first_row
            col = jnp.bitwise_and(cell, halves * LANES - 1)
            hit = jnp.broadcast_to(row, (ROWS, LANES)) == sub
            parts = []
            for s in range(steps):
                amount = jnp.broadcast_to(rtraces[s : s + 1, c * LANES : (c + 1) * LANES], (ROWS, LANES))
                amount = jnp.where(hit, amount, 0.0)
                coarse = amount.astype(BF16).astype(F32)
                parts += [coarse, amount - coarse]
            left.append(jnp.concatenate(parts, axis=0).astype(BF16))
            right.append(jnp.where(jnp.broadcast_to(col, col_iota.shape) == col_iota, 1.0, 0.0).astype(BF16))
        spread = lax.dot_general(
            jnp.concatenate(left, axis=1),
            jnp.concatenate(right, axis=1),
            (((1,), (1,)), ((), ())),
            preferred_element_type=F32,
        )
        for s in range(steps):
            total = spread[2 * s * ROWS : (2 * s + 1) * ROWS] + spread[(2 * s + 1) * ROWS : (2 * s + 2) * ROWS]
            for x in range(halves):
                inj[s, 1, x] = total[:, x * LANES : (x + 1) * LANES]
        for s in range(steps):
            for x in range(halves):
                total = jnp.zeros((ROWS, LANES), F32)
                for i in range(n_src):
                    cell = scells[i]
                    row = lax.shift_right_logical(cell, shift_bits) - first_row
                    col = jnp.bitwise_and(cell, halves * LANES - 1) - x * LANES
                    total = total + jnp.where((sub == row) & (lane == col), swave[s, i], 0.0)
                inj[s, 0, x] = total

    shift_bits = (halves * LANES).bit_length() - 1

    def halo_rows(window, x, low, high):
        window[0, x, :, pl.ds(0, ROWS), :] = turn(low)
        window[1, x, :, pl.ds(0, ROWS), :] = low
        window[0, x, :, pl.ds(2 * ROWS, ROWS), :] = high
        window[1, x, :, pl.ds(2 * ROWS, ROWS), :] = turn(high)

    part_chunk = 4

    def along_y(window, x, whole):
        def part(i, carry):
            z = i * part_chunk
            cells = pl.ds(z, part_chunk)
            for m in range(2):

                def rows(k):
                    return window[m, x, cells, pl.ds(ROWS + k, ROWS), :]

                second, first = 0.0, 0.0
                if whole:
                    second, first = SECOND_COEF[0] * rows(0), grad[m, x, pl.ds(PAD + z, part_chunk)]
                for k in range(1, PAD + 1):
                    above, below = rows(k), rows(-k)
                    second = second + SECOND_COEF[k] * (above + below)
                    first = first + FIRST_COEF[k - 1] * (above - below)
                grad[m, x, pl.ds(PAD + z, part_chunk)] = first
                base[m, x, cells] = base[m, x, cells] + a1[x, cells] * second
            return carry

        lax.fori_loop(0, zs // part_chunk, part, 0)

    def along_z(padded, member, x, z):
        mixed = jnp.zeros((part_chunk, ROWS, LANES), F32)
        for k in range(1, PAD + 1):
            mixed = mixed + FIRST_COEF[k - 1] * (
                padded[member, x, pl.ds(PAD + z + k, part_chunk)] - padded[member, x, pl.ds(PAD + z - k, part_chunk)]
            )
        return mixed

    def finish(step, x, send, whole=True):
        def part(i, carry):
            z = i * part_chunk
            cells = pl.ds(z, part_chunk)
            new = []
            for m in range(2):
                value = base[m, x, cells] + a2[x, cells] * along_z(grad, m, x, z)
                new.append(value)
                if not whole:
                    base[m, x, cells] = value
                    continue
                if step + 1 < steps:
                    pw[step + 1, m, x, pl.ds(PAD + z, part_chunk), own, :] = value
                win[step, m, x, cells, pl.ds(2 * ROWS, ROWS), :] = value.astype(BF16).astype(F32)
            pack(new[0], new[1], send, x, cells)
            return carry

        lax.fori_loop(0, zs // part_chunk, part, 0)

    def shares(x):
        def part(i, carry):
            z = i * part_chunk
            for side in range(2):
                second, first = [], []
                for m in range(2):
                    two, one = 0.0, 0.0
                    for k in range(1, PAD + 1):
                        row = ROWS - PAD + k if side == 0 else 2 * ROWS - k
                        value = pw[0, m, x, pl.ds(PAD + z, part_chunk), pl.ds(row, ROWS), :]
                        two = two + SECOND_COEF[k] * value
                        one = one + (FIRST_COEF[k - 1] if side == 0 else -FIRST_COEF[k - 1]) * value
                    second.append(two)
                    first.append(one)
                share2[side, x, pl.ds(z, part_chunk)] = jnp.where(low_rows, second[0], turn(second[1]))
                share1[side, x, pl.ds(PAD + z, part_chunk)] = jnp.where(low_rows, first[0], turn(first[1]))
            return carry

        lax.fori_loop(0, zs // part_chunk, part, 0)

    def border_rows(x):
        whole = []
        for side in range(2):
            blocks = []
            for z in range(0, zs, part_chunk):
                cells = pl.ds(z, part_chunk)
                pair = recvc[side, x, cells].astype(F32)
                flat, tilted = jnp.where(low_rows, pair, turn(pair)), jnp.where(low_rows, turn(pair), pair)
                blocks.append(
                    recvp[x, side, cells].astype(F32)
                    + flat * share2[side, x, cells]
                    + tilted * along_z(share1, side, x, z)
                )
            whole.append(jnp.concatenate(blocks, axis=0))
        halo_rows(pw.at[1, :, :, inner], x, whole[0], whole[1])

    def open_block(step, x, d, recv):
        slot = OFFSETS.index(d)
        rows = pl.ds((2 + d) * ROWS, ROWS)
        low = recv[slot, x, LO].astype(F32)
        high = recv[slot, x, HI].astype(F32)
        win[step, 0, x, :, rows, :] = jnp.where(low_rows, low, turn(high))
        win[step, 1, x, :, rows, :] = jnp.where(low_rows, turn(low), high)

    chunk = 4
    groups = zs // chunk

    def image(step, x):
        def part(i, carry):
            z = i * chunk
            if step == 0:
                bin_ids = [bins[x, z + j] for j in range(chunk)]
                total = [jnp.zeros((chunk, ROWS, LANES), F32)] * n_ang
            else:
                total = [acc[a, x, pl.ds(z, chunk)] for a in range(n_ang)]
            for h in range(n_off):
                lag = lags[h]
                product = (
                    win[step, 0, x, pl.ds(z, chunk), pl.ds(2 * ROWS - lag, ROWS), :]
                    * win[step, 1, x, pl.ds(z, chunk), pl.ds(2 * ROWS + lag, ROWS), :]
                )
                for a in range(n_ang):
                    if step == 0:
                        row = table[h, a]
                        weight = jnp.stack([jnp.take_along_axis(row, bin_ids[j], axis=0) for j in range(chunk)])
                        cache[h, a, x, pl.ds(z, chunk)] = weight
                    else:
                        weight = cache[h, a, x, pl.ds(z, chunk)]
                    total[a] = total[a] + weight * product
            for a in range(n_ang):
                if step + 1 == steps:
                    out[a, pl.ds(z, chunk), :, x * LANES : (x + 1) * LANES] = total[a].astype(BF16)
                else:
                    acc[a, x, pl.ds(z, chunk)] = total[a]
            return carry

        lax.fori_loop(0, groups, part, 0)

    injections()
    for x in range(halves):
        copies[("speed", x)].wait()
        copies[("aniso", x)].wait()
        copies[("tilt", x)].wait()
        a1[x] = speed[x] * (1.0 + 2.0 * a1[x])
        a2[x] = speed[x] * a2[x]
        pack(a1[x], a2[x], sendc, x, pl.ds(0, zs))
    coefs = [
        remote(sendc.at[:, half], recvc.at[i], send_semc.at[i], recv_semc.at[i], d)
        for i, (half, d) in enumerate(((HI, 1), (LO, -1)))
    ]
    for copy in coefs:
        copy.start()
    for m in range(2):
        for x in range(halves):
            copies[("before", m, x)].wait()
    local_part(0)
    partial = []
    for x in range(halves):
        along_y(pw.at[0, :, :, inner], x, True)
        finish(0, x, sendp, whole=False)
        partial.append(
            [
                remote(sendp.at[x, half], recvp.at[x, i], send_semp.at[2 * x + i], recv_semp.at[2 * x + i], d)
                for i, (half, d) in enumerate(((HI, 1), (LO, -1)))
            ]
        )
        for copy in partial[x]:
            copy.start()
    for x in range(halves):
        shares(x)
    copies["wt"].wait()
    copies["lags"].wait()
    by_bin = [wt[b].astype(F32) for b in range(n_bin)]
    for a in range(n_ang):
        rows = jnp.concatenate([v[a : a + 1] for v in by_bin], axis=0)
        for h in range(n_off):
            table[h, a] = jnp.broadcast_to(rows[:, h : h + 1], (n_bin, LANES))
    for x in range(halves):
        copies[("bins", x)].wait()

    slot_of = {d: OFFSETS.index(-d) for d in OFFSETS}
    for x in range(halves):
        for copy in halo[x]:
            copy.wait_recv()
        halo_rows(hw, x, recv0[x, 0].astype(F32), recv0[x, 1].astype(F32))
        along_y(hw, x, False)
        finish(0, x, send1)
    rest = [
        remote(send1, recv1.at[slot_of[d]], send_sem1.at[i], recv_sem1.at[i], d) for i, d in enumerate((2, -2, 1, -1))
    ]
    for copy in rest:
        copy.start()

    local_part(1)
    for copy in coefs:
        copy.wait_recv()
    final = []
    for x in range(halves):
        for copy in partial[x]:
            copy.wait_recv()
        border_rows(x)
        along_y(pw.at[1, :, :, inner], x, True)
        finish(1, x, send2)
        final.append(
            [
                remote(send2.at[x], recv2.at[slot_of[d], x], send_sem2.at[4 * x + i], recv_sem2.at[4 * x + i], d)
                for i, d in enumerate((2, -2, 1, -1))
            ]
        )
        for copy in final[x]:
            copy.start()

    for copy in rest:
        copy.wait_recv()
    for x in range(halves):
        for d in OFFSETS:
            open_block(0, x, d, recv1)
        image(0, x)

    for x in range(halves):
        for copy in final[x]:
            copy.wait_recv()
        for d in OFFSETS:
            open_block(1, x, d, recv2)
        image(1, x)

    for copy in sum([list(c) for c in halo + partial + final], []) + coefs + rest:
        copy.wait_send()


def per_device(
    source_now, source_before, receiver_now, receiver_before, speed_term, aniso_field, tilt_field,
    angle_bins, weight_table, offset_lags, source_cells, source_wavelet, receiver_cells, receiver_traces,
):
    zs, rows, width = source_now.shape
    halves = width // LANES
    steps = source_wavelet.shape[0]
    n_off, n_bin, n_ang = weight_table.shape
    n_src = source_cells.shape[0]
    receivers = receiver_cells.shape[0]
    assert rows == ROWS and n_bin == ROWS and width & (width - 1) == 0
    half = (halves, zs, ROWS, LANES)
    block = (halves, 2, zs, ROWS, LANES)
    any_space = pl.BlockSpec(memory_space=pl.ANY)
    dma = pltpu.SemaphoreType.DMA
    in_specs = [any_space] * 14
    return pl.pallas_call(
        kernel,
        out_shape=pltpu.VMEM((n_ang, zs, rows, width), BF16),
        in_specs=in_specs,
        out_specs=pl.BlockSpec(memory_space=pltpu.VMEM),
        scratch_shapes=[
            pltpu.VMEM((steps, 2, halves, zs + 2 * PAD, 3 * ROWS, LANES), F32),
            pltpu.VMEM((2,) + half, F32),
            pltpu.VMEM(half, F32),
            pltpu.VMEM(half, F32),
            pltpu.VMEM(half, F32),
            pltpu.VMEM(half, jnp.int32),
            pltpu.VMEM((n_bin, n_ang, n_off), BF16),
            pltpu.SMEM((n_off,), jnp.int32),
            pltpu.SMEM((n_src,), jnp.int32),
            pltpu.SMEM((steps, n_src), F32),
            pltpu.VMEM((receivers // LANES, LANES), jnp.int32),
            pltpu.VMEM((steps, receivers), F32),
            pltpu.VMEM((n_off, n_ang, n_bin, LANES), F32),
            pltpu.VMEM((n_off, n_ang) + half, F32),
            pltpu.VMEM((steps, 2, halves, ROWS, LANES), F32),
            pltpu.VMEM((2,) + half, F32),
            pltpu.VMEM((2, halves, zs + 2 * PAD, ROWS, LANES), F32),
            pltpu.VMEM((2, halves, zs, 3 * ROWS, LANES), F32),
            pltpu.VMEM((2,) + half, F32),
            pltpu.VMEM((2, halves, zs + 2 * PAD, ROWS, LANES), F32),
            pltpu.VMEM(block, BF16),
            pltpu.VMEM(block, BF16),
            pltpu.VMEM(block, BF16),
            pltpu.VMEM(block, BF16),
            pltpu.VMEM(block, BF16),
            pltpu.VMEM(block, BF16),
            pltpu.VMEM((2,) + half, BF16),
            pltpu.VMEM(block, BF16),
            pltpu.VMEM((len(OFFSETS),) + block, BF16),
            pltpu.VMEM((len(OFFSETS),) + block, BF16),
            pltpu.VMEM((steps, 2, halves, zs, 5 * ROWS, LANES), F32),
            pltpu.VMEM((n_ang,) + half, F32),
            dma((8 * halves + 6,)),
            dma((2 * halves,)),
            dma((2 * halves,)),
            dma((2,)),
            dma((2,)),
            dma((2 * halves,)),
            dma((2 * halves,)),
            dma((4,)),
            dma((4,)),
            dma((4 * halves,)),
            dma((4 * halves,)),
        ],
        compiler_params=pltpu.CompilerParams(collective_id=0, has_side_effects=True),
    )(
        source_now, source_before, receiver_now, receiver_before, speed_term, aniso_field, tilt_field,
        angle_bins, jnp.transpose(weight_table, (1, 2, 0)), offset_lags, source_cells, source_wavelet,
        receiver_cells.reshape(receivers // LANES, LANES), receiver_traces,
    )


def solution(mesh):
    return jax.shard_map(
        per_device,
        mesh=mesh,
        in_specs=(
            P("shot", "gy", None),
            P("shot", "gy", None),
            P("shot", "gy", None),
            P("shot", "gy", None),
            P(None, "gy", None),
            P(None, "gy", None),
            P(None, "gy", None),
            P(None, "gy", None),
            P(),
            P(),
            P("shot"),
            P("shot", None),
            P("shot"),
            P("shot", None),
        ),
        out_specs=P("shot", None, "gy", None),
        check_vma=False,
    )
```

```python
import functools

import jax
import jax.numpy as jnp
from jax import lax
from jax.experimental import pallas as pl
from jax.experimental.pallas import tpu as pltpu
from jax.sharding import PartitionSpec as P

SECOND_COEF = (-205.0 / 72.0, 8.0 / 5.0, -1.0 / 5.0, 8.0 / 315.0, -1.0 / 560.0)
FIRST_COEF = (4.0 / 5.0, -1.0 / 5.0, 4.0 / 105.0, -1.0 / 280.0)
MESH = pl.DeviceIdType.MESH
F32 = jnp.float32
BF16 = jnp.bfloat16
LANES = 128
ROWS = 8
PAD = 4
LO, HI = 0, 1
OFFSETS = (-2, -1, 1, 2)
PARTNER, OUTER, FAR, PASSED = range(4)
PIECES = 2


def kernel(
    sn_hbm, sb_hbm, rn_hbm, rb_hbm, speed_hbm, aniso_hbm, tilt_hbm, bins_hbm, wt_hbm,
    lags_hbm, scells_hbm, swave_hbm, rcells_hbm, rtraces_hbm,
    out,
    pw, qv, speed, a1, a2, bins, wt, lags, scells, swave, rcells, rtraces, table, cache, inj, base, grad,
    hw, share2, share1, send0, sendc, sendp, send1, send2, recv0, recvc, recvp, recv1, recv2, win, acc,
    in_sem, send_sem0, recv_sem0, send_semc, recv_semc, send_semp, recv_semp, send_sem1, recv_sem1, send_sem2, recv_sem2,
):
    n = lax.axis_size("gy")
    me = lax.axis_index("gy")
    peer = {d: lax.rem(me + (d + n), n) for d in OFFSETS}
    side_of = 1 - 2 * lax.rem(me, 2)
    target = {
        PARTNER: lax.rem(me + side_of + n, n),
        OUTER: lax.rem(me - side_of + n, n),
        FAR: lax.rem(me + 2 * side_of + n, n),
    }
    target[PASSED] = target[PARTNER]
    block_row = {
        PARTNER: (2 + side_of) * ROWS,
        OUTER: (2 - side_of) * ROWS,
        FAR: (2 - 2 * side_of) * ROWS,
        PASSED: (2 + 2 * side_of) * ROWS,
    }
    zs = sn_hbm.shape[0]
    halves = sn_hbm.shape[2] // LANES
    n_bin, n_ang, n_off = wt_hbm.shape
    steps = swave.shape[0]
    n_src = scells.shape[0]
    rec_rows = rcells_hbm.shape[0]
    own = pl.ds(ROWS, ROWS)
    inner = pl.ds(PAD, zs)

    barrier = pltpu.get_barrier_semaphore()
    for d in OFFSETS:
        pl.semaphore_signal(barrier, inc=1, device_id={"gy": peer[d]}, device_id_type=MESH)

    copies = {}

    def fetch(name, index, src, dst):
        copy = pltpu.make_async_copy(src, dst, in_sem.at[index])
        copy.start()
        copies[name] = copy

    wanted = [("rcells", rcells_hbm, rcells), ("rtraces", rtraces_hbm, rtraces)]
    wanted += [("scells", scells_hbm, scells), ("swave", swave_hbm, swave)]
    wanted += [
        (("now", m, x), ref.at[:, :, pl.ds(x * LANES, LANES)], pw.at[0, m, x, inner, own, :])
        for x in range(halves)
        for m, ref in enumerate((sn_hbm, rn_hbm))
    ]
    for name, ref, dst in (("speed", speed_hbm, speed), ("aniso", aniso_hbm, a1), ("tilt", tilt_hbm, a2)):
        wanted += [((name, x), ref.at[:, :, pl.ds(x * LANES, LANES)], dst.at[x]) for x in range(halves)]
    for m, ref in enumerate((sb_hbm, rb_hbm)):
        wanted += [(("before", m, x), ref.at[:, :, pl.ds(x * LANES, LANES)], qv.at[m, x]) for x in range(halves)]
    wanted += [(("bins", x), bins_hbm.at[:, :, pl.ds(x * LANES, LANES)], bins.at[x]) for x in range(halves)]
    wanted += [("wt", wt_hbm, wt), ("lags", lags_hbm, lags)]
    for index, (name, src, dst) in enumerate(wanted):
        fetch(name, index, src, dst)

    edge = jnp.zeros((PAD, ROWS, LANES), F32)
    plane = jnp.zeros((zs, ROWS, LANES), F32)
    for x in range(halves):
        for m in range(2):
            for s in range(steps):
                pw[s, m, x, pl.ds(0, PAD), own, :] = edge
                pw[s, m, x, pl.ds(PAD + zs, PAD), own, :] = edge
            pw[0, m, x, inner, pl.ds(0, ROWS), :] = plane
            pw[0, m, x, inner, pl.ds(2 * ROWS, ROWS), :] = plane
            hw[m, x, :, own, :] = plane
            for padded in (grad, share1):
                padded[m, x, pl.ds(0, PAD)] = edge
                padded[m, x, pl.ds(PAD + zs, PAD)] = edge

    sub = lax.broadcasted_iota(jnp.int32, (ROWS, LANES), 0)
    lane = lax.broadcasted_iota(jnp.int32, (ROWS, LANES), 1)
    low_rows = sub < PAD

    def turn(v):
        return pltpu.roll(v, PAD, axis=v.ndim - 2)

    def pack(source, receiver, send, x, where_z):
        send[x, LO, where_z] = jnp.where(low_rows, source, turn(receiver)).astype(BF16)
        send[x, HI, where_z] = jnp.where(low_rows, turn(source), receiver).astype(BF16)

    def remote(src, dst, ssem, rsem, device):
        return pltpu.make_async_remote_copy(
            src_ref=src, dst_ref=dst, send_sem=ssem, recv_sem=rsem, device_id={"gy": device}, device_id_type=MESH
        )

    shift_bits = (halves * LANES).bit_length() - 1

    def injections():
        first_row = me * ROWS
        for name in ("rcells", "rtraces", "scells", "swave"):
            copies[name].wait()
        left, right = [], []
        col_iota = lax.broadcasted_iota(jnp.int32, (halves * LANES, LANES), 0)
        for c in range(rec_rows):
            cell = rcells[c : c + 1, :]
            row = lax.shift_right_logical(cell, shift_bits) - first_row
            col = jnp.bitwise_and(cell, halves * LANES - 1)
            hit = jnp.broadcast_to(row, (ROWS, LANES)) == sub
            parts = []
            for s in range(steps):
                amount = jnp.broadcast_to(rtraces[s : s + 1, c * LANES : (c + 1) * LANES], (ROWS, LANES))
                amount = jnp.where(hit, amount, 0.0)
                coarse = amount.astype(BF16).astype(F32)
                parts += [coarse, amount - coarse]
            left.append(jnp.concatenate(parts, axis=0).astype(BF16))
            right.append(jnp.where(jnp.broadcast_to(col, col_iota.shape) == col_iota, 1.0, 0.0).astype(BF16))
        spread = lax.dot_general(
            jnp.concatenate(left, axis=1),
            jnp.concatenate(right, axis=1),
            (((1,), (1,)), ((), ())),
            preferred_element_type=F32,
        )
        for s in range(steps):
            total = spread[2 * s * ROWS : (2 * s + 1) * ROWS] + spread[(2 * s + 1) * ROWS : (2 * s + 2) * ROWS]
            for x in range(halves):
                inj[s, 1, x] = total[:, x * LANES : (x + 1) * LANES]
        for s in range(steps):
            for x in range(halves):
                total = jnp.zeros((ROWS, LANES), F32)
                for i in range(n_src):
                    cell = scells[i]
                    row = lax.shift_right_logical(cell, shift_bits) - first_row
                    col = jnp.bitwise_and(cell, halves * LANES - 1) - x * LANES
                    total = total + jnp.where((sub == row) & (lane == col), swave[s, i], 0.0)
                inj[s, 0, x] = total

    injections()

    halo = [
        (
            remote(send0.at[x, HI], recv0.at[x, 0], send_sem0.at[2 * x], recv_sem0.at[2 * x], peer[1]),
            remote(send0.at[x, LO], recv0.at[x, 1], send_sem0.at[2 * x + 1], recv_sem0.at[2 * x + 1], peer[-1]),
        )
        for x in range(halves)
    ]
    for x in range(halves):
        for m in range(2):
            copies[("now", m, x)].wait()
        pack(pw[0, 0, x, inner, own, :], pw[0, 1, x, inner, own, :], send0, x, pl.ds(0, zs))
        if x == 0:
            pl.semaphore_wait(barrier, len(OFFSETS))
        for copy in halo[x]:
            copy.start()

    def local_part(step):
        chunk = 4

        def part(i, carry):
            z = i * chunk
            for m in range(2):
                f = [pw[step, m, x, pl.ds(PAD + z, chunk), own, :] for x in range(halves)]
                first = [jnp.zeros_like(v) for v in f]
                second = [SECOND_COEF[0] * v for v in f]
                for k in range(1, PAD + 1):
                    up = [pltpu.roll(v, LANES - k, axis=2) for v in f] + [jnp.zeros_like(f[0])]
                    down = [jnp.zeros_like(f[0])] + [pltpu.roll(v, k, axis=2) for v in f]
                    for x in range(halves):
                        above = jnp.where(lane < LANES - k, up[x], up[x + 1])
                        below = jnp.where(lane >= k, down[x + 1], down[x])
                        second[x] = second[x] + SECOND_COEF[k] * (above + below)
                        first[x] = first[x] + FIRST_COEF[k - 1] * (above - below)
                for x in range(halves):
                    grad[m, x, pl.ds(PAD + z, chunk)] = first[x]
                    along_z = SECOND_COEF[0] * f[x]
                    for k in range(1, PAD + 1):
                        along_z = along_z + SECOND_COEF[k] * (
                            pw[step, m, x, pl.ds(PAD + z + k, chunk), own, :]
                            + pw[step, m, x, pl.ds(PAD + z - k, chunk), own, :]
                        )
                    before = qv[m, x, pl.ds(z, chunk)] if step == 0 else pw[step - 1, m, x, pl.ds(PAD + z, chunk), own, :]
                    base[m, x, pl.ds(z, chunk)] = (
                        2.0 * f[x]
                        - before
                        + a1[x, pl.ds(z, chunk)] * second[x]
                        + speed[x, pl.ds(z, chunk)] * along_z
                    )
            return carry

        lax.fori_loop(0, zs // chunk, part, 0)
        for m in range(2):
            for x in range(halves):
                base[m, x, 0] = base[m, x, 0] + inj[step, m, x]

    def halo_rows(window, x, low, high):
        window[0, x, :, pl.ds(0, ROWS), :] = turn(low)
        window[1, x, :, pl.ds(0, ROWS), :] = low
        window[0, x, :, pl.ds(2 * ROWS, ROWS), :] = high
        window[1, x, :, pl.ds(2 * ROWS, ROWS), :] = turn(high)

    part_chunk = 4

    def along_y(window, x, whole):
        def part(i, carry):
            z = i * part_chunk
            cells = pl.ds(z, part_chunk)
            for m in range(2):

                def rows(k):
                    return window[m, x, cells, pl.ds(ROWS + k, ROWS), :]

                second, first = 0.0, 0.0
                if whole:
                    second, first = SECOND_COEF[0] * rows(0), grad[m, x, pl.ds(PAD + z, part_chunk)]
                for k in range(1, PAD + 1):
                    above, below = rows(k), rows(-k)
                    second = second + SECOND_COEF[k] * (above + below)
                    first = first + FIRST_COEF[k - 1] * (above - below)
                grad[m, x, pl.ds(PAD + z, part_chunk)] = first
                base[m, x, cells] = base[m, x, cells] + a1[x, cells] * second
            return carry

        lax.fori_loop(0, zs // part_chunk, part, 0)

    def along_z(padded, member, x, z):
        mixed = jnp.zeros((part_chunk, ROWS, LANES), F32)
        for k in range(1, PAD + 1):
            mixed = mixed + FIRST_COEF[k - 1] * (
                padded[member, x, pl.ds(PAD + z + k, part_chunk)] - padded[member, x, pl.ds(PAD + z - k, part_chunk)]
            )
        return mixed

    def finish(step, x, send, whole=True):
        def part(i, carry):
            z = i * part_chunk
            cells = pl.ds(z, part_chunk)
            new = []
            for m in range(2):
                value = base[m, x, cells] + a2[x, cells] * along_z(grad, m, x, z)
                new.append(value)
                if not whole:
                    base[m, x, cells] = value
                    continue
                if step + 1 < steps:
                    pw[step + 1, m, x, pl.ds(PAD + z, part_chunk), own, :] = value
                win[step, m, x, cells, pl.ds(2 * ROWS, ROWS), :] = value.astype(BF16).astype(F32)
            pack(new[0], new[1], send, x, cells)
            return carry

        lax.fori_loop(0, zs // part_chunk, part, 0)

    def shares(x):
        def part(i, carry):
            z = i * part_chunk
            for side in range(2):
                second, first = [], []
                for m in range(2):
                    two, one = 0.0, 0.0
                    for k in range(1, PAD + 1):
                        row = ROWS - PAD + k if side == 0 else 2 * ROWS - k
                        value = pw[0, m, x, pl.ds(PAD + z, part_chunk), pl.ds(row, ROWS), :]
                        two = two + SECOND_COEF[k] * value
                        one = one + (FIRST_COEF[k - 1] if side == 0 else -FIRST_COEF[k - 1]) * value
                    second.append(two)
                    first.append(one)
                share2[side, x, pl.ds(z, part_chunk)] = jnp.where(low_rows, second[0], turn(second[1]))
                share1[side, x, pl.ds(PAD + z, part_chunk)] = jnp.where(low_rows, first[0], turn(first[1]))
            return carry

        lax.fori_loop(0, zs // part_chunk, part, 0)

    def border_rows(x):
        whole = []
        for side in range(2):
            blocks = []
            for z in range(0, zs, part_chunk):
                cells = pl.ds(z, part_chunk)
                pair = recvc[side, x, cells].astype(F32)
                flat, tilted = jnp.where(low_rows, pair, turn(pair)), jnp.where(low_rows, turn(pair), pair)
                blocks.append(
                    recvp[x, side, cells].astype(F32)
                    + flat * share2[side, x, cells]
                    + tilted * along_z(share1, side, x, z)
                )
            whole.append(jnp.concatenate(blocks, axis=0))
        halo_rows(pw.at[1, :, :, inner], x, whole[0], whole[1])

    def open_block(step, role, recv, x, z, length):
        cells = pl.ds(z, length)
        rows = pl.ds(pl.multiple_of(block_row[role], ROWS), ROWS)
        low = recv[role, x, LO, cells].astype(F32)
        high = recv[role, x, HI, cells].astype(F32)
        win[step, 0, x, cells, rows, :] = jnp.where(low_rows, low, turn(high))
        win[step, 1, x, cells, rows, :] = jnp.where(low_rows, turn(low), high)

    chunk = 4

    def image(step, x, start, length):
        def part(i, carry):
            z = start + i * chunk
            if step == 0:
                bin_ids = [bins[x, z + j] for j in range(chunk)]
                total = [jnp.zeros((chunk, ROWS, LANES), F32)] * n_ang
            else:
                total = [acc[a, x, pl.ds(z, chunk)] for a in range(n_ang)]
            for h in range(n_off):
                lag = lags[h]
                product = (
                    win[step, 0, x, pl.ds(z, chunk), pl.ds(2 * ROWS - lag, ROWS), :]
                    * win[step, 1, x, pl.ds(z, chunk), pl.ds(2 * ROWS + lag, ROWS), :]
                )
                for a in range(n_ang):
                    if step == 0:
                        row = table[h, a]
                        weight = jnp.stack([jnp.take_along_axis(row, bin_ids[j], axis=0) for j in range(chunk)])
                        cache[h, a, x, pl.ds(z, chunk)] = weight
                    else:
                        weight = cache[h, a, x, pl.ds(z, chunk)]
                    total[a] = total[a] + weight * product
            for a in range(n_ang):
                if step + 1 == steps:
                    out[a, pl.ds(z, chunk), :, x * LANES : (x + 1) * LANES] = total[a].astype(BF16)
                else:
                    acc[a, x, pl.ds(z, chunk)] = total[a]
            return carry

        lax.fori_loop(0, length // chunk, part, 0)

    for x in range(halves):
        copies[("speed", x)].wait()
        copies[("aniso", x)].wait()
        copies[("tilt", x)].wait()
        a1[x] = speed[x] * (1.0 + 2.0 * a1[x])
        a2[x] = speed[x] * a2[x]
        pack(a1[x], a2[x], sendc, x, pl.ds(0, zs))
    coefs = [
        remote(sendc.at[:, half], recvc.at[i], send_semc.at[i], recv_semc.at[i], peer[d])
        for i, (half, d) in enumerate(((HI, 1), (LO, -1)))
    ]
    for copy in coefs:
        copy.start()
    for m in range(2):
        for x in range(halves):
            copies[("before", m, x)].wait()
    local_part(0)
    partial = []
    for x in range(halves):
        along_y(pw.at[0, :, :, inner], x, True)
        finish(0, x, sendp, whole=False)
        partial.append(
            [
                remote(sendp.at[x, half], recvp.at[x, i], send_semp.at[2 * x + i], recv_semp.at[2 * x + i], peer[d])
                for i, (half, d) in enumerate(((HI, 1), (LO, -1)))
            ]
        )
        for copy in partial[x]:
            copy.start()
    for x in range(halves):
        shares(x)
    copies["wt"].wait()
    copies["lags"].wait()
    by_bin = [wt[b].astype(F32) for b in range(n_bin)]
    for a in range(n_ang):
        rows = jnp.concatenate([v[a : a + 1] for v in by_bin], axis=0)
        for h in range(n_off):
            table[h, a] = jnp.broadcast_to(rows[:, h : h + 1], (n_bin, LANES))
    for x in range(halves):
        copies[("bins", x)].wait()

    for x in range(halves):
        for copy in halo[x]:
            copy.wait_recv()
        halo_rows(hw, x, recv0[x, 0].astype(F32), recv0[x, 1].astype(F32))
        along_y(hw, x, False)
        finish(0, x, send1)
    first = {
        role: remote(
            recv1.at[OUTER] if role == PASSED else send1,
            recv1.at[role],
            send_sem1.at[role],
            recv_sem1.at[role],
            target[role],
        )
        for role in target
    }
    for role in (FAR, OUTER, PARTNER):
        first[role].start()

    local_part(1)
    for copy in coefs:
        copy.wait_recv()
    length = zs // PIECES
    pieces = [(x, p * length) for x in range(halves) for p in range(PIECES)]
    final = []
    for index, (x, z) in enumerate(pieces):
        cells = (x, slice(None), pl.ds(z, length))
        final.append(
            {
                role: remote(
                    recv2.at[(OUTER,) + cells] if role == PASSED else send2.at[cells],
                    recv2.at[(role,) + cells],
                    send_sem2.at[4 * index + role],
                    recv_sem2.at[4 * index + role],
                    target[role],
                )
                for role in target
            }
        )
    for x in range(halves):
        for copy in partial[x]:
            copy.wait_recv()
        border_rows(x)
        along_y(pw.at[1, :, :, inner], x, True)
        finish(1, x, send2)
        for index, (x_of, z) in enumerate(pieces):
            if x_of == x:
                for role in (FAR, OUTER, PARTNER):
                    final[index][role].start()

    first[OUTER].wait_recv()
    first[PASSED].start()
    for role in (OUTER, PARTNER, FAR, PASSED):
        if role != OUTER:
            first[role].wait_recv()
        for x in range(halves):
            open_block(0, role, recv1, x, 0, zs)
    for x in range(halves):
        image(0, x, 0, zs)

    def last_image(index):
        x, z = pieces[index]
        final[index][PASSED].wait_recv()
        open_block(1, PASSED, recv2, x, z, length)
        image(1, x, z, length)

    for index, (x, z) in enumerate(pieces):
        final[index][OUTER].wait_recv()
        final[index][PASSED].start()
        for role in (OUTER, PARTNER, FAR):
            if role != OUTER:
                final[index][role].wait_recv()
            open_block(1, role, recv2, x, z, length)
        if index:
            last_image(index - 1)
    last_image(len(pieces) - 1)

    sent = coefs + list(first.values()) + sum([list(c) for c in halo + partial], [])
    for copy in sent + sum([list(c.values()) for c in final], []):
        copy.wait_send()


def per_device(
    source_now, source_before, receiver_now, receiver_before, speed_term, aniso_field, tilt_field,
    angle_bins, weight_table, offset_lags, source_cells, source_wavelet, receiver_cells, receiver_traces,
):
    zs, rows, width = source_now.shape
    halves = width // LANES
    steps = source_wavelet.shape[0]
    n_off, n_bin, n_ang = weight_table.shape
    n_src = source_cells.shape[0]
    receivers = receiver_cells.shape[0]
    assert rows == ROWS and n_bin == ROWS and width & (width - 1) == 0
    half = (halves, zs, ROWS, LANES)
    block = (halves, 2, zs, ROWS, LANES)
    any_space = pl.BlockSpec(memory_space=pl.ANY)
    dma = pltpu.SemaphoreType.DMA
    in_specs = [any_space] * 14
    return pl.pallas_call(
        kernel,
        out_shape=pltpu.VMEM((n_ang, zs, rows, width), BF16),
        in_specs=in_specs,
        out_specs=pl.BlockSpec(memory_space=pltpu.VMEM),
        scratch_shapes=[
            pltpu.VMEM((steps, 2, halves, zs + 2 * PAD, 3 * ROWS, LANES), F32),
            pltpu.VMEM((2,) + half, F32),
            pltpu.VMEM(half, F32),
            pltpu.VMEM(half, F32),
            pltpu.VMEM(half, F32),
            pltpu.VMEM(half, jnp.int32),
            pltpu.VMEM((n_bin, n_ang, n_off), BF16),
            pltpu.SMEM((n_off,), jnp.int32),
            pltpu.SMEM((n_src,), jnp.int32),
            pltpu.SMEM((steps, n_src), F32),
            pltpu.VMEM((receivers // LANES, LANES), jnp.int32),
            pltpu.VMEM((steps, receivers), F32),
            pltpu.VMEM((n_off, n_ang, n_bin, LANES), F32),
            pltpu.VMEM((n_off, n_ang) + half, F32),
            pltpu.VMEM((steps, 2, halves, ROWS, LANES), F32),
            pltpu.VMEM((2,) + half, F32),
            pltpu.VMEM((2, halves, zs + 2 * PAD, ROWS, LANES), F32),
            pltpu.VMEM((2, halves, zs, 3 * ROWS, LANES), F32),
            pltpu.VMEM((2,) + half, F32),
            pltpu.VMEM((2, halves, zs + 2 * PAD, ROWS, LANES), F32),
            pltpu.VMEM(block, BF16),
            pltpu.VMEM(block, BF16),
            pltpu.VMEM(block, BF16),
            pltpu.VMEM(block, BF16),
            pltpu.VMEM(block, BF16),
            pltpu.VMEM(block, BF16),
            pltpu.VMEM((2,) + half, BF16),
            pltpu.VMEM(block, BF16),
            pltpu.VMEM((4,) + block, BF16),
            pltpu.VMEM((4,) + block, BF16),
            pltpu.VMEM((steps, 2, halves, zs, 5 * ROWS, LANES), F32),
            pltpu.VMEM((n_ang,) + half, F32),
            dma((8 * halves + 6,)),
            dma((2 * halves,)),
            dma((2 * halves,)),
            dma((2,)),
            dma((2,)),
            dma((2 * halves,)),
            dma((2 * halves,)),
            dma((4,)),
            dma((4,)),
            dma((4 * halves * PIECES,)),
            dma((4 * halves * PIECES,)),
        ],
        compiler_params=pltpu.CompilerParams(collective_id=0, has_side_effects=True),
    )(
        source_now, source_before, receiver_now, receiver_before, speed_term, aniso_field, tilt_field,
        angle_bins, jnp.transpose(weight_table, (1, 2, 0)), offset_lags, source_cells, source_wavelet,
        receiver_cells.reshape(receivers // LANES, LANES), receiver_traces,
    )


def solution(mesh):
    return jax.shard_map(
        per_device,
        mesh=mesh,
        in_specs=(
            P("shot", "gy", None),
            P("shot", "gy", None),
            P("shot", "gy", None),
            P("shot", "gy", None),
            P(None, "gy", None),
            P(None, "gy", None),
            P(None, "gy", None),
            P(None, "gy", None),
            P(),
            P(),
            P("shot"),
            P("shot", None),
            P("shot"),
            P("shot", None),
        ),
        out_specs=P("shot", None, "gy", None),
        check_vma=False,
    )
```

```python
import functools

import jax
import jax.numpy as jnp
from jax import lax
from jax.experimental import pallas as pl
from jax.experimental.pallas import tpu as pltpu
from jax.sharding import PartitionSpec as P

SECOND_COEF = (-205.0 / 72.0, 8.0 / 5.0, -1.0 / 5.0, 8.0 / 315.0, -1.0 / 560.0)
FIRST_COEF = (4.0 / 5.0, -1.0 / 5.0, 4.0 / 105.0, -1.0 / 280.0)
MESH = pl.DeviceIdType.MESH
F32 = jnp.float32
BF16 = jnp.bfloat16
LANES = 128
ROWS = 8
PAD = 4
LO, HI = 0, 1
OFFSETS = (-2, -1, 1, 2)
DIRECT = ((2, -1, 1), (2, -2, -1))
PASSED = ((1, 2), (-2, -1))
PIECES = 2


def kernel(
    sn_hbm, sb_hbm, rn_hbm, rb_hbm, speed_hbm, aniso_hbm, tilt_hbm, bins_hbm, wt_hbm,
    lags_hbm, scells_hbm, swave_hbm, rcells_hbm, rtraces_hbm,
    out,
    pw, qv, speed, a1, a2, bins, wt, lags, scells, swave, rcells, rtraces, table, cache, inj, base, grad,
    hw, share2, share1, send0, sendc, sendp, send1, send2, recv0, recvc, recvp, recv1, recv2, win, acc,
    in_sem, send_sem0, recv_sem0, send_semc, recv_semc, send_semp, recv_semp, send_sem1, recv_sem1, send_sem2, recv_sem2,
):
    n = lax.axis_size("gy")
    me = lax.axis_index("gy")
    peer = {d: lax.rem(me + (d + n), n) for d in OFFSETS}
    odd = lax.rem(me, 2) == 1
    zs = sn_hbm.shape[0]
    halves = sn_hbm.shape[2] // LANES
    n_bin, n_ang, n_off = wt_hbm.shape
    steps = swave.shape[0]
    n_src = scells.shape[0]
    rec_rows = rcells_hbm.shape[0]
    own = pl.ds(ROWS, ROWS)
    inner = pl.ds(PAD, zs)

    barrier = pltpu.get_barrier_semaphore()
    for d in OFFSETS:
        pl.semaphore_signal(barrier, inc=1, device_id={"gy": peer[d]}, device_id_type=MESH)

    copies = {}

    def fetch(name, index, src, dst):
        copy = pltpu.make_async_copy(src, dst, in_sem.at[index])
        copy.start()
        copies[name] = copy

    wanted = [
        (("now", m, x), ref.at[:, :, pl.ds(x * LANES, LANES)], pw.at[0, m, x, inner, own, :])
        for x in range(halves)
        for m, ref in enumerate((sn_hbm, rn_hbm))
    ]
    wanted += [("rcells", rcells_hbm, rcells), ("rtraces", rtraces_hbm, rtraces)]
    wanted += [("scells", scells_hbm, scells), ("swave", swave_hbm, swave)]
    for name, ref, dst in (("speed", speed_hbm, speed), ("aniso", aniso_hbm, a1), ("tilt", tilt_hbm, a2)):
        wanted += [((name, x), ref.at[:, :, pl.ds(x * LANES, LANES)], dst.at[x]) for x in range(halves)]
    for m, ref in enumerate((sb_hbm, rb_hbm)):
        wanted += [(("before", m, x), ref.at[:, :, pl.ds(x * LANES, LANES)], qv.at[m, x]) for x in range(halves)]
    wanted += [(("bins", x), bins_hbm.at[:, :, pl.ds(x * LANES, LANES)], bins.at[x]) for x in range(halves)]
    wanted += [("wt", wt_hbm, wt), ("lags", lags_hbm, lags)]
    for index, (name, src, dst) in enumerate(wanted):
        fetch(name, index, src, dst)

    edge = jnp.zeros((PAD, ROWS, LANES), F32)
    plane = jnp.zeros((zs, ROWS, LANES), F32)
    for x in range(halves):
        for m in range(2):
            for s in range(steps):
                pw[s, m, x, pl.ds(0, PAD), own, :] = edge
                pw[s, m, x, pl.ds(PAD + zs, PAD), own, :] = edge
            pw[0, m, x, inner, pl.ds(0, ROWS), :] = plane
            pw[0, m, x, inner, pl.ds(2 * ROWS, ROWS), :] = plane
            hw[m, x, :, own, :] = plane
            for padded in (grad, share1):
                padded[m, x, pl.ds(0, PAD)] = edge
                padded[m, x, pl.ds(PAD + zs, PAD)] = edge

    sub = lax.broadcasted_iota(jnp.int32, (ROWS, LANES), 0)
    lane = lax.broadcasted_iota(jnp.int32, (ROWS, LANES), 1)
    low_rows = sub < PAD

    def turn(v):
        return pltpu.roll(v, PAD, axis=v.ndim - 2)

    def pack(source, receiver, send, x, where_z):
        send[x, LO, where_z] = jnp.where(low_rows, source, turn(receiver)).astype(BF16)
        send[x, HI, where_z] = jnp.where(low_rows, turn(source), receiver).astype(BF16)

    def remote(src, dst, ssem, rsem, device):
        return pltpu.make_async_remote_copy(
            src_ref=src, dst_ref=dst, send_sem=ssem, recv_sem=rsem, device_id={"gy": device}, device_id_type=MESH
        )

    shift_bits = (halves * LANES).bit_length() - 1

    def injections():
        first_row = me * ROWS
        for name in ("rcells", "rtraces", "scells", "swave"):
            copies[name].wait()
        left, right = [], []
        col_iota = lax.broadcasted_iota(jnp.int32, (halves * LANES, LANES), 0)
        for c in range(rec_rows):
            cell = rcells[c : c + 1, :]
            row = lax.shift_right_logical(cell, shift_bits) - first_row
            col = jnp.bitwise_and(cell, halves * LANES - 1)
            hit = jnp.broadcast_to(row, (ROWS, LANES)) == sub
            parts = []
            for s in range(steps):
                amount = jnp.broadcast_to(rtraces[s : s + 1, c * LANES : (c + 1) * LANES], (ROWS, LANES))
                amount = jnp.where(hit, amount, 0.0)
                coarse = amount.astype(BF16).astype(F32)
                parts += [coarse, amount - coarse]
            left.append(jnp.concatenate(parts, axis=0).astype(BF16))
            right.append(jnp.where(jnp.broadcast_to(col, col_iota.shape) == col_iota, 1.0, 0.0).astype(BF16))
        spread = lax.dot_general(
            jnp.concatenate(left, axis=1),
            jnp.concatenate(right, axis=1),
            (((1,), (1,)), ((), ())),
            preferred_element_type=F32,
        )
        for s in range(steps):
            total = spread[2 * s * ROWS : (2 * s + 1) * ROWS] + spread[(2 * s + 1) * ROWS : (2 * s + 2) * ROWS]
            for x in range(halves):
                inj[s, 1, x] = total[:, x * LANES : (x + 1) * LANES]
        for s in range(steps):
            for x in range(halves):
                total = jnp.zeros((ROWS, LANES), F32)
                for i in range(n_src):
                    cell = scells[i]
                    row = lax.shift_right_logical(cell, shift_bits) - first_row
                    col = jnp.bitwise_and(cell, halves * LANES - 1) - x * LANES
                    total = total + jnp.where((sub == row) & (lane == col), swave[s, i], 0.0)
                inj[s, 0, x] = total

    halo = [
        (
            remote(send0.at[x, HI], recv0.at[x, 0], send_sem0.at[2 * x], recv_sem0.at[2 * x], peer[1]),
            remote(send0.at[x, LO], recv0.at[x, 1], send_sem0.at[2 * x + 1], recv_sem0.at[2 * x + 1], peer[-1]),
        )
        for x in range(halves)
    ]
    for x in range(halves):
        for m in range(2):
            copies[("now", m, x)].wait()
        pack(pw[0, 0, x, inner, own, :], pw[0, 1, x, inner, own, :], send0, x, pl.ds(0, zs))
        if x == 0:
            pl.semaphore_wait(barrier, len(OFFSETS))
        for copy in halo[x]:
            copy.start()

    def local_part(step):
        chunk = 4

        def part(i, carry):
            z = i * chunk
            for m in range(2):
                f = [pw[step, m, x, pl.ds(PAD + z, chunk), own, :] for x in range(halves)]
                first = [jnp.zeros_like(v) for v in f]
                second = [SECOND_COEF[0] * v for v in f]
                for k in range(1, PAD + 1):
                    up = [pltpu.roll(v, LANES - k, axis=2) for v in f] + [jnp.zeros_like(f[0])]
                    down = [jnp.zeros_like(f[0])] + [pltpu.roll(v, k, axis=2) for v in f]
                    for x in range(halves):
                        above = jnp.where(lane < LANES - k, up[x], up[x + 1])
                        below = jnp.where(lane >= k, down[x + 1], down[x])
                        second[x] = second[x] + SECOND_COEF[k] * (above + below)
                        first[x] = first[x] + FIRST_COEF[k - 1] * (above - below)
                for x in range(halves):
                    grad[m, x, pl.ds(PAD + z, chunk)] = first[x]
                    along_z = SECOND_COEF[0] * f[x]
                    for k in range(1, PAD + 1):
                        along_z = along_z + SECOND_COEF[k] * (
                            pw[step, m, x, pl.ds(PAD + z + k, chunk), own, :]
                            + pw[step, m, x, pl.ds(PAD + z - k, chunk), own, :]
                        )
                    before = qv[m, x, pl.ds(z, chunk)] if step == 0 else pw[step - 1, m, x, pl.ds(PAD + z, chunk), own, :]
                    base[m, x, pl.ds(z, chunk)] = (
                        2.0 * f[x]
                        - before
                        + a1[x, pl.ds(z, chunk)] * second[x]
                        + speed[x, pl.ds(z, chunk)] * along_z
                    )
            return carry

        lax.fori_loop(0, zs // chunk, part, 0)
        for m in range(2):
            for x in range(halves):
                base[m, x, 0] = base[m, x, 0] + inj[step, m, x]

    def halo_rows(window, x, low, high):
        window[0, x, :, pl.ds(0, ROWS), :] = turn(low)
        window[1, x, :, pl.ds(0, ROWS), :] = low
        window[0, x, :, pl.ds(2 * ROWS, ROWS), :] = high
        window[1, x, :, pl.ds(2 * ROWS, ROWS), :] = turn(high)

    part_chunk = 4

    def along_y(window, x, whole):
        def part(i, carry):
            z = i * part_chunk
            cells = pl.ds(z, part_chunk)
            for m in range(2):

                def rows(k):
                    return window[m, x, cells, pl.ds(ROWS + k, ROWS), :]

                second, first = 0.0, 0.0
                if whole:
                    second, first = SECOND_COEF[0] * rows(0), grad[m, x, pl.ds(PAD + z, part_chunk)]
                for k in range(1, PAD + 1):
                    above, below = rows(k), rows(-k)
                    second = second + SECOND_COEF[k] * (above + below)
                    first = first + FIRST_COEF[k - 1] * (above - below)
                grad[m, x, pl.ds(PAD + z, part_chunk)] = first
                base[m, x, cells] = base[m, x, cells] + a1[x, cells] * second
            return carry

        lax.fori_loop(0, zs // part_chunk, part, 0)

    def along_z(padded, member, x, z):
        mixed = jnp.zeros((part_chunk, ROWS, LANES), F32)
        for k in range(1, PAD + 1):
            mixed = mixed + FIRST_COEF[k - 1] * (
                padded[member, x, pl.ds(PAD + z + k, part_chunk)] - padded[member, x, pl.ds(PAD + z - k, part_chunk)]
            )
        return mixed

    def finish(step, x, send, whole=True):
        def part(i, carry):
            z = i * part_chunk
            cells = pl.ds(z, part_chunk)
            new = []
            for m in range(2):
                value = base[m, x, cells] + a2[x, cells] * along_z(grad, m, x, z)
                new.append(value)
                if not whole:
                    base[m, x, cells] = value
                    continue
                if step + 1 < steps:
                    pw[step + 1, m, x, pl.ds(PAD + z, part_chunk), own, :] = value
                win[step, m, x, cells, pl.ds(2 * ROWS, ROWS), :] = value.astype(BF16).astype(F32)
            pack(new[0], new[1], send, x, cells)
            return carry

        lax.fori_loop(0, zs // part_chunk, part, 0)

    def shares(x):
        def part(i, carry):
            z = i * part_chunk
            for side in range(2):
                second, first = [], []
                for m in range(2):
                    two, one = 0.0, 0.0
                    for k in range(1, PAD + 1):
                        row = ROWS - PAD + k if side == 0 else 2 * ROWS - k
                        value = pw[0, m, x, pl.ds(PAD + z, part_chunk), pl.ds(row, ROWS), :]
                        two = two + SECOND_COEF[k] * value
                        one = one + (FIRST_COEF[k - 1] if side == 0 else -FIRST_COEF[k - 1]) * value
                    second.append(two)
                    first.append(one)
                share2[side, x, pl.ds(z, part_chunk)] = jnp.where(low_rows, second[0], turn(second[1]))
                share1[side, x, pl.ds(PAD + z, part_chunk)] = jnp.where(low_rows, first[0], turn(first[1]))
            return carry

        lax.fori_loop(0, zs // part_chunk, part, 0)

    def border_rows(x):
        whole = []
        for side in range(2):
            blocks = []
            for z in range(0, zs, part_chunk):
                cells = pl.ds(z, part_chunk)
                pair = recvc[side, x, cells].astype(F32)
                flat, tilted = jnp.where(low_rows, pair, turn(pair)), jnp.where(low_rows, turn(pair), pair)
                blocks.append(
                    recvp[x, side, cells].astype(F32)
                    + flat * share2[side, x, cells]
                    + tilted * along_z(share1, side, x, z)
                )
            whole.append(jnp.concatenate(blocks, axis=0))
        halo_rows(pw.at[1, :, :, inner], x, whole[0], whole[1])

    def open_block(step, d, recv, x, z, length):
        cells = pl.ds(z, length)
        rows = pl.ds((2 + d) * ROWS, ROWS)
        slot = OFFSETS.index(d)
        low = recv[slot, x, LO, cells].astype(F32)
        high = recv[slot, x, HI, cells].astype(F32)
        win[step, 0, x, cells, rows, :] = jnp.where(low_rows, low, turn(high))
        win[step, 1, x, cells, rows, :] = jnp.where(low_rows, turn(low), high)

    chunk = 4

    def image(step, x, start, length):
        def part(i, carry):
            z = start + i * chunk
            if step == 0:
                bin_ids = [bins[x, z + j] for j in range(chunk)]
                total = [jnp.zeros((chunk, ROWS, LANES), F32)] * n_ang
            else:
                total = [acc[a, x, pl.ds(z, chunk)] for a in range(n_ang)]
            for h in range(n_off):
                lag = lags[h]
                product = (
                    win[step, 0, x, pl.ds(z, chunk), pl.ds(2 * ROWS - lag, ROWS), :]
                    * win[step, 1, x, pl.ds(z, chunk), pl.ds(2 * ROWS + lag, ROWS), :]
                )
                for a in range(n_ang):
                    if step == 0:
                        row = table[h, a]
                        weight = jnp.stack([jnp.take_along_axis(row, bin_ids[j], axis=0) for j in range(chunk)])
                        cache[h, a, x, pl.ds(z, chunk)] = weight
                    else:
                        weight = cache[h, a, x, pl.ds(z, chunk)]
                    total[a] = total[a] + weight * product
            for a in range(n_ang):
                if step + 1 == steps:
                    out[a, pl.ds(z, chunk), :, x * LANES : (x + 1) * LANES] = total[a].astype(BF16)
                else:
                    acc[a, x, pl.ds(z, chunk)] = total[a]
            return carry

        lax.fori_loop(0, length // chunk, part, 0)

    injections()
    for x in range(halves):
        copies[("speed", x)].wait()
        copies[("aniso", x)].wait()
        copies[("tilt", x)].wait()
        a1[x] = speed[x] * (1.0 + 2.0 * a1[x])
        a2[x] = speed[x] * a2[x]
        pack(a1[x], a2[x], sendc, x, pl.ds(0, zs))
    coefs = [
        remote(sendc.at[:, half], recvc.at[i], send_semc.at[i], recv_semc.at[i], peer[d])
        for i, (half, d) in enumerate(((HI, 1), (LO, -1)))
    ]
    for copy in coefs:
        copy.start()
    for m in range(2):
        for x in range(halves):
            copies[("before", m, x)].wait()
    local_part(0)
    partial = []
    for x in range(halves):
        along_y(pw.at[0, :, :, inner], x, True)
        finish(0, x, sendp, whole=False)
        partial.append(
            [
                remote(sendp.at[x, half], recvp.at[x, i], send_semp.at[2 * x + i], recv_semp.at[2 * x + i], peer[d])
                for i, (half, d) in enumerate(((HI, 1), (LO, -1)))
            ]
        )
        for copy in partial[x]:
            copy.start()
    for x in range(halves):
        shares(x)
    copies["wt"].wait()
    copies["lags"].wait()
    by_bin = [wt[b].astype(F32) for b in range(n_bin)]
    for a in range(n_ang):
        rows = jnp.concatenate([v[a : a + 1] for v in by_bin], axis=0)
        for h in range(n_off):
            table[h, a] = jnp.broadcast_to(rows[:, h : h + 1], (n_bin, LANES))
    for x in range(halves):
        copies[("bins", x)].wait()

    for x in range(halves):
        for copy in halo[x]:
            copy.wait_recv()
        halo_rows(hw, x, recv0[x, 0].astype(F32), recv0[x, 1].astype(F32))
        along_y(hw, x, False)
        finish(0, x, send1)
    def direct(send, recv, send_sems, recv_sems, cells):
        for parity, here in enumerate((jnp.logical_not(odd), odd)):

            @pl.when(here)
            def _():
                for i, d in enumerate(DIRECT[parity]):
                    slot = OFFSETS.index(-d)
                    remote(send.at[cells], recv.at[(slot,) + cells], send_sems[i], recv_sems[slot], peer[d]).start()

    def passed(recv, send_sems, recv_sems, cells, index):
        here, there = (OFFSETS.index(d) for d in PASSED[index])
        return remote(recv.at[(here,) + cells], recv.at[(there,) + cells], send_sems[index], recv_sems[there], peer[-1])

    def collect(step, recv, send_sems, recv_sems, cells, x_list, z, length):
        for d in (1, -2, -1, 2):
            slot = OFFSETS.index(d)
            remote(recv.at[(slot,) + cells], recv.at[(slot,) + cells], send_sems[0], recv_sems[slot], peer[1]).wait_recv()
            for index, (source, _) in enumerate(PASSED):
                if source == d:

                    @pl.when(odd)
                    def _():
                        passed(recv, send_sems[3:], recv_sems, cells, index).start()

        for d in OFFSETS:
            for x in x_list:
                open_block(step, d, recv, x, z, length)

    def sent(send, recv, send_sems, recv_sems, cells):
        for i in range(3):
            remote(send.at[cells], recv.at[(0,) + cells], send_sems[i], recv_sems[0], peer[1]).wait_send()

        @pl.when(odd)
        def _():
            for index in range(len(PASSED)):
                passed(recv, send_sems[3:], recv_sems, cells, index).wait_send()

    everything = (pl.ds(0, halves),)
    first_sems = [send_sem1.at[i] for i in range(5)], [recv_sem1.at[i] for i in range(4)]
    direct(send1, recv1, *first_sems, everything)

    local_part(1)
    for copy in coefs:
        copy.wait_recv()
    length = zs // PIECES
    pieces = [(x, p * length) for x in range(halves) for p in range(PIECES)]
    cells_of = [(x, slice(None), pl.ds(z, length)) for x, z in pieces]
    last_sems = [
        ([send_sem2.at[5 * index + i] for i in range(5)], [recv_sem2.at[4 * index + i] for i in range(4)])
        for index in range(len(pieces))
    ]
    for x in range(halves):
        for copy in partial[x]:
            copy.wait_recv()
        border_rows(x)
        along_y(pw.at[1, :, :, inner], x, True)
        finish(1, x, send2)
        for index, (x_of, z) in enumerate(pieces):
            if x_of == x:
                direct(send2, recv2, *last_sems[index], cells_of[index])

    collect(0, recv1, *first_sems, everything, range(halves), 0, zs)
    for x in range(halves):
        image(0, x, 0, zs)
    for index, (x, z) in enumerate(pieces):
        collect(1, recv2, *last_sems[index], cells_of[index], (x,), z, length)
        image(1, x, z, length)

    for copy in coefs + sum([list(c) for c in halo + partial], []):
        copy.wait_send()
    sent(send1, recv1, *first_sems, everything)
    for index in range(len(pieces)):
        sent(send2, recv2, *last_sems[index], cells_of[index])


def per_device(
    source_now, source_before, receiver_now, receiver_before, speed_term, aniso_field, tilt_field,
    angle_bins, weight_table, offset_lags, source_cells, source_wavelet, receiver_cells, receiver_traces,
):
    zs, rows, width = source_now.shape
    halves = width // LANES
    steps = source_wavelet.shape[0]
    n_off, n_bin, n_ang = weight_table.shape
    n_src = source_cells.shape[0]
    receivers = receiver_cells.shape[0]
    assert rows == ROWS and n_bin == ROWS and width & (width - 1) == 0
    half = (halves, zs, ROWS, LANES)
    block = (halves, 2, zs, ROWS, LANES)
    any_space = pl.BlockSpec(memory_space=pl.ANY)
    dma = pltpu.SemaphoreType.DMA
    in_specs = [any_space] * 14
    return pl.pallas_call(
        kernel,
        out_shape=pltpu.VMEM((n_ang, zs, rows, width), BF16),
        in_specs=in_specs,
        out_specs=pl.BlockSpec(memory_space=pltpu.VMEM),
        scratch_shapes=[
            pltpu.VMEM((steps, 2, halves, zs + 2 * PAD, 3 * ROWS, LANES), F32),
            pltpu.VMEM((2,) + half, F32),
            pltpu.VMEM(half, F32),
            pltpu.VMEM(half, F32),
            pltpu.VMEM(half, F32),
            pltpu.VMEM(half, jnp.int32),
            pltpu.VMEM((n_bin, n_ang, n_off), BF16),
            pltpu.SMEM((n_off,), jnp.int32),
            pltpu.SMEM((n_src,), jnp.int32),
            pltpu.SMEM((steps, n_src), F32),
            pltpu.VMEM((receivers // LANES, LANES), jnp.int32),
            pltpu.VMEM((steps, receivers), F32),
            pltpu.VMEM((n_off, n_ang, n_bin, LANES), F32),
            pltpu.VMEM((n_off, n_ang) + half, F32),
            pltpu.VMEM((steps, 2, halves, ROWS, LANES), F32),
            pltpu.VMEM((2,) + half, F32),
            pltpu.VMEM((2, halves, zs + 2 * PAD, ROWS, LANES), F32),
            pltpu.VMEM((2, halves, zs, 3 * ROWS, LANES), F32),
            pltpu.VMEM((2,) + half, F32),
            pltpu.VMEM((2, halves, zs + 2 * PAD, ROWS, LANES), F32),
            pltpu.VMEM(block, BF16),
            pltpu.VMEM(block, BF16),
            pltpu.VMEM(block, BF16),
            pltpu.VMEM(block, BF16),
            pltpu.VMEM(block, BF16),
            pltpu.VMEM(block, BF16),
            pltpu.VMEM((2,) + half, BF16),
            pltpu.VMEM(block, BF16),
            pltpu.VMEM((4,) + block, BF16),
            pltpu.VMEM((4,) + block, BF16),
            pltpu.VMEM((steps, 2, halves, zs, 5 * ROWS, LANES), F32),
            pltpu.VMEM((n_ang,) + half, F32),
            dma((8 * halves + 6,)),
            dma((2 * halves,)),
            dma((2 * halves,)),
            dma((2,)),
            dma((2,)),
            dma((2 * halves,)),
            dma((2 * halves,)),
            dma((5,)),
            dma((4,)),
            dma((5 * halves * PIECES,)),
            dma((4 * halves * PIECES,)),
        ],
        compiler_params=pltpu.CompilerParams(collective_id=0, has_side_effects=True),
    )(
        source_now, source_before, receiver_now, receiver_before, speed_term, aniso_field, tilt_field,
        angle_bins, jnp.transpose(weight_table, (1, 2, 0)), offset_lags, source_cells, source_wavelet,
        receiver_cells.reshape(receivers // LANES, LANES), receiver_traces,
    )


def solution(mesh):
    return jax.shard_map(
        per_device,
        mesh=mesh,
        in_specs=(
            P("shot", "gy", None),
            P("shot", "gy", None),
            P("shot", "gy", None),
            P("shot", "gy", None),
            P(None, "gy", None),
            P(None, "gy", None),
            P(None, "gy", None),
            P(None, "gy", None),
            P(),
            P(),
            P("shot"),
            P("shot", None),
            P("shot"),
            P("shot", None),
        ),
        out_specs=P("shot", None, "gy", None),
        check_vma=False,
    )
```

```python
import functools

import jax
import jax.numpy as jnp
from jax import lax
from jax.experimental import pallas as pl
from jax.experimental.pallas import tpu as pltpu
from jax.sharding import PartitionSpec as P

SECOND_COEF = (-205.0 / 72.0, 8.0 / 5.0, -1.0 / 5.0, 8.0 / 315.0, -1.0 / 560.0)
FIRST_COEF = (4.0 / 5.0, -1.0 / 5.0, 4.0 / 105.0, -1.0 / 280.0)
MESH = pl.DeviceIdType.MESH
F32 = jnp.float32
BF16 = jnp.bfloat16
LANES = 128
ROWS = 8
PAD = 4
LO, HI = 0, 1
OFFSETS = (-2, -1, 1, 2)
DIRECT = ((2, -1, 1), (2, -2, -1))
PASSED = ((1, 2), (-2, -1))
KEPT = 4
PIECES = 2


def kernel(
    sn_hbm, sb_hbm, rn_hbm, rb_hbm, speed_hbm, aniso_hbm, tilt_hbm, bins_hbm, wt_hbm,
    lags_hbm, scells_hbm, swave_hbm, rcells_hbm, rtraces_hbm,
    out,
    pw, qv, speed, a1, a2, bins, wt, lags, scells, swave, rcells, rtraces, table, cache, inj, base, grad,
    hw, share2, share1, send0, sendc, sendp, send1, send2, recv0, recvc, recvp, recv1, recv2, win,
    in_sem, send_sem0, recv_sem0, send_semc, recv_semc, send_semp, recv_semp, send_sem1, recv_sem1, send_sem2, recv_sem2,
):
    n = lax.axis_size("gy")
    me = lax.axis_index("gy")
    peer = {d: lax.rem(me + (d + n), n) for d in OFFSETS}
    odd = lax.rem(me, 2) == 1
    zs = sn_hbm.shape[0]
    halves = sn_hbm.shape[2] // LANES
    n_bin, n_ang, n_off = wt_hbm.shape
    kept = cache.shape[1]
    steps = swave.shape[0]
    n_src = scells.shape[0]
    rec_rows = rcells_hbm.shape[0]
    own = pl.ds(ROWS, ROWS)
    inner = pl.ds(PAD, zs)

    barrier = pltpu.get_barrier_semaphore()
    for d in OFFSETS:
        pl.semaphore_signal(barrier, inc=1, device_id={"gy": peer[d]}, device_id_type=MESH)

    copies = {}

    def fetch(name, index, src, dst):
        copy = pltpu.make_async_copy(src, dst, in_sem.at[index])
        copy.start()
        copies[name] = copy

    wanted = [
        (("now", m, x), ref.at[:, :, pl.ds(x * LANES, LANES)], pw.at[0, m, x, inner, own, :])
        for x in range(halves)
        for m, ref in enumerate((sn_hbm, rn_hbm))
    ]
    wanted += [("rcells", rcells_hbm, rcells), ("rtraces", rtraces_hbm, rtraces)]
    wanted += [("scells", scells_hbm, scells), ("swave", swave_hbm, swave)]
    for name, ref, dst in (("speed", speed_hbm, speed), ("aniso", aniso_hbm, a1), ("tilt", tilt_hbm, a2)):
        wanted += [((name, x), ref.at[:, :, pl.ds(x * LANES, LANES)], dst.at[x]) for x in range(halves)]
    for m, ref in enumerate((sb_hbm, rb_hbm)):
        wanted += [(("before", m, x), ref.at[:, :, pl.ds(x * LANES, LANES)], qv.at[m, x]) for x in range(halves)]
    wanted += [(("bins", x), bins_hbm.at[:, :, pl.ds(x * LANES, LANES)], bins.at[x]) for x in range(halves)]
    wanted += [("wt", wt_hbm, wt), ("lags", lags_hbm, lags)]
    for index, (name, src, dst) in enumerate(wanted):
        fetch(name, index, src, dst)

    edge = jnp.zeros((PAD, ROWS, LANES), F32)
    plane = jnp.zeros((zs, ROWS, LANES), F32)
    for x in range(halves):
        for m in range(2):
            for s in range(steps):
                pw[s, m, x, pl.ds(0, PAD), own, :] = edge
                pw[s, m, x, pl.ds(PAD + zs, PAD), own, :] = edge
            pw[0, m, x, inner, pl.ds(0, ROWS), :] = plane
            pw[0, m, x, inner, pl.ds(2 * ROWS, ROWS), :] = plane
            hw[m, x, :, own, :] = plane
            for padded in (grad, share1):
                padded[m, x, pl.ds(0, PAD)] = edge
                padded[m, x, pl.ds(PAD + zs, PAD)] = edge

    sub = lax.broadcasted_iota(jnp.int32, (ROWS, LANES), 0)
    lane = lax.broadcasted_iota(jnp.int32, (ROWS, LANES), 1)
    low_rows = sub < PAD

    def turn(v):
        return pltpu.roll(v, PAD, axis=v.ndim - 2)

    def pack(source, receiver, send, x, where_z):
        send[x, LO, where_z] = jnp.where(low_rows, source, turn(receiver)).astype(BF16)
        send[x, HI, where_z] = jnp.where(low_rows, turn(source), receiver).astype(BF16)

    def remote(src, dst, ssem, rsem, device):
        return pltpu.make_async_remote_copy(
            src_ref=src, dst_ref=dst, send_sem=ssem, recv_sem=rsem, device_id={"gy": device}, device_id_type=MESH
        )

    shift_bits = (halves * LANES).bit_length() - 1

    def injections():
        first_row = me * ROWS
        for name in ("rcells", "rtraces", "scells", "swave"):
            copies[name].wait()
        left, right = [], []
        col_iota = lax.broadcasted_iota(jnp.int32, (halves * LANES, LANES), 0)
        for c in range(rec_rows):
            cell = rcells[c : c + 1, :]
            row = lax.shift_right_logical(cell, shift_bits) - first_row
            col = jnp.bitwise_and(cell, halves * LANES - 1)
            hit = jnp.broadcast_to(row, (ROWS, LANES)) == sub
            parts = []
            for s in range(steps):
                amount = jnp.broadcast_to(rtraces[s : s + 1, c * LANES : (c + 1) * LANES], (ROWS, LANES))
                amount = jnp.where(hit, amount, 0.0)
                coarse = amount.astype(BF16).astype(F32)
                parts += [coarse, amount - coarse]
            left.append(jnp.concatenate(parts, axis=0).astype(BF16))
            right.append(jnp.where(jnp.broadcast_to(col, col_iota.shape) == col_iota, 1.0, 0.0).astype(BF16))
        spread = lax.dot_general(
            jnp.concatenate(left, axis=1),
            jnp.concatenate(right, axis=1),
            (((1,), (1,)), ((), ())),
            preferred_element_type=F32,
        )
        for s in range(steps):
            total = spread[2 * s * ROWS : (2 * s + 1) * ROWS] + spread[(2 * s + 1) * ROWS : (2 * s + 2) * ROWS]
            for x in range(halves):
                inj[s, 1, x] = total[:, x * LANES : (x + 1) * LANES]
        for s in range(steps):
            for x in range(halves):
                total = jnp.zeros((ROWS, LANES), F32)
                for i in range(n_src):
                    cell = scells[i]
                    row = lax.shift_right_logical(cell, shift_bits) - first_row
                    col = jnp.bitwise_and(cell, halves * LANES - 1) - x * LANES
                    total = total + jnp.where((sub == row) & (lane == col), swave[s, i], 0.0)
                inj[s, 0, x] = total

    halo = [
        (
            remote(send0.at[x, HI], recv0.at[x, 0], send_sem0.at[2 * x], recv_sem0.at[2 * x], peer[1]),
            remote(send0.at[x, LO], recv0.at[x, 1], send_sem0.at[2 * x + 1], recv_sem0.at[2 * x + 1], peer[-1]),
        )
        for x in range(halves)
    ]
    for x in range(halves):
        for m in range(2):
            copies[("now", m, x)].wait()
        pack(pw[0, 0, x, inner, own, :], pw[0, 1, x, inner, own, :], send0, x, pl.ds(0, zs))
        if x == 0:
            pl.semaphore_wait(barrier, len(OFFSETS))
        for copy in halo[x]:
            copy.start()

    def local_part(step):
        chunk = 4

        def part(i, carry):
            z = i * chunk
            for m in range(2):
                f = [pw[step, m, x, pl.ds(PAD + z, chunk), own, :] for x in range(halves)]
                first = [jnp.zeros_like(v) for v in f]
                second = [SECOND_COEF[0] * v for v in f]
                for k in range(1, PAD + 1):
                    up = [pltpu.roll(v, LANES - k, axis=2) for v in f] + [jnp.zeros_like(f[0])]
                    down = [jnp.zeros_like(f[0])] + [pltpu.roll(v, k, axis=2) for v in f]
                    for x in range(halves):
                        above = jnp.where(lane < LANES - k, up[x], up[x + 1])
                        below = jnp.where(lane >= k, down[x + 1], down[x])
                        second[x] = second[x] + SECOND_COEF[k] * (above + below)
                        first[x] = first[x] + FIRST_COEF[k - 1] * (above - below)
                for x in range(halves):
                    grad[m, x, pl.ds(PAD + z, chunk)] = first[x]
                    along_z = SECOND_COEF[0] * f[x]
                    for k in range(1, PAD + 1):
                        along_z = along_z + SECOND_COEF[k] * (
                            pw[step, m, x, pl.ds(PAD + z + k, chunk), own, :]
                            + pw[step, m, x, pl.ds(PAD + z - k, chunk), own, :]
                        )
                    before = qv[m, x, pl.ds(z, chunk)] if step == 0 else pw[step - 1, m, x, pl.ds(PAD + z, chunk), own, :]
                    base[m, x, pl.ds(z, chunk)] = (
                        2.0 * f[x]
                        - before
                        + a1[x, pl.ds(z, chunk)] * second[x]
                        + speed[x, pl.ds(z, chunk)] * along_z
                    )
            return carry

        lax.fori_loop(0, zs // chunk, part, 0)
        for m in range(2):
            for x in range(halves):
                base[m, x, 0] = base[m, x, 0] + inj[step, m, x]

    def halo_rows(window, x, low, high):
        window[0, x, :, pl.ds(0, ROWS), :] = turn(low)
        window[1, x, :, pl.ds(0, ROWS), :] = low
        window[0, x, :, pl.ds(2 * ROWS, ROWS), :] = high
        window[1, x, :, pl.ds(2 * ROWS, ROWS), :] = turn(high)

    part_chunk = 4

    def along_y(window, x, whole):
        def part(i, carry):
            z = i * part_chunk
            cells = pl.ds(z, part_chunk)
            for m in range(2):

                def rows(k):
                    return window[m, x, cells, pl.ds(ROWS + k, ROWS), :]

                second, first = 0.0, 0.0
                if whole:
                    second, first = SECOND_COEF[0] * rows(0), grad[m, x, pl.ds(PAD + z, part_chunk)]
                for k in range(1, PAD + 1):
                    above, below = rows(k), rows(-k)
                    second = second + SECOND_COEF[k] * (above + below)
                    first = first + FIRST_COEF[k - 1] * (above - below)
                grad[m, x, pl.ds(PAD + z, part_chunk)] = first
                base[m, x, cells] = base[m, x, cells] + a1[x, cells] * second
            return carry

        lax.fori_loop(0, zs // part_chunk, part, 0)

    def along_z(padded, member, x, z):
        mixed = jnp.zeros((part_chunk, ROWS, LANES), F32)
        for k in range(1, PAD + 1):
            mixed = mixed + FIRST_COEF[k - 1] * (
                padded[member, x, pl.ds(PAD + z + k, part_chunk)] - padded[member, x, pl.ds(PAD + z - k, part_chunk)]
            )
        return mixed

    def finish(step, x, send, whole=True):
        def part(i, carry):
            z = i * part_chunk
            cells = pl.ds(z, part_chunk)
            new = []
            for m in range(2):
                value = base[m, x, cells] + a2[x, cells] * along_z(grad, m, x, z)
                new.append(value)
                if not whole:
                    base[m, x, cells] = value
                    continue
                if step + 1 < steps:
                    pw[step + 1, m, x, pl.ds(PAD + z, part_chunk), own, :] = value
                win[step, m, x, cells, pl.ds(2 * ROWS, ROWS), :] = value.astype(BF16).astype(F32)
            pack(new[0], new[1], send, x, cells)
            return carry

        lax.fori_loop(0, zs // part_chunk, part, 0)

    def shares(x):
        def part(i, carry):
            z = i * part_chunk
            for side in range(2):
                second, first = [], []
                for m in range(2):
                    two, one = 0.0, 0.0
                    for k in range(1, PAD + 1):
                        row = ROWS - PAD + k if side == 0 else 2 * ROWS - k
                        value = pw[0, m, x, pl.ds(PAD + z, part_chunk), pl.ds(row, ROWS), :]
                        two = two + SECOND_COEF[k] * value
                        one = one + (FIRST_COEF[k - 1] if side == 0 else -FIRST_COEF[k - 1]) * value
                    second.append(two)
                    first.append(one)
                share2[side, x, pl.ds(z, part_chunk)] = jnp.where(low_rows, second[0], turn(second[1]))
                share1[side, x, pl.ds(PAD + z, part_chunk)] = jnp.where(low_rows, first[0], turn(first[1]))
            return carry

        lax.fori_loop(0, zs // part_chunk, part, 0)

    def border_rows(x):
        whole = []
        for side in range(2):
            blocks = []
            for z in range(0, zs, part_chunk):
                cells = pl.ds(z, part_chunk)
                pair = recvc[side, x, cells].astype(F32)
                flat, tilted = jnp.where(low_rows, pair, turn(pair)), jnp.where(low_rows, turn(pair), pair)
                blocks.append(
                    recvp[x, side, cells].astype(F32)
                    + flat * share2[side, x, cells]
                    + tilted * along_z(share1, side, x, z)
                )
            whole.append(jnp.concatenate(blocks, axis=0))
        halo_rows(pw.at[1, :, :, inner], x, whole[0], whole[1])

    def open_block(step, d, recv, x, z, length):
        cells = pl.ds(z, length)
        rows = pl.ds((2 + d) * ROWS, ROWS)
        slot = OFFSETS.index(d)
        low = recv[slot, x, LO, cells].astype(F32)
        high = recv[slot, x, HI, cells].astype(F32)
        win[step, 0, x, cells, rows, :] = jnp.where(low_rows, low, turn(high))
        win[step, 1, x, cells, rows, :] = jnp.where(low_rows, turn(low), high)

    chunk = 4

    def gathered(h, a, bin_ids):
        row = table[h, a]
        return jnp.stack([jnp.take_along_axis(row, ids, axis=0) for ids in bin_ids])

    def keep_weights(x):
        def part(i, carry):
            z = i * chunk
            bin_ids = [bins[x, z + j] for j in range(chunk)]
            for h in range(n_off):
                for a in range(kept):
                    cache[h, a, x, pl.ds(z, chunk)] = gathered(h, a, bin_ids)
            return carry

        lax.fori_loop(0, zs // chunk, part, 0)

    def image(x, start, length):
        def part(i, carry):
            z = start + i * chunk
            bin_ids = [bins[x, z + j] for j in range(chunk)]
            total = [jnp.zeros((chunk, ROWS, LANES), F32)] * n_ang
            for h in range(n_off):
                lag = lags[h]
                product = 0.0
                for step in range(steps):
                    product = product + (
                        win[step, 0, x, pl.ds(z, chunk), pl.ds(2 * ROWS - lag, ROWS), :]
                        * win[step, 1, x, pl.ds(z, chunk), pl.ds(2 * ROWS + lag, ROWS), :]
                    )
                for a in range(n_ang):
                    weight = cache[h, a, x, pl.ds(z, chunk)] if a < kept else gathered(h, a, bin_ids)
                    total[a] = total[a] + weight * product
            for a in range(n_ang):
                out[a, pl.ds(z, chunk), :, x * LANES : (x + 1) * LANES] = total[a].astype(BF16)
            return carry

        lax.fori_loop(0, length // chunk, part, 0)

    injections()
    for x in range(halves):
        copies[("speed", x)].wait()
        copies[("aniso", x)].wait()
        copies[("tilt", x)].wait()
        a1[x] = speed[x] * (1.0 + 2.0 * a1[x])
        a2[x] = speed[x] * a2[x]
        pack(a1[x], a2[x], sendc, x, pl.ds(0, zs))
    coefs = [
        remote(sendc.at[:, half], recvc.at[i], send_semc.at[i], recv_semc.at[i], peer[d])
        for i, (half, d) in enumerate(((HI, 1), (LO, -1)))
    ]
    for copy in coefs:
        copy.start()
    for m in range(2):
        for x in range(halves):
            copies[("before", m, x)].wait()
    local_part(0)
    partial = []
    for x in range(halves):
        along_y(pw.at[0, :, :, inner], x, True)
        finish(0, x, sendp, whole=False)
        partial.append(
            [
                remote(sendp.at[x, half], recvp.at[x, i], send_semp.at[2 * x + i], recv_semp.at[2 * x + i], peer[d])
                for i, (half, d) in enumerate(((HI, 1), (LO, -1)))
            ]
        )
        for copy in partial[x]:
            copy.start()
    for x in range(halves):
        shares(x)
    copies["wt"].wait()
    copies["lags"].wait()
    by_bin = [wt[b].astype(F32) for b in range(n_bin)]
    for a in range(n_ang):
        rows = jnp.concatenate([v[a : a + 1] for v in by_bin], axis=0)
        for h in range(n_off):
            table[h, a] = jnp.broadcast_to(rows[:, h : h + 1], (n_bin, LANES))
    for x in range(halves):
        copies[("bins", x)].wait()

    def direct(send, recv, send_sems, recv_sems, cells):
        for parity, here in enumerate((jnp.logical_not(odd), odd)):

            @pl.when(here)
            def _():
                for i, d in enumerate(DIRECT[parity]):
                    slot = OFFSETS.index(-d)
                    remote(send.at[cells], recv.at[(slot,) + cells], send_sems[i], recv_sems[slot], peer[d]).start()

    def passed(recv, send_sems, recv_sems, cells, index):
        here, there = (OFFSETS.index(d) for d in PASSED[index])
        return remote(recv.at[(here,) + cells], recv.at[(there,) + cells], send_sems[index], recv_sems[there], peer[-1])

    def collect(step, recv, send_sems, recv_sems, cells, x_list, z, length):
        for d in (1, -2, -1, 2):
            slot = OFFSETS.index(d)
            remote(recv.at[(slot,) + cells], recv.at[(slot,) + cells], send_sems[0], recv_sems[slot], peer[1]).wait_recv()
            for index, (source, _) in enumerate(PASSED):
                if source == d:

                    @pl.when(odd)
                    def _():
                        passed(recv, send_sems[3:], recv_sems, cells, index).start()

        for d in OFFSETS:
            for x in x_list:
                open_block(step, d, recv, x, z, length)

    def sent(send, recv, send_sems, recv_sems, cells):
        for i in range(3):
            remote(send.at[cells], recv.at[(0,) + cells], send_sems[i], recv_sems[0], peer[1]).wait_send()

        @pl.when(odd)
        def _():
            for index in range(len(PASSED)):
                passed(recv, send_sems[3:], recv_sems, cells, index).wait_send()

    first_sems = [
        ([send_sem1.at[5 * x + i] for i in range(5)], [recv_sem1.at[4 * x + i] for i in range(4)]) for x in range(halves)
    ]

    for x in range(halves):
        for copy in halo[x]:
            copy.wait_recv()
        halo_rows(hw, x, recv0[x, 0].astype(F32), recv0[x, 1].astype(F32))
        along_y(hw, x, False)
        finish(0, x, send1)
        direct(send1, recv1, *first_sems[x], (x,))
    local_part(1)
    for copy in coefs:
        copy.wait_recv()
    length = zs // PIECES
    pieces = [(x, p * length) for x in range(halves) for p in range(PIECES)]
    cells_of = [(x, slice(None), pl.ds(z, length)) for x, z in pieces]
    last_sems = [
        ([send_sem2.at[5 * index + i] for i in range(5)], [recv_sem2.at[4 * index + i] for i in range(4)])
        for index in range(len(pieces))
    ]
    for x in range(halves):
        for copy in partial[x]:
            copy.wait_recv()
        border_rows(x)
        along_y(pw.at[1, :, :, inner], x, True)
        finish(1, x, send2)
        for index, (x_of, z) in enumerate(pieces):
            if x_of == x:
                direct(send2, recv2, *last_sems[index], cells_of[index])

    for x in range(halves):
        keep_weights(x)
    for x in range(halves):
        collect(0, recv1, *first_sems[x], (x,), (x,), 0, zs)
    for index, (x, z) in enumerate(pieces):
        collect(1, recv2, *last_sems[index], cells_of[index], (x,), z, length)
        if index:
            image(*pieces[index - 1], length)
    image(*pieces[-1], length)

    for copy in coefs + sum([list(c) for c in halo + partial], []):
        copy.wait_send()
    for x in range(halves):
        sent(send1, recv1, *first_sems[x], (x,))
    for index in range(len(pieces)):
        sent(send2, recv2, *last_sems[index], cells_of[index])


def per_device(
    source_now, source_before, receiver_now, receiver_before, speed_term, aniso_field, tilt_field,
    angle_bins, weight_table, offset_lags, source_cells, source_wavelet, receiver_cells, receiver_traces,
):
    zs, rows, width = source_now.shape
    halves = width // LANES
    steps = source_wavelet.shape[0]
    n_off, n_bin, n_ang = weight_table.shape
    n_src = source_cells.shape[0]
    receivers = receiver_cells.shape[0]
    assert rows == ROWS and n_bin == ROWS and width & (width - 1) == 0
    half = (halves, zs, ROWS, LANES)
    block = (halves, 2, zs, ROWS, LANES)
    any_space = pl.BlockSpec(memory_space=pl.ANY)
    dma = pltpu.SemaphoreType.DMA
    in_specs = [any_space] * 14
    return pl.pallas_call(
        kernel,
        out_shape=pltpu.VMEM((n_ang, zs, rows, width), BF16),
        in_specs=in_specs,
        out_specs=pl.BlockSpec(memory_space=pltpu.VMEM),
        scratch_shapes=[
            pltpu.VMEM((steps, 2, halves, zs + 2 * PAD, 3 * ROWS, LANES), F32),
            pltpu.VMEM((2,) + half, F32),
            pltpu.VMEM(half, F32),
            pltpu.VMEM(half, F32),
            pltpu.VMEM(half, F32),
            pltpu.VMEM(half, jnp.int32),
            pltpu.VMEM((n_bin, n_ang, n_off), BF16),
            pltpu.SMEM((n_off,), jnp.int32),
            pltpu.SMEM((n_src,), jnp.int32),
            pltpu.SMEM((steps, n_src), F32),
            pltpu.VMEM((receivers // LANES, LANES), jnp.int32),
            pltpu.VMEM((steps, receivers), F32),
            pltpu.VMEM((n_off, n_ang, n_bin, LANES), F32),
            pltpu.VMEM((n_off, KEPT) + half, F32),
            pltpu.VMEM((steps, 2, halves, ROWS, LANES), F32),
            pltpu.VMEM((2,) + half, F32),
            pltpu.VMEM((2, halves, zs + 2 * PAD, ROWS, LANES), F32),
            pltpu.VMEM((2, halves, zs, 3 * ROWS, LANES), F32),
            pltpu.VMEM((2,) + half, F32),
            pltpu.VMEM((2, halves, zs + 2 * PAD, ROWS, LANES), F32),
            pltpu.VMEM(block, BF16),
            pltpu.VMEM(block, BF16),
            pltpu.VMEM(block, BF16),
            pltpu.VMEM(block, BF16),
            pltpu.VMEM(block, BF16),
            pltpu.VMEM(block, BF16),
            pltpu.VMEM((2,) + half, BF16),
            pltpu.VMEM(block, BF16),
            pltpu.VMEM((4,) + block, BF16),
            pltpu.VMEM((4,) + block, BF16),
            pltpu.VMEM((steps, 2, halves, zs, 5 * ROWS, LANES), F32),
            dma((8 * halves + 6,)),
            dma((2 * halves,)),
            dma((2 * halves,)),
            dma((2,)),
            dma((2,)),
            dma((2 * halves,)),
            dma((2 * halves,)),
            dma((5 * halves,)),
            dma((4 * halves,)),
            dma((5 * halves * PIECES,)),
            dma((4 * halves * PIECES,)),
        ],
        compiler_params=pltpu.CompilerParams(collective_id=0, has_side_effects=True),
    )(
        source_now, source_before, receiver_now, receiver_before, speed_term, aniso_field, tilt_field,
        angle_bins, jnp.transpose(weight_table, (1, 2, 0)), offset_lags, source_cells, source_wavelet,
        receiver_cells.reshape(receivers // LANES, LANES), receiver_traces,
    )


def solution(mesh):
    return jax.shard_map(
        per_device,
        mesh=mesh,
        in_specs=(
            P("shot", "gy", None),
            P("shot", "gy", None),
            P("shot", "gy", None),
            P("shot", "gy", None),
            P(None, "gy", None),
            P(None, "gy", None),
            P(None, "gy", None),
            P(None, "gy", None),
            P(),
            P(),
            P("shot"),
            P("shot", None),
            P("shot"),
            P("shot", None),
        ),
        out_specs=P("shot", None, "gy", None),
        check_vma=False,
    )
```

```python
import functools

import jax
import jax.numpy as jnp
from jax import lax
from jax.experimental import pallas as pl
from jax.experimental.pallas import tpu as pltpu
from jax.sharding import PartitionSpec as P

SECOND_COEF = (-205.0 / 72.0, 8.0 / 5.0, -1.0 / 5.0, 8.0 / 315.0, -1.0 / 560.0)
FIRST_COEF = (4.0 / 5.0, -1.0 / 5.0, 4.0 / 105.0, -1.0 / 280.0)
MESH = pl.DeviceIdType.MESH
F32 = jnp.float32
BF16 = jnp.bfloat16
LANES = 128
ROWS = 8
PAD = 4
LO, HI = 0, 1
OFFSETS = (-2, -1, 1, 2)
DIRECT = ((2, -1, 1), (2, -2, -1))
PASSED = ((1, 2), (-2, -1))
GROUP = 8
KEPT = 4
PIECES = 2


def kernel(
    sn_hbm, sb_hbm, rn_hbm, rb_hbm, speed_hbm, aniso_hbm, tilt_hbm, bins_hbm, wt_hbm,
    lags_hbm, scells_hbm, swave_hbm, rcells_hbm, rtraces_hbm,
    out,
    pw, qv, speed, a1, a2, bins, wt, lags, scells, swave, rcells, rtraces, table, cache, inj, base, grad,
    hw, share2, share1, send0, sendc, sendp, send1, send2, recv0, recvc, recvp, recv1, recv2, win,
    in_sem, beyond, send_sem0, recv_sem0, send_semc, recv_semc, send_semp, recv_semp, send_sem1, recv_sem1, send_sem2, recv_sem2,
):
    n = lax.axis_size("gy")
    me = lax.axis_index("gy")
    peer = {d: lax.rem(me + (d + n), n) for d in OFFSETS}
    odd = lax.rem(me, 2) == 1
    zs = sn_hbm.shape[0]
    halves = sn_hbm.shape[2] // LANES
    n_bin, n_ang, n_off = wt_hbm.shape
    kept = cache.shape[1]
    steps = swave.shape[0]
    n_src = scells.shape[0]
    rec_rows = rcells_hbm.shape[0]
    own = pl.ds(ROWS, ROWS)
    inner = pl.ds(PAD, zs)

    barrier = pltpu.get_barrier_semaphore()
    for d in (1, -1):
        pl.semaphore_signal(barrier, inc=1, device_id={"gy": peer[d]}, device_id_type=MESH)

    copies = {}

    def fetch(name, index, src, dst):
        copy = pltpu.make_async_copy(src, dst, in_sem.at[index])
        copy.start()
        copies[name] = copy

    wanted = [
        (("now", m, x), ref.at[:, :, pl.ds(x * LANES, LANES)], pw.at[0, m, x, inner, own, :])
        for x in range(halves)
        for m, ref in enumerate((sn_hbm, rn_hbm))
    ]
    wanted += [("rcells", rcells_hbm, rcells), ("rtraces", rtraces_hbm, rtraces)]
    wanted += [("scells", scells_hbm, scells), ("swave", swave_hbm, swave)]
    for name, ref, dst in (("speed", speed_hbm, speed), ("aniso", aniso_hbm, a1), ("tilt", tilt_hbm, a2)):
        wanted += [((name, x), ref.at[:, :, pl.ds(x * LANES, LANES)], dst.at[x]) for x in range(halves)]
    for m, ref in enumerate((sb_hbm, rb_hbm)):
        wanted += [(("before", m, x), ref.at[:, :, pl.ds(x * LANES, LANES)], qv.at[m, x]) for x in range(halves)]
    wanted += [(("bins", x), bins_hbm.at[:, :, pl.ds(x * LANES, LANES)], bins.at[x]) for x in range(halves)]
    wanted += [("wt", wt_hbm, wt), ("lags", lags_hbm, lags)]
    for index, (name, src, dst) in enumerate(wanted):
        fetch(name, index, src, dst)

    edge = jnp.zeros((PAD, ROWS, LANES), F32)
    plane = jnp.zeros((zs, ROWS, LANES), F32)
    for x in range(halves):
        for m in range(2):
            for s in range(steps):
                pw[s, m, x, pl.ds(0, PAD), own, :] = edge
                pw[s, m, x, pl.ds(PAD + zs, PAD), own, :] = edge
            pw[0, m, x, inner, pl.ds(0, ROWS), :] = plane
            pw[0, m, x, inner, pl.ds(2 * ROWS, ROWS), :] = plane
            hw[m, x, :, own, :] = plane
            for padded in (grad, share1):
                padded[m, x, pl.ds(0, PAD)] = edge
                padded[m, x, pl.ds(PAD + zs, PAD)] = edge

    sub = lax.broadcasted_iota(jnp.int32, (ROWS, LANES), 0)
    lane = lax.broadcasted_iota(jnp.int32, (ROWS, LANES), 1)
    low_rows = sub < PAD

    def turn(v):
        return pltpu.roll(v, PAD, axis=v.ndim - 2)

    def pack(source, receiver, send, x, where_z):
        send[x, LO, where_z] = jnp.where(low_rows, source, turn(receiver)).astype(BF16)
        send[x, HI, where_z] = jnp.where(low_rows, turn(source), receiver).astype(BF16)

    def remote(src, dst, ssem, rsem, device):
        return pltpu.make_async_remote_copy(
            src_ref=src, dst_ref=dst, send_sem=ssem, recv_sem=rsem, device_id={"gy": device}, device_id_type=MESH
        )

    shift_bits = (halves * LANES).bit_length() - 1

    def injections():
        first_row = me * ROWS
        for name in ("rcells", "rtraces", "scells", "swave"):
            copies[name].wait()
        left, right = [], []
        col_iota = lax.broadcasted_iota(jnp.int32, (halves * LANES, LANES), 0)
        for c in range(rec_rows):
            cell = rcells[c : c + 1, :]
            row = lax.shift_right_logical(cell, shift_bits) - first_row
            col = jnp.bitwise_and(cell, halves * LANES - 1)
            hit = jnp.broadcast_to(row, (ROWS, LANES)) == sub
            parts = []
            for s in range(steps):
                amount = jnp.broadcast_to(rtraces[s : s + 1, c * LANES : (c + 1) * LANES], (ROWS, LANES))
                amount = jnp.where(hit, amount, 0.0)
                coarse = amount.astype(BF16).astype(F32)
                parts += [coarse, amount - coarse]
            left.append(jnp.concatenate(parts, axis=0).astype(BF16))
            right.append(jnp.where(jnp.broadcast_to(col, col_iota.shape) == col_iota, 1.0, 0.0).astype(BF16))
        spread = lax.dot_general(
            jnp.concatenate(left, axis=1),
            jnp.concatenate(right, axis=1),
            (((1,), (1,)), ((), ())),
            preferred_element_type=F32,
        )
        for s in range(steps):
            total = spread[2 * s * ROWS : (2 * s + 1) * ROWS] + spread[(2 * s + 1) * ROWS : (2 * s + 2) * ROWS]
            for x in range(halves):
                inj[s, 1, x] = total[:, x * LANES : (x + 1) * LANES]
        for s in range(steps):
            for x in range(halves):
                total = jnp.zeros((ROWS, LANES), F32)
                for i in range(n_src):
                    cell = scells[i]
                    row = lax.shift_right_logical(cell, shift_bits) - first_row
                    col = jnp.bitwise_and(cell, halves * LANES - 1) - x * LANES
                    total = total + jnp.where((sub == row) & (lane == col), swave[s, i], 0.0)
                inj[s, 0, x] = total

    halo = [
        (
            remote(send0.at[x, HI], recv0.at[x, 0], send_sem0.at[2 * x], recv_sem0.at[2 * x], peer[1]),
            remote(send0.at[x, LO], recv0.at[x, 1], send_sem0.at[2 * x + 1], recv_sem0.at[2 * x + 1], peer[-1]),
        )
        for x in range(halves)
    ]
    for x in range(halves):
        for m in range(2):
            copies[("now", m, x)].wait()
        pack(pw[0, 0, x, inner, own, :], pw[0, 1, x, inner, own, :], send0, x, pl.ds(0, zs))
        if x == 0:
            pl.semaphore_wait(barrier, 2)
        for copy in halo[x]:
            copy.start()

    def local_part(step):
        chunk = 4

        def part(i, carry):
            z = i * chunk
            for m in range(2):
                f = [pw[step, m, x, pl.ds(PAD + z, chunk), own, :] for x in range(halves)]
                first = [jnp.zeros_like(v) for v in f]
                second = [SECOND_COEF[0] * v for v in f]
                for k in range(1, PAD + 1):
                    up = [pltpu.roll(v, LANES - k, axis=2) for v in f] + [jnp.zeros_like(f[0])]
                    down = [jnp.zeros_like(f[0])] + [pltpu.roll(v, k, axis=2) for v in f]
                    for x in range(halves):
                        above = jnp.where(lane < LANES - k, up[x], up[x + 1])
                        below = jnp.where(lane >= k, down[x + 1], down[x])
                        second[x] = second[x] + SECOND_COEF[k] * (above + below)
                        first[x] = first[x] + FIRST_COEF[k - 1] * (above - below)
                for x in range(halves):
                    grad[m, x, pl.ds(PAD + z, chunk)] = first[x]
                    along_z = SECOND_COEF[0] * f[x]
                    for k in range(1, PAD + 1):
                        along_z = along_z + SECOND_COEF[k] * (
                            pw[step, m, x, pl.ds(PAD + z + k, chunk), own, :]
                            + pw[step, m, x, pl.ds(PAD + z - k, chunk), own, :]
                        )
                    before = qv[m, x, pl.ds(z, chunk)] if step == 0 else pw[step - 1, m, x, pl.ds(PAD + z, chunk), own, :]
                    base[m, x, pl.ds(z, chunk)] = (
                        2.0 * f[x]
                        - before
                        + a1[x, pl.ds(z, chunk)] * second[x]
                        + speed[x, pl.ds(z, chunk)] * along_z
                    )
            return carry

        lax.fori_loop(0, zs // chunk, part, 0)
        for m in range(2):
            for x in range(halves):
                base[m, x, 0] = base[m, x, 0] + inj[step, m, x]

    def halo_rows(window, x, low, high):
        window[0, x, :, pl.ds(0, ROWS), :] = turn(low)
        window[1, x, :, pl.ds(0, ROWS), :] = low
        window[0, x, :, pl.ds(2 * ROWS, ROWS), :] = high
        window[1, x, :, pl.ds(2 * ROWS, ROWS), :] = turn(high)

    part_chunk = 4

    def along_y(window, x, whole):
        def part(i, carry):
            z = i * part_chunk
            cells = pl.ds(z, part_chunk)
            for m in range(2):

                def rows(k):
                    return window[m, x, cells, pl.ds(ROWS + k, ROWS), :]

                second, first = 0.0, 0.0
                if whole:
                    second, first = SECOND_COEF[0] * rows(0), grad[m, x, pl.ds(PAD + z, part_chunk)]
                for k in range(1, PAD + 1):
                    above, below = rows(k), rows(-k)
                    second = second + SECOND_COEF[k] * (above + below)
                    first = first + FIRST_COEF[k - 1] * (above - below)
                grad[m, x, pl.ds(PAD + z, part_chunk)] = first
                base[m, x, cells] = base[m, x, cells] + a1[x, cells] * second
            return carry

        lax.fori_loop(0, zs // part_chunk, part, 0)

    def along_z(padded, member, x, z):
        mixed = jnp.zeros((part_chunk, ROWS, LANES), F32)
        for k in range(1, PAD + 1):
            mixed = mixed + FIRST_COEF[k - 1] * (
                padded[member, x, pl.ds(PAD + z + k, part_chunk)] - padded[member, x, pl.ds(PAD + z - k, part_chunk)]
            )
        return mixed

    def finish(step, x, send, whole=True):
        def part(i, carry):
            z = i * part_chunk
            cells = pl.ds(z, part_chunk)
            new = []
            for m in range(2):
                value = base[m, x, cells] + a2[x, cells] * along_z(grad, m, x, z)
                new.append(value)
                if not whole:
                    base[m, x, cells] = value
                    continue
                if step + 1 < steps:
                    pw[step + 1, m, x, pl.ds(PAD + z, part_chunk), own, :] = value
                win[step, m, x, cells, pl.ds(2 * ROWS, ROWS), :] = value.astype(BF16).astype(F32)
            pack(new[0], new[1], send, x, cells)
            return carry

        lax.fori_loop(0, zs // part_chunk, part, 0)

    def shares(x):
        def part(i, carry):
            z = i * part_chunk
            for side in range(2):
                second, first = [], []
                for m in range(2):
                    two, one = 0.0, 0.0
                    for k in range(1, PAD + 1):
                        row = ROWS - PAD + k if side == 0 else 2 * ROWS - k
                        value = pw[0, m, x, pl.ds(PAD + z, part_chunk), pl.ds(row, ROWS), :]
                        two = two + SECOND_COEF[k] * value
                        one = one + (FIRST_COEF[k - 1] if side == 0 else -FIRST_COEF[k - 1]) * value
                    second.append(two)
                    first.append(one)
                share2[side, x, pl.ds(z, part_chunk)] = jnp.where(low_rows, second[0], turn(second[1]))
                share1[side, x, pl.ds(PAD + z, part_chunk)] = jnp.where(low_rows, first[0], turn(first[1]))
            return carry

        lax.fori_loop(0, zs // part_chunk, part, 0)

    def border_rows(x):
        whole = []
        for side in range(2):
            blocks = []
            for z in range(0, zs, part_chunk):
                cells = pl.ds(z, part_chunk)
                pair = recvc[side, x, cells].astype(F32)
                flat, tilted = jnp.where(low_rows, pair, turn(pair)), jnp.where(low_rows, turn(pair), pair)
                blocks.append(
                    recvp[x, side, cells].astype(F32)
                    + flat * share2[side, x, cells]
                    + tilted * along_z(share1, side, x, z)
                )
            whole.append(jnp.concatenate(blocks, axis=0))
        halo_rows(pw.at[1, :, :, inner], x, whole[0], whole[1])

    def open_block(step, d, recv, x, z, length):
        cells = pl.ds(z, length)
        rows = pl.ds((2 + d) * ROWS, ROWS)
        slot = OFFSETS.index(d)
        low = recv[slot, x, LO, cells].astype(F32)
        high = recv[slot, x, HI, cells].astype(F32)
        win[step, 0, x, cells, rows, :] = jnp.where(low_rows, low, turn(high))
        win[step, 1, x, cells, rows, :] = jnp.where(low_rows, turn(low), high)

    chunk = 4

    def gathered(h, a, bin_ids):
        row = table[h, a]
        return jnp.stack([jnp.take_along_axis(row, ids, axis=0) for ids in bin_ids])

    def keep_weights(x):
        def part(i, carry):
            z = i * chunk
            bin_ids = [bins[x, z + j] for j in range(chunk)]
            for h in range(n_off):
                for a in range(kept):
                    cache[h, a, x, pl.ds(z, chunk)] = gathered(h, a, bin_ids)
            return carry

        lax.fori_loop(0, zs // chunk, part, 0)

    def image(x, start, length):
        def part(i, carry):
            z = start + i * chunk
            bin_ids = [bins[x, z + j] for j in range(chunk)]
            def lag_group(g, total):
                total = list(total)
                for j in range(GROUP):
                    h = g * GROUP + j
                    lag = lags[h]
                    product = 0.0
                    for step in range(steps):
                        product = product + (
                            win[step, 0, x, pl.ds(z, chunk), pl.ds(2 * ROWS - lag, ROWS), :]
                            * win[step, 1, x, pl.ds(z, chunk), pl.ds(2 * ROWS + lag, ROWS), :]
                        )
                    for a in range(n_ang):
                        weight = cache[h, a, x, pl.ds(z, chunk)] if a < kept else gathered(h, a, bin_ids)
                        total[a] = total[a] + weight * product
                return tuple(total)

            total = lax.fori_loop(0, n_off // GROUP, lag_group, (jnp.zeros((chunk, ROWS, LANES), F32),) * n_ang)
            for a in range(n_ang):
                out[a, pl.ds(z, chunk), :, x * LANES : (x + 1) * LANES] = total[a].astype(BF16)
            return carry

        lax.fori_loop(0, length // chunk, part, 0)

    for d in (1, -1):
        pl.semaphore_signal(beyond, inc=1, device_id={"gy": peer[d]}, device_id_type=MESH)

    injections()
    for x in range(halves):
        copies[("speed", x)].wait()
        copies[("aniso", x)].wait()
        copies[("tilt", x)].wait()
        a1[x] = speed[x] * (1.0 + 2.0 * a1[x])
        a2[x] = speed[x] * a2[x]
        pack(a1[x], a2[x], sendc, x, pl.ds(0, zs))
    coefs = [
        remote(sendc.at[:, half], recvc.at[i], send_semc.at[i], recv_semc.at[i], peer[d])
        for i, (half, d) in enumerate(((HI, 1), (LO, -1)))
    ]
    for copy in coefs:
        copy.start()
    for m in range(2):
        for x in range(halves):
            copies[("before", m, x)].wait()
    local_part(0)
    partial = []
    for x in range(halves):
        along_y(pw.at[0, :, :, inner], x, True)
        finish(0, x, sendp, whole=False)
        partial.append(
            [
                remote(sendp.at[x, half], recvp.at[x, i], send_semp.at[2 * x + i], recv_semp.at[2 * x + i], peer[d])
                for i, (half, d) in enumerate(((HI, 1), (LO, -1)))
            ]
        )
        for copy in partial[x]:
            copy.start()
    for x in range(halves):
        shares(x)
    copies["wt"].wait()
    copies["lags"].wait()
    by_bin = [wt[b].astype(F32) for b in range(n_bin)]
    for a in range(n_ang):
        rows = jnp.concatenate([v[a : a + 1] for v in by_bin], axis=0)
        for h in range(n_off):
            table[h, a] = jnp.broadcast_to(rows[:, h : h + 1], (n_bin, LANES))
    for x in range(halves):
        copies[("bins", x)].wait()

    def direct(send, recv, send_sems, recv_sems, cells):
        for parity, here in enumerate((jnp.logical_not(odd), odd)):

            @pl.when(here)
            def _():
                for i, d in enumerate(DIRECT[parity]):
                    slot = OFFSETS.index(-d)
                    remote(send.at[cells], recv.at[(slot,) + cells], send_sems[i], recv_sems[slot], peer[d]).start()

    def passed(recv, send_sems, recv_sems, cells, index):
        here, there = (OFFSETS.index(d) for d in PASSED[index])
        return remote(recv.at[(here,) + cells], recv.at[(there,) + cells], send_sems[index], recv_sems[there], peer[-1])

    def collect(step, recv, send_sems, recv_sems, cells, x_list, z, length):
        for d in (1, -2, -1, 2):
            slot = OFFSETS.index(d)
            remote(recv.at[(slot,) + cells], recv.at[(slot,) + cells], send_sems[0], recv_sems[slot], peer[1]).wait_recv()
            for index, (source, _) in enumerate(PASSED):
                if source == d:

                    @pl.when(odd)
                    def _():
                        passed(recv, send_sems[3:], recv_sems, cells, index).start()

        for d in OFFSETS:
            for x in x_list:
                open_block(step, d, recv, x, z, length)

    def sent(send, recv, send_sems, recv_sems, cells):
        for i in range(3):
            remote(send.at[cells], recv.at[(0,) + cells], send_sems[i], recv_sems[0], peer[1]).wait_send()

        @pl.when(odd)
        def _():
            for index in range(len(PASSED)):
                passed(recv, send_sems[3:], recv_sems, cells, index).wait_send()

    first_sems = [
        ([send_sem1.at[5 * x + i] for i in range(5)], [recv_sem1.at[4 * x + i] for i in range(4)]) for x in range(halves)
    ]

    for x in range(halves):
        for copy in halo[x]:
            copy.wait_recv()
        halo_rows(hw, x, recv0[x, 0].astype(F32), recv0[x, 1].astype(F32))
        along_y(hw, x, False)
        finish(0, x, send1)
        if x == 0:
            pl.semaphore_wait(beyond, 2)
        direct(send1, recv1, *first_sems[x], (x,))
    local_part(1)
    for copy in coefs:
        copy.wait_recv()
    length = zs // PIECES
    pieces = [(x, p * length) for x in range(halves) for p in range(PIECES)]
    cells_of = [(x, slice(None), pl.ds(z, length)) for x, z in pieces]
    last_sems = [
        ([send_sem2.at[5 * index + i] for i in range(5)], [recv_sem2.at[4 * index + i] for i in range(4)])
        for index in range(len(pieces))
    ]
    for x in range(halves):
        for copy in partial[x]:
            copy.wait_recv()
        border_rows(x)
        along_y(pw.at[1, :, :, inner], x, True)
        finish(1, x, send2)
        for index, (x_of, z) in enumerate(pieces):
            if x_of == x:
                direct(send2, recv2, *last_sems[index], cells_of[index])

    for x in range(halves):
        keep_weights(x)
    for x in range(halves):
        collect(0, recv1, *first_sems[x], (x,), (x,), 0, zs)
    for index, (x, z) in enumerate(pieces):
        collect(1, recv2, *last_sems[index], cells_of[index], (x,), z, length)
        if index:
            image(*pieces[index - 1], length)
    image(*pieces[-1], length)

    for copy in coefs + sum([list(c) for c in halo + partial], []):
        copy.wait_send()
    for x in range(halves):
        sent(send1, recv1, *first_sems[x], (x,))
    for index in range(len(pieces)):
        sent(send2, recv2, *last_sems[index], cells_of[index])


def per_device(
    source_now, source_before, receiver_now, receiver_before, speed_term, aniso_field, tilt_field,
    angle_bins, weight_table, offset_lags, source_cells, source_wavelet, receiver_cells, receiver_traces,
):
    zs, rows, width = source_now.shape
    halves = width // LANES
    steps = source_wavelet.shape[0]
    n_off, n_bin, n_ang = weight_table.shape
    n_src = source_cells.shape[0]
    receivers = receiver_cells.shape[0]
    assert rows == ROWS and n_bin == ROWS and width & (width - 1) == 0
    half = (halves, zs, ROWS, LANES)
    block = (halves, 2, zs, ROWS, LANES)
    any_space = pl.BlockSpec(memory_space=pl.ANY)
    dma = pltpu.SemaphoreType.DMA
    in_specs = [any_space] * 14
    return pl.pallas_call(
        kernel,
        out_shape=pltpu.VMEM((n_ang, zs, rows, width), BF16),
        in_specs=in_specs,
        out_specs=pl.BlockSpec(memory_space=pltpu.VMEM),
        scratch_shapes=[
            pltpu.VMEM((steps, 2, halves, zs + 2 * PAD, 3 * ROWS, LANES), F32),
            pltpu.VMEM((2,) + half, F32),
            pltpu.VMEM(half, F32),
            pltpu.VMEM(half, F32),
            pltpu.VMEM(half, F32),
            pltpu.VMEM(half, jnp.int32),
            pltpu.VMEM((n_bin, n_ang, n_off), BF16),
            pltpu.SMEM((n_off,), jnp.int32),
            pltpu.SMEM((n_src,), jnp.int32),
            pltpu.SMEM((steps, n_src), F32),
            pltpu.VMEM((receivers // LANES, LANES), jnp.int32),
            pltpu.VMEM((steps, receivers), F32),
            pltpu.VMEM((n_off, n_ang, n_bin, LANES), F32),
            pltpu.VMEM((n_off, KEPT) + half, F32),
            pltpu.VMEM((steps, 2, halves, ROWS, LANES), F32),
            pltpu.VMEM((2,) + half, F32),
            pltpu.VMEM((2, halves, zs + 2 * PAD, ROWS, LANES), F32),
            pltpu.VMEM((2, halves, zs, 3 * ROWS, LANES), F32),
            pltpu.VMEM((2,) + half, F32),
            pltpu.VMEM((2, halves, zs + 2 * PAD, ROWS, LANES), F32),
            pltpu.VMEM(block, BF16),
            pltpu.VMEM(block, BF16),
            pltpu.VMEM(block, BF16),
            pltpu.VMEM(block, BF16),
            pltpu.VMEM(block, BF16),
            pltpu.VMEM(block, BF16),
            pltpu.VMEM((2,) + half, BF16),
            pltpu.VMEM(block, BF16),
            pltpu.VMEM((4,) + block, BF16),
            pltpu.VMEM((4,) + block, BF16),
            pltpu.VMEM((steps, 2, halves, zs, 5 * ROWS, LANES), F32),
            dma((8 * halves + 6,)),
            pltpu.SemaphoreType.REGULAR,
            dma((2 * halves,)),
            dma((2 * halves,)),
            dma((2,)),
            dma((2,)),
            dma((2 * halves,)),
            dma((2 * halves,)),
            dma((5 * halves,)),
            dma((4 * halves,)),
            dma((5 * halves * PIECES,)),
            dma((4 * halves * PIECES,)),
        ],
        compiler_params=pltpu.CompilerParams(collective_id=0, has_side_effects=True),
    )(
        source_now, source_before, receiver_now, receiver_before, speed_term, aniso_field, tilt_field,
        angle_bins, jnp.transpose(weight_table, (1, 2, 0)), offset_lags, source_cells, source_wavelet,
        receiver_cells.reshape(receivers // LANES, LANES), receiver_traces,
    )


def solution(mesh):
    return jax.shard_map(
        per_device,
        mesh=mesh,
        in_specs=(
            P("shot", "gy", None),
            P("shot", "gy", None),
            P("shot", "gy", None),
            P("shot", "gy", None),
            P(None, "gy", None),
            P(None, "gy", None),
            P(None, "gy", None),
            P(None, "gy", None),
            P(),
            P(),
            P("shot"),
            P("shot", None),
            P("shot"),
            P("shot", None),
        ),
        out_specs=P("shot", None, "gy", None),
        check_vma=False,
    )
```

```python
import functools

import jax
import jax.numpy as jnp
from jax import lax
from jax.experimental import pallas as pl
from jax.experimental.pallas import tpu as pltpu
from jax.sharding import PartitionSpec as P

SECOND_COEF = (-205.0 / 72.0, 8.0 / 5.0, -1.0 / 5.0, 8.0 / 315.0, -1.0 / 560.0)
FIRST_COEF = (4.0 / 5.0, -1.0 / 5.0, 4.0 / 105.0, -1.0 / 280.0)
MESH = pl.DeviceIdType.MESH
F32 = jnp.float32
BF16 = jnp.bfloat16
LANES = 128
ROWS = 8
PAD = 4
LO, HI = 0, 1
OFFSETS = (-2, -1, 1, 2)
DIRECT = ((2, -1, 1), (2, -2, -1))
PASSED = ((1, 2), (-2, -1))
GROUP = 8
KEPT = 4
PIECES = 1


def kernel(
    sn_hbm, sb_hbm, rn_hbm, rb_hbm, speed_hbm, aniso_hbm, tilt_hbm, bins_hbm, wt_hbm,
    lags_hbm, scells_hbm, swave_hbm, rcells_hbm, rtraces_hbm,
    out,
    pw, qv, speed, a1, a2, bins, wt, lags, scells, swave, rcells, rtraces, table, cache, inj, base, grad,
    hw, share2, share1, send0, sendc, sendp, send1, send2, recv0, recvc, recvp, recv1, recv2, win,
    in_sem, send_sem0, recv_sem0, send_semc, recv_semc, send_semp, recv_semp, recv_sem1, recv_sem2,
):
    n = lax.axis_size("gy")
    me = lax.axis_index("gy")
    peer = {d: lax.rem(me + (d + n), n) for d in OFFSETS}
    odd = lax.rem(me, 2) == 1
    zs = sn_hbm.shape[0]
    halves = sn_hbm.shape[2] // LANES
    n_bin, n_ang, n_off = wt_hbm.shape
    kept = cache.shape[1]
    steps = swave.shape[0]
    n_src = scells.shape[0]
    rec_rows = rcells_hbm.shape[0]
    own = pl.ds(ROWS, ROWS)
    inner = pl.ds(PAD, zs)

    barrier = pltpu.get_barrier_semaphore()
    for d in OFFSETS:
        pl.semaphore_signal(barrier, inc=1, device_id={"gy": peer[d]}, device_id_type=MESH)

    copies = {}

    def fetch(name, index, src, dst):
        copy = pltpu.make_async_copy(src, dst, in_sem.at[index])
        copy.start()
        copies[name] = copy

    wanted = [
        (("now", m, x), ref.at[:, :, pl.ds(x * LANES, LANES)], pw.at[0, m, x, inner, own, :])
        for x in range(halves)
        for m, ref in enumerate((sn_hbm, rn_hbm))
    ]
    wanted += [("rcells", rcells_hbm, rcells), ("rtraces", rtraces_hbm, rtraces)]
    wanted += [("scells", scells_hbm, scells), ("swave", swave_hbm, swave)]
    for name, ref, dst in (("speed", speed_hbm, speed), ("aniso", aniso_hbm, a1), ("tilt", tilt_hbm, a2)):
        wanted += [((name, x), ref.at[:, :, pl.ds(x * LANES, LANES)], dst.at[x]) for x in range(halves)]
    for m, ref in enumerate((sb_hbm, rb_hbm)):
        wanted += [(("before", m, x), ref.at[:, :, pl.ds(x * LANES, LANES)], qv.at[m, x]) for x in range(halves)]
    wanted += [(("bins", x), bins_hbm.at[:, :, pl.ds(x * LANES, LANES)], bins.at[x]) for x in range(halves)]
    wanted += [("wt", wt_hbm, wt), ("lags", lags_hbm, lags)]
    for index, (name, src, dst) in enumerate(wanted):
        fetch(name, index, src, dst)

    edge = jnp.zeros((PAD, ROWS, LANES), F32)
    plane = jnp.zeros((zs, ROWS, LANES), F32)
    for x in range(halves):
        for m in range(2):
            for s in range(steps):
                pw[s, m, x, pl.ds(0, PAD), own, :] = edge
                pw[s, m, x, pl.ds(PAD + zs, PAD), own, :] = edge
            pw[0, m, x, inner, pl.ds(0, ROWS), :] = plane
            pw[0, m, x, inner, pl.ds(2 * ROWS, ROWS), :] = plane
            hw[m, x, :, own, :] = plane
            for padded in (grad, share1):
                padded[m, x, pl.ds(0, PAD)] = edge
                padded[m, x, pl.ds(PAD + zs, PAD)] = edge

    sub = lax.broadcasted_iota(jnp.int32, (ROWS, LANES), 0)
    lane = lax.broadcasted_iota(jnp.int32, (ROWS, LANES), 1)
    low_rows = sub < PAD

    def turn(v):
        return pltpu.roll(v, PAD, axis=v.ndim - 2)

    def pack(source, receiver, send, x, where_z):
        send[x, LO, where_z] = jnp.where(low_rows, source, turn(receiver)).astype(BF16)
        send[x, HI, where_z] = jnp.where(low_rows, turn(source), receiver).astype(BF16)

    def remote(src, dst, ssem, rsem, device):
        return pltpu.make_async_remote_copy(
            src_ref=src, dst_ref=dst, send_sem=ssem, recv_sem=rsem, device_id={"gy": device}, device_id_type=MESH
        )

    shift_bits = (halves * LANES).bit_length() - 1

    def injections():
        first_row = me * ROWS
        for name in ("rcells", "rtraces", "scells", "swave"):
            copies[name].wait()
        left, right = [], []
        col_iota = lax.broadcasted_iota(jnp.int32, (halves * LANES, LANES), 0)
        for c in range(rec_rows):
            cell = rcells[c : c + 1, :]
            row = lax.shift_right_logical(cell, shift_bits) - first_row
            col = jnp.bitwise_and(cell, halves * LANES - 1)
            hit = jnp.broadcast_to(row, (ROWS, LANES)) == sub
            parts = []
            for s in range(steps):
                amount = jnp.broadcast_to(rtraces[s : s + 1, c * LANES : (c + 1) * LANES], (ROWS, LANES))
                amount = jnp.where(hit, amount, 0.0)
                coarse = amount.astype(BF16).astype(F32)
                parts += [coarse, amount - coarse]
            left.append(jnp.concatenate(parts, axis=0).astype(BF16))
            right.append(jnp.where(jnp.broadcast_to(col, col_iota.shape) == col_iota, 1.0, 0.0).astype(BF16))
        spread = lax.dot_general(
            jnp.concatenate(left, axis=1),
            jnp.concatenate(right, axis=1),
            (((1,), (1,)), ((), ())),
            preferred_element_type=F32,
        )
        for s in range(steps):
            total = spread[2 * s * ROWS : (2 * s + 1) * ROWS] + spread[(2 * s + 1) * ROWS : (2 * s + 2) * ROWS]
            for x in range(halves):
                inj[s, 1, x] = total[:, x * LANES : (x + 1) * LANES]
        for s in range(steps):
            for x in range(halves):
                total = jnp.zeros((ROWS, LANES), F32)
                for i in range(n_src):
                    cell = scells[i]
                    row = lax.shift_right_logical(cell, shift_bits) - first_row
                    col = jnp.bitwise_and(cell, halves * LANES - 1) - x * LANES
                    total = total + jnp.where((sub == row) & (lane == col), swave[s, i], 0.0)
                inj[s, 0, x] = total

    halo = [
        (
            remote(send0.at[x, HI], recv0.at[x, 0], send_sem0.at[2 * x], recv_sem0.at[2 * x], peer[1]),
            remote(send0.at[x, LO], recv0.at[x, 1], send_sem0.at[2 * x + 1], recv_sem0.at[2 * x + 1], peer[-1]),
        )
        for x in range(halves)
    ]
    for x in range(halves):
        for m in range(2):
            copies[("now", m, x)].wait()
        pack(pw[0, 0, x, inner, own, :], pw[0, 1, x, inner, own, :], send0, x, pl.ds(0, zs))
        if x == 0:
            pl.semaphore_wait(barrier, len(OFFSETS))
        for copy in halo[x]:
            copy.start()

    def local_part(step):
        chunk = 4

        def part(i, carry):
            z = i * chunk
            for m in range(2):
                f = [pw[step, m, x, pl.ds(PAD + z, chunk), own, :] for x in range(halves)]
                first = [jnp.zeros_like(v) for v in f]
                second = [SECOND_COEF[0] * v for v in f]
                for k in range(1, PAD + 1):
                    up = [pltpu.roll(v, LANES - k, axis=2) for v in f] + [jnp.zeros_like(f[0])]
                    down = [jnp.zeros_like(f[0])] + [pltpu.roll(v, k, axis=2) for v in f]
                    for x in range(halves):
                        above = jnp.where(lane < LANES - k, up[x], up[x + 1])
                        below = jnp.where(lane >= k, down[x + 1], down[x])
                        second[x] = second[x] + SECOND_COEF[k] * (above + below)
                        first[x] = first[x] + FIRST_COEF[k - 1] * (above - below)
                for x in range(halves):
                    grad[m, x, pl.ds(PAD + z, chunk)] = first[x]
                    along_z = SECOND_COEF[0] * f[x]
                    for k in range(1, PAD + 1):
                        along_z = along_z + SECOND_COEF[k] * (
                            pw[step, m, x, pl.ds(PAD + z + k, chunk), own, :]
                            + pw[step, m, x, pl.ds(PAD + z - k, chunk), own, :]
                        )
                    before = qv[m, x, pl.ds(z, chunk)] if step == 0 else pw[step - 1, m, x, pl.ds(PAD + z, chunk), own, :]
                    base[m, x, pl.ds(z, chunk)] = (
                        2.0 * f[x]
                        - before
                        + a1[x, pl.ds(z, chunk)] * second[x]
                        + speed[x, pl.ds(z, chunk)] * along_z
                    )
            return carry

        lax.fori_loop(0, zs // chunk, part, 0)
        for m in range(2):
            for x in range(halves):
                base[m, x, 0] = base[m, x, 0] + inj[step, m, x]

    def halo_rows(window, x, low, high):
        window[0, x, :, pl.ds(0, ROWS), :] = turn(low)
        window[1, x, :, pl.ds(0, ROWS), :] = low
        window[0, x, :, pl.ds(2 * ROWS, ROWS), :] = high
        window[1, x, :, pl.ds(2 * ROWS, ROWS), :] = turn(high)

    part_chunk = 4

    def along_y(window, x, whole):
        def part(i, carry):
            z = i * part_chunk
            cells = pl.ds(z, part_chunk)
            for m in range(2):

                def rows(k):
                    return window[m, x, cells, pl.ds(ROWS + k, ROWS), :]

                second, first = 0.0, 0.0
                if whole:
                    second, first = SECOND_COEF[0] * rows(0), grad[m, x, pl.ds(PAD + z, part_chunk)]
                for k in range(1, PAD + 1):
                    above, below = rows(k), rows(-k)
                    second = second + SECOND_COEF[k] * (above + below)
                    first = first + FIRST_COEF[k - 1] * (above - below)
                grad[m, x, pl.ds(PAD + z, part_chunk)] = first
                base[m, x, cells] = base[m, x, cells] + a1[x, cells] * second
            return carry

        lax.fori_loop(0, zs // part_chunk, part, 0)

    def along_z(padded, member, x, z):
        mixed = jnp.zeros((part_chunk, ROWS, LANES), F32)
        for k in range(1, PAD + 1):
            mixed = mixed + FIRST_COEF[k - 1] * (
                padded[member, x, pl.ds(PAD + z + k, part_chunk)] - padded[member, x, pl.ds(PAD + z - k, part_chunk)]
            )
        return mixed

    def finish(step, x, send, whole=True):
        def part(i, carry):
            z = i * part_chunk
            cells = pl.ds(z, part_chunk)
            new = []
            for m in range(2):
                value = base[m, x, cells] + a2[x, cells] * along_z(grad, m, x, z)
                new.append(value)
                if not whole:
                    base[m, x, cells] = value
                    continue
                if step + 1 < steps:
                    pw[step + 1, m, x, pl.ds(PAD + z, part_chunk), own, :] = value
                win[step, m, x, cells, pl.ds(2 * ROWS, ROWS), :] = value.astype(BF16).astype(F32)
            pack(new[0], new[1], send, x, cells)
            return carry

        lax.fori_loop(0, zs // part_chunk, part, 0)

    def shares(x):
        def part(i, carry):
            z = i * part_chunk
            for side in range(2):
                second, first = [], []
                for m in range(2):
                    two, one = 0.0, 0.0
                    for k in range(1, PAD + 1):
                        row = ROWS - PAD + k if side == 0 else 2 * ROWS - k
                        value = pw[0, m, x, pl.ds(PAD + z, part_chunk), pl.ds(row, ROWS), :]
                        two = two + SECOND_COEF[k] * value
                        one = one + (FIRST_COEF[k - 1] if side == 0 else -FIRST_COEF[k - 1]) * value
                    second.append(two)
                    first.append(one)
                share2[side, x, pl.ds(z, part_chunk)] = jnp.where(low_rows, second[0], turn(second[1]))
                share1[side, x, pl.ds(PAD + z, part_chunk)] = jnp.where(low_rows, first[0], turn(first[1]))
            return carry

        lax.fori_loop(0, zs // part_chunk, part, 0)

    def border_rows(x):
        whole = []
        for side in range(2):
            blocks = []
            for z in range(0, zs, part_chunk):
                cells = pl.ds(z, part_chunk)
                pair = recvc[side, x, cells].astype(F32)
                flat, tilted = jnp.where(low_rows, pair, turn(pair)), jnp.where(low_rows, turn(pair), pair)
                blocks.append(
                    recvp[x, side, cells].astype(F32)
                    + flat * share2[side, x, cells]
                    + tilted * along_z(share1, side, x, z)
                )
            whole.append(jnp.concatenate(blocks, axis=0))
        halo_rows(pw.at[1, :, :, inner], x, whole[0], whole[1])

    def open_block(step, d, recv, x, z, length):
        cells = pl.ds(z, length)
        rows = pl.ds((2 + d) * ROWS, ROWS)
        slot = OFFSETS.index(d)
        low = recv[slot, x, LO, cells].astype(F32)
        high = recv[slot, x, HI, cells].astype(F32)
        win[step, 0, x, cells, rows, :] = jnp.where(low_rows, low, turn(high))
        win[step, 1, x, cells, rows, :] = jnp.where(low_rows, turn(low), high)

    chunk = 4

    def gathered(h, a, bin_ids):
        row = table[h, a]
        return jnp.stack([jnp.take_along_axis(row, ids, axis=0) for ids in bin_ids])

    def keep_weights(x):
        def part(i, carry):
            z = i * chunk
            bin_ids = [bins[x, z + j] for j in range(chunk)]
            for h in range(n_off):
                for a in range(kept):
                    cache[h, a, x, pl.ds(z, chunk)] = gathered(h, a, bin_ids)
            return carry

        lax.fori_loop(0, zs // chunk, part, 0)

    def image(x, start, length):
        def part(i, carry):
            z = start + i * chunk
            bin_ids = [bins[x, z + j] for j in range(chunk)]
            def lag_group(g, total):
                total = list(total)
                for j in range(GROUP):
                    h = g * GROUP + j
                    lag = lags[h]
                    product = 0.0
                    for step in range(steps):
                        product = product + (
                            win[step, 0, x, pl.ds(z, chunk), pl.ds(2 * ROWS - lag, ROWS), :]
                            * win[step, 1, x, pl.ds(z, chunk), pl.ds(2 * ROWS + lag, ROWS), :]
                        )
                    for a in range(n_ang):
                        weight = cache[h, a, x, pl.ds(z, chunk)] if a < kept else gathered(h, a, bin_ids)
                        total[a] = total[a] + weight * product
                return tuple(total)

            total = lax.fori_loop(0, n_off // GROUP, lag_group, (jnp.zeros((chunk, ROWS, LANES), F32),) * n_ang)
            for a in range(n_ang):
                out[a, pl.ds(z, chunk), :, x * LANES : (x + 1) * LANES] = total[a].astype(BF16)
            return carry

        lax.fori_loop(0, length // chunk, part, 0)

    injections()
    for x in range(halves):
        copies[("speed", x)].wait()
        copies[("aniso", x)].wait()
        copies[("tilt", x)].wait()
        a1[x] = speed[x] * (1.0 + 2.0 * a1[x])
        a2[x] = speed[x] * a2[x]
        pack(a1[x], a2[x], sendc, x, pl.ds(0, zs))
    coefs = [
        remote(sendc.at[:, half], recvc.at[i], send_semc.at[i], recv_semc.at[i], peer[d])
        for i, (half, d) in enumerate(((HI, 1), (LO, -1)))
    ]
    for copy in coefs:
        copy.start()
    for m in range(2):
        for x in range(halves):
            copies[("before", m, x)].wait()
    local_part(0)
    partial = []
    for x in range(halves):
        along_y(pw.at[0, :, :, inner], x, True)
        finish(0, x, sendp, whole=False)
        partial.append(
            [
                remote(sendp.at[x, half], recvp.at[x, i], send_semp.at[2 * x + i], recv_semp.at[2 * x + i], peer[d])
                for i, (half, d) in enumerate(((HI, 1), (LO, -1)))
            ]
        )
        for copy in partial[x]:
            copy.start()
    for x in range(halves):
        shares(x)
    copies["wt"].wait()
    copies["lags"].wait()
    by_bin = [wt[b].astype(F32) for b in range(n_bin)]
    for a in range(n_ang):
        rows = jnp.concatenate([v[a : a + 1] for v in by_bin], axis=0)
        for h in range(n_off):
            table[h, a] = jnp.broadcast_to(rows[:, h : h + 1], (n_bin, LANES))
    for x in range(halves):
        copies[("bins", x)].wait()

    def direct(send, recv, send_sems, recv_sems, cells):
        for parity, here in enumerate((jnp.logical_not(odd), odd)):

            @pl.when(here)
            def _():
                for i, d in enumerate(DIRECT[parity]):
                    slot = OFFSETS.index(-d)
                    remote(send.at[cells], recv.at[(slot,) + cells], send_sems[i], recv_sems[slot], peer[d]).start()

    def passed(recv, send_sems, recv_sems, cells, index):
        here, there = (OFFSETS.index(d) for d in PASSED[index])
        return remote(recv.at[(here,) + cells], recv.at[(there,) + cells], send_sems[index], recv_sems[there], peer[-1])

    def collect(step, recv, send_sems, recv_sems, cells, x_list, z, length):
        for d in (1, -2, -1, 2):
            slot = OFFSETS.index(d)
            remote(recv.at[(slot,) + cells], recv.at[(slot,) + cells], send_sems[0], recv_sems[slot], peer[1]).wait_recv()
            for index, (source, _) in enumerate(PASSED):
                if source == d:

                    @pl.when(odd)
                    def _():
                        passed(recv, send_sems[3:], recv_sems, cells, index).start()

        for d in OFFSETS:
            for x in x_list:
                open_block(step, d, recv, x, z, length)

    def sent(send, recv, send_sems, recv_sems, cells):
        for i in range(3):
            remote(send.at[cells], recv.at[(0,) + cells], send_sems[i], recv_sems[0], peer[1]).wait_send()

        @pl.when(odd)
        def _():
            for index in range(len(PASSED)):
                passed(recv, send_sems[3:], recv_sems, cells, index).wait_send()

    first_sems = [
        ([in_sem.at[5 * x + i] for i in range(5)], [recv_sem1.at[4 * x + i] for i in range(4)]) for x in range(halves)
    ]

    for x in range(halves):
        for copy in halo[x]:
            copy.wait_recv()
        halo_rows(hw, x, recv0[x, 0].astype(F32), recv0[x, 1].astype(F32))
        along_y(hw, x, False)
        finish(0, x, send1)
        direct(send1, recv1, *first_sems[x], (x,))
    local_part(1)
    for copy in coefs:
        copy.wait_recv()
    length = zs // PIECES
    pieces = [(x, p * length) for x in range(halves) for p in range(PIECES)]
    cells_of = [(x, slice(None), pl.ds(z, length)) for x, z in pieces]
    last_sems = [
        ([in_sem.at[5 * (halves + index) + i] for i in range(5)], [recv_sem2.at[4 * index + i] for i in range(4)])
        for index in range(len(pieces))
    ]
    for x in range(halves):
        for copy in partial[x]:
            copy.wait_recv()
        border_rows(x)
        along_y(pw.at[1, :, :, inner], x, True)
        finish(1, x, send2)
        for index, (x_of, z) in enumerate(pieces):
            if x_of == x:
                direct(send2, recv2, *last_sems[index], cells_of[index])

    for x in range(halves):
        keep_weights(x)
    for x in range(halves):
        collect(0, recv1, *first_sems[x], (x,), (x,), 0, zs)
    for index, (x, z) in enumerate(pieces):
        collect(1, recv2, *last_sems[index], cells_of[index], (x,), z, length)
        image(x, z, length)

    for copy in coefs + sum([list(c) for c in halo + partial], []):
        copy.wait_send()
    for x in range(halves):
        sent(send1, recv1, *first_sems[x], (x,))
    for index in range(len(pieces)):
        sent(send2, recv2, *last_sems[index], cells_of[index])


def per_device(
    source_now, source_before, receiver_now, receiver_before, speed_term, aniso_field, tilt_field,
    angle_bins, weight_table, offset_lags, source_cells, source_wavelet, receiver_cells, receiver_traces,
):
    zs, rows, width = source_now.shape
    halves = width // LANES
    steps = source_wavelet.shape[0]
    n_off, n_bin, n_ang = weight_table.shape
    n_src = source_cells.shape[0]
    receivers = receiver_cells.shape[0]
    assert rows == ROWS and n_bin == ROWS and width & (width - 1) == 0
    half = (halves, zs, ROWS, LANES)
    block = (halves, 2, zs, ROWS, LANES)
    any_space = pl.BlockSpec(memory_space=pl.ANY)
    dma = pltpu.SemaphoreType.DMA
    in_specs = [any_space] * 14
    return pl.pallas_call(
        kernel,
        out_shape=pltpu.VMEM((n_ang, zs, rows, width), BF16),
        in_specs=in_specs,
        out_specs=pl.BlockSpec(memory_space=pltpu.VMEM),
        scratch_shapes=[
            pltpu.VMEM((steps, 2, halves, zs + 2 * PAD, 3 * ROWS, LANES), F32),
            pltpu.VMEM((2,) + half, F32),
            pltpu.VMEM(half, F32),
            pltpu.VMEM(half, F32),
            pltpu.VMEM(half, F32),
            pltpu.VMEM(half, jnp.int32),
            pltpu.VMEM((n_bin, n_ang, n_off), BF16),
            pltpu.SMEM((n_off,), jnp.int32),
            pltpu.SMEM((n_src,), jnp.int32),
            pltpu.SMEM((steps, n_src), F32),
            pltpu.VMEM((receivers // LANES, LANES), jnp.int32),
            pltpu.VMEM((steps, receivers), F32),
            pltpu.VMEM((n_off, n_ang, n_bin, LANES), F32),
            pltpu.VMEM((n_off, KEPT) + half, F32),
            pltpu.VMEM((steps, 2, halves, ROWS, LANES), F32),
            pltpu.VMEM((2,) + half, F32),
            pltpu.VMEM((2, halves, zs + 2 * PAD, ROWS, LANES), F32),
            pltpu.VMEM((2, halves, zs, 3 * ROWS, LANES), F32),
            pltpu.VMEM((2,) + half, F32),
            pltpu.VMEM((2, halves, zs + 2 * PAD, ROWS, LANES), F32),
            pltpu.VMEM(block, BF16),
            pltpu.VMEM(block, BF16),
            pltpu.VMEM(block, BF16),
            pltpu.VMEM(block, BF16),
            pltpu.VMEM(block, BF16),
            pltpu.VMEM(block, BF16),
            pltpu.VMEM((2,) + half, BF16),
            pltpu.VMEM(block, BF16),
            pltpu.VMEM((4,) + block, BF16),
            pltpu.VMEM((4,) + block, BF16),
            pltpu.VMEM((steps, 2, halves, zs, 5 * ROWS, LANES), F32),
            dma((8 * halves + 6,)),
            dma((2 * halves,)),
            dma((2 * halves,)),
            dma((2,)),
            dma((2,)),
            dma((2 * halves,)),
            dma((2 * halves,)),
            dma((4 * halves,)),
            dma((4 * halves * PIECES,)),
        ],
        compiler_params=pltpu.CompilerParams(collective_id=0, has_side_effects=True),
    )(
        source_now, source_before, receiver_now, receiver_before, speed_term, aniso_field, tilt_field,
        angle_bins, jnp.transpose(weight_table, (1, 2, 0)), offset_lags, source_cells, source_wavelet,
        receiver_cells.reshape(receivers // LANES, LANES), receiver_traces,
    )


def solution(mesh):
    return jax.shard_map(
        per_device,
        mesh=mesh,
        in_specs=(
            P("shot", "gy", None),
            P("shot", "gy", None),
            P("shot", "gy", None),
            P("shot", "gy", None),
            P(None, "gy", None),
            P(None, "gy", None),
            P(None, "gy", None),
            P(None, "gy", None),
            P(),
            P(),
            P("shot"),
            P("shot", None),
            P("shot"),
            P("shot", None),
        ),
        out_specs=P("shot", None, "gy", None),
        check_vma=False,
    )
```

```python
import functools

import jax
import jax.numpy as jnp
from jax import lax
from jax.experimental import pallas as pl
from jax.experimental.pallas import tpu as pltpu
from jax.sharding import PartitionSpec as P

SECOND_COEF = (-205.0 / 72.0, 8.0 / 5.0, -1.0 / 5.0, 8.0 / 315.0, -1.0 / 560.0)
FIRST_COEF = (4.0 / 5.0, -1.0 / 5.0, 4.0 / 105.0, -1.0 / 280.0)
MESH = pl.DeviceIdType.MESH
F32 = jnp.float32
BF16 = jnp.bfloat16
LANES = 128
ROWS = 8
PAD = 4
LO, HI = 0, 1
OFFSETS = (-2, -1, 1, 2)
DIRECT = ((2, -1, 1), (2, -2, -1))
PASSED = ((1, 2), (-2, -1))
GROUP = 8
KEPT = 4
PIECES = 1


def kernel(
    sn_hbm, sb_hbm, rn_hbm, rb_hbm, speed_hbm, aniso_hbm, tilt_hbm, bins_hbm, wt_hbm,
    lags_hbm, scells_hbm, swave_hbm, rcells_hbm, rtraces_hbm,
    out,
    pw, qv, speed, a1, a2, bins, wt, lags, scells, swave, rcells, rtraces, table, cache, inj, base, grad,
    hw, share2, share1, send0, sendc, sendp, send1, send2, recv0, recvc, recvp, recv1, recv2, win, acc,
    in_sem, send_sem0, recv_sem0, send_semc, recv_semc, send_semp, recv_semp, recv_sem1, recv_sem2,
):
    n = lax.axis_size("gy")
    me = lax.axis_index("gy")
    peer = {d: lax.rem(me + (d + n), n) for d in OFFSETS}
    odd = lax.rem(me, 2) == 1
    zs = sn_hbm.shape[0]
    halves = sn_hbm.shape[2] // LANES
    n_bin, n_ang, n_off = wt_hbm.shape
    kept = cache.shape[1]
    steps = swave.shape[0]
    n_src = scells.shape[0]
    rec_rows = rcells_hbm.shape[0]
    own = pl.ds(ROWS, ROWS)
    inner = pl.ds(PAD, zs)

    barrier = pltpu.get_barrier_semaphore()
    for d in OFFSETS:
        pl.semaphore_signal(barrier, inc=1, device_id={"gy": peer[d]}, device_id_type=MESH)

    copies = {}

    def fetch(name, index, src, dst):
        copy = pltpu.make_async_copy(src, dst, in_sem.at[index])
        copy.start()
        copies[name] = copy

    wanted = [
        (("now", m, x), ref.at[:, :, pl.ds(x * LANES, LANES)], pw.at[0, m, x, inner, own, :])
        for x in range(halves)
        for m, ref in enumerate((sn_hbm, rn_hbm))
    ]
    wanted += [("rcells", rcells_hbm, rcells), ("rtraces", rtraces_hbm, rtraces)]
    wanted += [("scells", scells_hbm, scells), ("swave", swave_hbm, swave)]
    for name, ref, dst in (("speed", speed_hbm, speed), ("aniso", aniso_hbm, a1), ("tilt", tilt_hbm, a2)):
        wanted += [((name, x), ref.at[:, :, pl.ds(x * LANES, LANES)], dst.at[x]) for x in range(halves)]
    for m, ref in enumerate((sb_hbm, rb_hbm)):
        wanted += [(("before", m, x), ref.at[:, :, pl.ds(x * LANES, LANES)], qv.at[m, x]) for x in range(halves)]
    wanted += [(("bins", x), bins_hbm.at[:, :, pl.ds(x * LANES, LANES)], bins.at[x]) for x in range(halves)]
    wanted += [("wt", wt_hbm, wt), ("lags", lags_hbm, lags)]
    for index, (name, src, dst) in enumerate(wanted):
        fetch(name, index, src, dst)

    edge = jnp.zeros((PAD, ROWS, LANES), F32)
    plane = jnp.zeros((zs, ROWS, LANES), F32)
    for x in range(halves):
        for m in range(2):
            for s in range(steps):
                pw[s, m, x, pl.ds(0, PAD), own, :] = edge
                pw[s, m, x, pl.ds(PAD + zs, PAD), own, :] = edge
            pw[0, m, x, inner, pl.ds(0, ROWS), :] = plane
            pw[0, m, x, inner, pl.ds(2 * ROWS, ROWS), :] = plane
            hw[m, x, :, own, :] = plane
            for padded in (grad, share1):
                padded[m, x, pl.ds(0, PAD)] = edge
                padded[m, x, pl.ds(PAD + zs, PAD)] = edge

    sub = lax.broadcasted_iota(jnp.int32, (ROWS, LANES), 0)
    lane = lax.broadcasted_iota(jnp.int32, (ROWS, LANES), 1)
    low_rows = sub < PAD

    def turn(v):
        return pltpu.roll(v, PAD, axis=v.ndim - 2)

    def pack(source, receiver, send, x, where_z):
        send[x, LO, where_z] = jnp.where(low_rows, source, turn(receiver)).astype(BF16)
        send[x, HI, where_z] = jnp.where(low_rows, turn(source), receiver).astype(BF16)

    def remote(src, dst, ssem, rsem, device):
        return pltpu.make_async_remote_copy(
            src_ref=src, dst_ref=dst, send_sem=ssem, recv_sem=rsem, device_id={"gy": device}, device_id_type=MESH
        )

    shift_bits = (halves * LANES).bit_length() - 1

    def injections():
        first_row = me * ROWS
        for name in ("rcells", "rtraces", "scells", "swave"):
            copies[name].wait()
        left, right = [], []
        col_iota = lax.broadcasted_iota(jnp.int32, (halves * LANES, LANES), 0)
        for c in range(rec_rows):
            cell = rcells[c : c + 1, :]
            row = lax.shift_right_logical(cell, shift_bits) - first_row
            col = jnp.bitwise_and(cell, halves * LANES - 1)
            hit = jnp.broadcast_to(row, (ROWS, LANES)) == sub
            parts = []
            for s in range(steps):
                amount = jnp.broadcast_to(rtraces[s : s + 1, c * LANES : (c + 1) * LANES], (ROWS, LANES))
                amount = jnp.where(hit, amount, 0.0)
                coarse = amount.astype(BF16).astype(F32)
                parts += [coarse, amount - coarse]
            left.append(jnp.concatenate(parts, axis=0).astype(BF16))
            right.append(jnp.where(jnp.broadcast_to(col, col_iota.shape) == col_iota, 1.0, 0.0).astype(BF16))
        spread = lax.dot_general(
            jnp.concatenate(left, axis=1),
            jnp.concatenate(right, axis=1),
            (((1,), (1,)), ((), ())),
            preferred_element_type=F32,
        )
        for s in range(steps):
            total = spread[2 * s * ROWS : (2 * s + 1) * ROWS] + spread[(2 * s + 1) * ROWS : (2 * s + 2) * ROWS]
            for x in range(halves):
                inj[s, 1, x] = total[:, x * LANES : (x + 1) * LANES]
        for s in range(steps):
            for x in range(halves):
                total = jnp.zeros((ROWS, LANES), F32)
                for i in range(n_src):
                    cell = scells[i]
                    row = lax.shift_right_logical(cell, shift_bits) - first_row
                    col = jnp.bitwise_and(cell, halves * LANES - 1) - x * LANES
                    total = total + jnp.where((sub == row) & (lane == col), swave[s, i], 0.0)
                inj[s, 0, x] = total

    halo = [
        (
            remote(send0.at[x, HI], recv0.at[x, 0], send_sem0.at[2 * x], recv_sem0.at[2 * x], peer[1]),
            remote(send0.at[x, LO], recv0.at[x, 1], send_sem0.at[2 * x + 1], recv_sem0.at[2 * x + 1], peer[-1]),
        )
        for x in range(halves)
    ]
    for x in range(halves):
        for m in range(2):
            copies[("now", m, x)].wait()
        pack(pw[0, 0, x, inner, own, :], pw[0, 1, x, inner, own, :], send0, x, pl.ds(0, zs))
        if x == 0:
            pl.semaphore_wait(barrier, len(OFFSETS))
        for copy in halo[x]:
            copy.start()

    def local_part(step):
        chunk = 4

        def part(i, carry):
            z = i * chunk
            for m in range(2):
                f = [pw[step, m, x, pl.ds(PAD + z, chunk), own, :] for x in range(halves)]
                first = [jnp.zeros_like(v) for v in f]
                second = [SECOND_COEF[0] * v for v in f]
                for k in range(1, PAD + 1):
                    up = [pltpu.roll(v, LANES - k, axis=2) for v in f] + [jnp.zeros_like(f[0])]
                    down = [jnp.zeros_like(f[0])] + [pltpu.roll(v, k, axis=2) for v in f]
                    for x in range(halves):
                        above = jnp.where(lane < LANES - k, up[x], up[x + 1])
                        below = jnp.where(lane >= k, down[x + 1], down[x])
                        second[x] = second[x] + SECOND_COEF[k] * (above + below)
                        first[x] = first[x] + FIRST_COEF[k - 1] * (above - below)
                for x in range(halves):
                    grad[m, x, pl.ds(PAD + z, chunk)] = first[x]
                    along_z = SECOND_COEF[0] * f[x]
                    for k in range(1, PAD + 1):
                        along_z = along_z + SECOND_COEF[k] * (
                            pw[step, m, x, pl.ds(PAD + z + k, chunk), own, :]
                            + pw[step, m, x, pl.ds(PAD + z - k, chunk), own, :]
                        )
                    before = qv[m, x, pl.ds(z, chunk)] if step == 0 else pw[step - 1, m, x, pl.ds(PAD + z, chunk), own, :]
                    base[m, x, pl.ds(z, chunk)] = (
                        2.0 * f[x]
                        - before
                        + a1[x, pl.ds(z, chunk)] * second[x]
                        + speed[x, pl.ds(z, chunk)] * along_z
                    )
            return carry

        lax.fori_loop(0, zs // chunk, part, 0)
        for m in range(2):
            for x in range(halves):
                base[m, x, 0] = base[m, x, 0] + inj[step, m, x]

    def halo_rows(window, x, low, high):
        window[0, x, :, pl.ds(0, ROWS), :] = turn(low)
        window[1, x, :, pl.ds(0, ROWS), :] = low
        window[0, x, :, pl.ds(2 * ROWS, ROWS), :] = high
        window[1, x, :, pl.ds(2 * ROWS, ROWS), :] = turn(high)

    part_chunk = 4

    def along_y(window, x, whole):
        def part(i, carry):
            z = i * part_chunk
            cells = pl.ds(z, part_chunk)
            for m in range(2):

                def rows(k):
                    return window[m, x, cells, pl.ds(ROWS + k, ROWS), :]

                second, first = 0.0, 0.0
                if whole:
                    second, first = SECOND_COEF[0] * rows(0), grad[m, x, pl.ds(PAD + z, part_chunk)]
                for k in range(1, PAD + 1):
                    above, below = rows(k), rows(-k)
                    second = second + SECOND_COEF[k] * (above + below)
                    first = first + FIRST_COEF[k - 1] * (above - below)
                grad[m, x, pl.ds(PAD + z, part_chunk)] = first
                base[m, x, cells] = base[m, x, cells] + a1[x, cells] * second
            return carry

        lax.fori_loop(0, zs // part_chunk, part, 0)

    def along_z(padded, member, x, z):
        mixed = jnp.zeros((part_chunk, ROWS, LANES), F32)
        for k in range(1, PAD + 1):
            mixed = mixed + FIRST_COEF[k - 1] * (
                padded[member, x, pl.ds(PAD + z + k, part_chunk)] - padded[member, x, pl.ds(PAD + z - k, part_chunk)]
            )
        return mixed

    def finish(step, x, send, whole=True):
        def part(i, carry):
            z = i * part_chunk
            cells = pl.ds(z, part_chunk)
            new = []
            for m in range(2):
                value = base[m, x, cells] + a2[x, cells] * along_z(grad, m, x, z)
                new.append(value)
                if not whole:
                    base[m, x, cells] = value
                    continue
                if step + 1 < steps:
                    pw[step + 1, m, x, pl.ds(PAD + z, part_chunk), own, :] = value
                win[step, m, x, cells, pl.ds(2 * ROWS, ROWS), :] = value.astype(BF16).astype(F32)
            pack(new[0], new[1], send, x, cells)
            return carry

        lax.fori_loop(0, zs // part_chunk, part, 0)

    def shares(x):
        def part(i, carry):
            z = i * part_chunk
            for side in range(2):
                second, first = [], []
                for m in range(2):
                    two, one = 0.0, 0.0
                    for k in range(1, PAD + 1):
                        row = ROWS - PAD + k if side == 0 else 2 * ROWS - k
                        value = pw[0, m, x, pl.ds(PAD + z, part_chunk), pl.ds(row, ROWS), :]
                        two = two + SECOND_COEF[k] * value
                        one = one + (FIRST_COEF[k - 1] if side == 0 else -FIRST_COEF[k - 1]) * value
                    second.append(two)
                    first.append(one)
                share2[side, x, pl.ds(z, part_chunk)] = jnp.where(low_rows, second[0], turn(second[1]))
                share1[side, x, pl.ds(PAD + z, part_chunk)] = jnp.where(low_rows, first[0], turn(first[1]))
            return carry

        lax.fori_loop(0, zs // part_chunk, part, 0)

    def border_rows(x):
        whole = []
        for side in range(2):
            blocks = []
            for z in range(0, zs, part_chunk):
                cells = pl.ds(z, part_chunk)
                pair = recvc[side, x, cells].astype(F32)
                flat, tilted = jnp.where(low_rows, pair, turn(pair)), jnp.where(low_rows, turn(pair), pair)
                blocks.append(
                    recvp[x, side, cells].astype(F32)
                    + flat * share2[side, x, cells]
                    + tilted * along_z(share1, side, x, z)
                )
            whole.append(jnp.concatenate(blocks, axis=0))
        halo_rows(pw.at[1, :, :, inner], x, whole[0], whole[1])

    def open_block(step, d, recv, x, z, length):
        cells = pl.ds(z, length)
        rows = pl.ds((2 + d) * ROWS, ROWS)
        slot = OFFSETS.index(d)
        low = recv[slot, x, LO, cells].astype(F32)
        high = recv[slot, x, HI, cells].astype(F32)
        win[step, 0, x, cells, rows, :] = jnp.where(low_rows, low, turn(high))
        win[step, 1, x, cells, rows, :] = jnp.where(low_rows, turn(low), high)

    chunk = 4

    def gathered(h, a, bin_ids):
        row = table[h, a]
        return jnp.stack([jnp.take_along_axis(row, ids, axis=0) for ids in bin_ids])

    def keep_weights(x):
        def part(i, carry):
            z = i * chunk
            bin_ids = [bins[x, z + j] for j in range(chunk)]
            for h in range(n_off):
                for a in range(kept):
                    cache[h, a, x, pl.ds(z, chunk)] = gathered(h, a, bin_ids)
            return carry

        lax.fori_loop(0, zs // chunk, part, 0)

    def image(step, x, start, length):
        def part(i, carry):
            z = start + i * chunk
            bin_ids = [bins[x, z + j] for j in range(chunk)]
            def lag_group(g, total):
                total = list(total)
                for j in range(GROUP):
                    h = g * GROUP + j
                    lag = lags[h]
                    product = (
                        win[step, 0, x, pl.ds(z, chunk), pl.ds(2 * ROWS - lag, ROWS), :]
                        * win[step, 1, x, pl.ds(z, chunk), pl.ds(2 * ROWS + lag, ROWS), :]
                    )
                    for a in range(n_ang):
                        weight = cache[h, a, x, pl.ds(z, chunk)] if a < kept else gathered(h, a, bin_ids)
                        total[a] = total[a] + weight * product
                return tuple(total)

            total = tuple(
                jnp.zeros((chunk, ROWS, LANES), F32) if step == 0 else acc[a, x, pl.ds(z, chunk)] for a in range(n_ang)
            )
            total = lax.fori_loop(0, n_off // GROUP, lag_group, total)
            for a in range(n_ang):
                if step + 1 < steps:
                    acc[a, x, pl.ds(z, chunk)] = total[a]
                else:
                    out[a, pl.ds(z, chunk), :, x * LANES : (x + 1) * LANES] = total[a].astype(BF16)
            return carry

        lax.fori_loop(0, length // chunk, part, 0)

    injections()
    for x in range(halves):
        copies[("speed", x)].wait()
        copies[("aniso", x)].wait()
        copies[("tilt", x)].wait()
        a1[x] = speed[x] * (1.0 + 2.0 * a1[x])
        a2[x] = speed[x] * a2[x]
        pack(a1[x], a2[x], sendc, x, pl.ds(0, zs))
    coefs = [
        remote(sendc.at[:, half], recvc.at[i], send_semc.at[i], recv_semc.at[i], peer[d])
        for i, (half, d) in enumerate(((HI, 1), (LO, -1)))
    ]
    for copy in coefs:
        copy.start()
    for m in range(2):
        for x in range(halves):
            copies[("before", m, x)].wait()
    local_part(0)
    partial = []
    for x in range(halves):
        along_y(pw.at[0, :, :, inner], x, True)
        finish(0, x, sendp, whole=False)
        partial.append(
            [
                remote(sendp.at[x, half], recvp.at[x, i], send_semp.at[2 * x + i], recv_semp.at[2 * x + i], peer[d])
                for i, (half, d) in enumerate(((HI, 1), (LO, -1)))
            ]
        )
        for copy in partial[x]:
            copy.start()
    for x in range(halves):
        shares(x)
    copies["wt"].wait()
    copies["lags"].wait()
    by_bin = [wt[b].astype(F32) for b in range(n_bin)]
    for a in range(n_ang):
        rows = jnp.concatenate([v[a : a + 1] for v in by_bin], axis=0)
        for h in range(n_off):
            table[h, a] = jnp.broadcast_to(rows[:, h : h + 1], (n_bin, LANES))
    for x in range(halves):
        copies[("bins", x)].wait()

    def direct(send, recv, send_sems, recv_sems, cells):
        for parity, here in enumerate((jnp.logical_not(odd), odd)):

            @pl.when(here)
            def _():
                for i, d in enumerate(DIRECT[parity]):
                    slot = OFFSETS.index(-d)
                    remote(send.at[cells], recv.at[(slot,) + cells], send_sems[i], recv_sems[slot], peer[d]).start()

    def passed(recv, send_sems, recv_sems, cells, index):
        here, there = (OFFSETS.index(d) for d in PASSED[index])
        return remote(recv.at[(here,) + cells], recv.at[(there,) + cells], send_sems[index], recv_sems[there], peer[-1])

    def collect(step, recv, send_sems, recv_sems, cells, x_list, z, length):
        for d in (1, -2, -1, 2):
            slot = OFFSETS.index(d)
            remote(recv.at[(slot,) + cells], recv.at[(slot,) + cells], send_sems[0], recv_sems[slot], peer[1]).wait_recv()
            for index, (source, _) in enumerate(PASSED):
                if source == d:

                    @pl.when(odd)
                    def _():
                        passed(recv, send_sems[3:], recv_sems, cells, index).start()

        for d in OFFSETS:
            for x in x_list:
                open_block(step, d, recv, x, z, length)

    def sent(send, recv, send_sems, recv_sems, cells):
        for i in range(3):
            remote(send.at[cells], recv.at[(0,) + cells], send_sems[i], recv_sems[0], peer[1]).wait_send()

        @pl.when(odd)
        def _():
            for index in range(len(PASSED)):
                passed(recv, send_sems[3:], recv_sems, cells, index).wait_send()

    first_sems = [
        ([in_sem.at[5 * x + i] for i in range(5)], [recv_sem1.at[4 * x + i] for i in range(4)]) for x in range(halves)
    ]

    for x in range(halves):
        for copy in halo[x]:
            copy.wait_recv()
        halo_rows(hw, x, recv0[x, 0].astype(F32), recv0[x, 1].astype(F32))
        along_y(hw, x, False)
        finish(0, x, send1)
        direct(send1, recv1, *first_sems[x], (x,))
    local_part(1)
    for copy in coefs:
        copy.wait_recv()
    length = zs // PIECES
    pieces = [(x, p * length) for x in range(halves) for p in range(PIECES)]
    cells_of = [(x, slice(None), pl.ds(z, length)) for x, z in pieces]
    last_sems = [
        ([in_sem.at[5 * (halves + index) + i] for i in range(5)], [recv_sem2.at[4 * index + i] for i in range(4)])
        for index in range(len(pieces))
    ]
    for x in range(halves):
        for copy in partial[x]:
            copy.wait_recv()
        border_rows(x)
        along_y(pw.at[1, :, :, inner], x, True)
        finish(1, x, send2)
        for index, (x_of, z) in enumerate(pieces):
            if x_of == x:
                direct(send2, recv2, *last_sems[index], cells_of[index])

    for x in range(halves):
        keep_weights(x)
    for x in range(halves):
        collect(0, recv1, *first_sems[x], (x,), (x,), 0, zs)
        image(0, x, 0, zs)
    for index, (x, z) in enumerate(pieces):
        collect(1, recv2, *last_sems[index], cells_of[index], (x,), z, length)
        image(1, x, z, length)

    for copy in coefs + sum([list(c) for c in halo + partial], []):
        copy.wait_send()
    for x in range(halves):
        sent(send1, recv1, *first_sems[x], (x,))
    for index in range(len(pieces)):
        sent(send2, recv2, *last_sems[index], cells_of[index])


def per_device(
    source_now, source_before, receiver_now, receiver_before, speed_term, aniso_field, tilt_field,
    angle_bins, weight_table, offset_lags, source_cells, source_wavelet, receiver_cells, receiver_traces,
):
    zs, rows, width = source_now.shape
    halves = width // LANES
    steps = source_wavelet.shape[0]
    n_off, n_bin, n_ang = weight_table.shape
    n_src = source_cells.shape[0]
    receivers = receiver_cells.shape[0]
    assert rows == ROWS and n_bin == ROWS and width & (width - 1) == 0
    half = (halves, zs, ROWS, LANES)
    block = (halves, 2, zs, ROWS, LANES)
    any_space = pl.BlockSpec(memory_space=pl.ANY)
    dma = pltpu.SemaphoreType.DMA
    in_specs = [any_space] * 14
    return pl.pallas_call(
        kernel,
        out_shape=pltpu.VMEM((n_ang, zs, rows, width), BF16),
        in_specs=in_specs,
        out_specs=pl.BlockSpec(memory_space=pltpu.VMEM),
        scratch_shapes=[
            pltpu.VMEM((steps, 2, halves, zs + 2 * PAD, 3 * ROWS, LANES), F32),
            pltpu.VMEM((2,) + half, F32),
            pltpu.VMEM(half, F32),
            pltpu.VMEM(half, F32),
            pltpu.VMEM(half, F32),
            pltpu.VMEM(half, jnp.int32),
            pltpu.VMEM((n_bin, n_ang, n_off), BF16),
            pltpu.SMEM((n_off,), jnp.int32),
            pltpu.SMEM((n_src,), jnp.int32),
            pltpu.SMEM((steps, n_src), F32),
            pltpu.VMEM((receivers // LANES, LANES), jnp.int32),
            pltpu.VMEM((steps, receivers), F32),
            pltpu.VMEM((n_off, n_ang, n_bin, LANES), F32),
            pltpu.VMEM((n_off, KEPT) + half, F32),
            pltpu.VMEM((steps, 2, halves, ROWS, LANES), F32),
            pltpu.VMEM((2,) + half, F32),
            pltpu.VMEM((2, halves, zs + 2 * PAD, ROWS, LANES), F32),
            pltpu.VMEM((2, halves, zs, 3 * ROWS, LANES), F32),
            pltpu.VMEM((2,) + half, F32),
            pltpu.VMEM((2, halves, zs + 2 * PAD, ROWS, LANES), F32),
            pltpu.VMEM(block, BF16),
            pltpu.VMEM(block, BF16),
            pltpu.VMEM(block, BF16),
            pltpu.VMEM(block, BF16),
            pltpu.VMEM(block, BF16),
            pltpu.VMEM(block, BF16),
            pltpu.VMEM((2,) + half, BF16),
            pltpu.VMEM(block, BF16),
            pltpu.VMEM((4,) + block, BF16),
            pltpu.VMEM((4,) + block, BF16),
            pltpu.VMEM((steps, 2, halves, zs, 5 * ROWS, LANES), F32),
            pltpu.VMEM((n_ang,) + half, F32),
            dma((8 * halves + 6,)),
            dma((2 * halves,)),
            dma((2 * halves,)),
            dma((2,)),
            dma((2,)),
            dma((2 * halves,)),
            dma((2 * halves,)),
            dma((4 * halves,)),
            dma((4 * halves * PIECES,)),
        ],
        compiler_params=pltpu.CompilerParams(collective_id=0, has_side_effects=True),
    )(
        source_now, source_before, receiver_now, receiver_before, speed_term, aniso_field, tilt_field,
        angle_bins, jnp.transpose(weight_table, (1, 2, 0)), offset_lags, source_cells, source_wavelet,
        receiver_cells.reshape(receivers // LANES, LANES), receiver_traces,
    )


def solution(mesh):
    return jax.shard_map(
        per_device,
        mesh=mesh,
        in_specs=(
            P("shot", "gy", None),
            P("shot", "gy", None),
            P("shot", "gy", None),
            P("shot", "gy", None),
            P(None, "gy", None),
            P(None, "gy", None),
            P(None, "gy", None),
            P(None, "gy", None),
            P(),
            P(),
            P("shot"),
            P("shot", None),
            P("shot"),
            P("shot", None),
        ),
        out_specs=P("shot", None, "gy", None),
        check_vma=False,
    )
```

```python
import functools

import jax
import jax.numpy as jnp
from jax import lax
from jax.experimental import pallas as pl
from jax.experimental.pallas import tpu as pltpu
from jax.sharding import PartitionSpec as P

SECOND_COEF = (-205.0 / 72.0, 8.0 / 5.0, -1.0 / 5.0, 8.0 / 315.0, -1.0 / 560.0)
FIRST_COEF = (4.0 / 5.0, -1.0 / 5.0, 4.0 / 105.0, -1.0 / 280.0)
MESH = pl.DeviceIdType.MESH
F32 = jnp.float32
BF16 = jnp.bfloat16
LANES = 128
ROWS = 8
PAD = 4
LO, HI = 0, 1
OFFSETS = (-2, -1, 1, 2)
DIRECT = ((2, -1, 1), (2, -2, -1))
PASSED = ((1, 2), (-2, -1))
GROUP = 8
KEPT = 4
PIECES = 1


def kernel(
    sn_hbm, sb_hbm, rn_hbm, rb_hbm, speed_hbm, aniso_hbm, tilt_hbm, bins_hbm, wt_hbm,
    lags_hbm, scells_hbm, swave_hbm, rcells_hbm, rtraces_hbm,
    out,
    pw, qv, speed, a1, a2, bins, wt, lags, scells, swave, rcells, rtraces, table, cache, inj, base, grad,
    hw, share2, share1, send0, sendc, sendp, send1, send2, recv0, recvc, recvp, recv1, recv2, win, acc,
    in_sem, send_sem0, recv_sem0, send_semc, recv_semc, send_semp, recv_semp, recv_sem1, recv_sem2,
):
    n = lax.axis_size("gy")
    me = lax.axis_index("gy")
    peer = {d: lax.rem(me + (d + n), n) for d in OFFSETS}
    odd = lax.rem(me, 2) == 1
    zs = sn_hbm.shape[0]
    halves = sn_hbm.shape[2] // LANES
    n_bin, n_ang, n_off = wt_hbm.shape
    kept = cache.shape[1]
    steps = swave.shape[0]
    n_src = scells.shape[0]
    rec_rows = rcells_hbm.shape[0]
    own = pl.ds(ROWS, ROWS)
    inner = pl.ds(PAD, zs)

    barrier = pltpu.get_barrier_semaphore()
    for d in OFFSETS:
        pl.semaphore_signal(barrier, inc=1, device_id={"gy": peer[d]}, device_id_type=MESH)

    copies = {}

    def fetch(name, index, src, dst):
        copy = pltpu.make_async_copy(src, dst, in_sem.at[index])
        copy.start()
        copies[name] = copy

    wanted = [
        (("now", m, x), ref.at[:, :, pl.ds(x * LANES, LANES)], pw.at[0, m, x, inner, own, :])
        for x in range(halves)
        for m, ref in enumerate((sn_hbm, rn_hbm))
    ]
    wanted += [("rcells", rcells_hbm, rcells), ("rtraces", rtraces_hbm, rtraces)]
    wanted += [("scells", scells_hbm, scells), ("swave", swave_hbm, swave)]
    for name, ref, dst in (("speed", speed_hbm, speed), ("aniso", aniso_hbm, a1), ("tilt", tilt_hbm, a2)):
        wanted += [((name, x), ref.at[:, :, pl.ds(x * LANES, LANES)], dst.at[x]) for x in range(halves)]
    for m, ref in enumerate((sb_hbm, rb_hbm)):
        wanted += [(("before", m, x), ref.at[:, :, pl.ds(x * LANES, LANES)], qv.at[m, x]) for x in range(halves)]
    wanted += [(("bins", x), bins_hbm.at[:, :, pl.ds(x * LANES, LANES)], bins.at[x]) for x in range(halves)]
    wanted += [("wt", wt_hbm, wt), ("lags", lags_hbm, lags)]
    for index, (name, src, dst) in enumerate(wanted):
        fetch(name, index, src, dst)

    edge = jnp.zeros((PAD, ROWS, LANES), F32)
    plane = jnp.zeros((zs, ROWS, LANES), F32)
    for x in range(halves):
        for m in range(2):
            for s in range(steps):
                pw[s, m, x, pl.ds(0, PAD), own, :] = edge
                pw[s, m, x, pl.ds(PAD + zs, PAD), own, :] = edge
            pw[0, m, x, inner, pl.ds(0, ROWS), :] = plane
            pw[0, m, x, inner, pl.ds(2 * ROWS, ROWS), :] = plane
            hw[m, x, :, own, :] = plane
            for padded in (grad, share1):
                padded[m, x, pl.ds(0, PAD)] = edge
                padded[m, x, pl.ds(PAD + zs, PAD)] = edge

    sub = lax.broadcasted_iota(jnp.int32, (ROWS, LANES), 0)
    lane = lax.broadcasted_iota(jnp.int32, (ROWS, LANES), 1)
    low_rows = sub < PAD

    def turn(v):
        return pltpu.roll(v, PAD, axis=v.ndim - 2)

    def pack(source, receiver, send, x, where_z):
        send[x, LO, where_z] = jnp.where(low_rows, source, turn(receiver)).astype(BF16)
        send[x, HI, where_z] = jnp.where(low_rows, turn(source), receiver).astype(BF16)

    def remote(src, dst, ssem, rsem, device):
        return pltpu.make_async_remote_copy(
            src_ref=src, dst_ref=dst, send_sem=ssem, recv_sem=rsem, device_id={"gy": device}, device_id_type=MESH
        )

    shift_bits = (halves * LANES).bit_length() - 1

    def injections():
        first_row = me * ROWS
        for name in ("rcells", "rtraces", "scells", "swave"):
            copies[name].wait()
        left, right = [], []
        col_iota = lax.broadcasted_iota(jnp.int32, (halves * LANES, LANES), 0)
        for c in range(rec_rows):
            cell = rcells[c : c + 1, :]
            row = lax.shift_right_logical(cell, shift_bits) - first_row
            col = jnp.bitwise_and(cell, halves * LANES - 1)
            hit = jnp.broadcast_to(row, (ROWS, LANES)) == sub
            parts = []
            for s in range(steps):
                amount = jnp.broadcast_to(rtraces[s : s + 1, c * LANES : (c + 1) * LANES], (ROWS, LANES))
                amount = jnp.where(hit, amount, 0.0)
                coarse = amount.astype(BF16).astype(F32)
                parts += [coarse, amount - coarse]
            left.append(jnp.concatenate(parts, axis=0).astype(BF16))
            right.append(jnp.where(jnp.broadcast_to(col, col_iota.shape) == col_iota, 1.0, 0.0).astype(BF16))
        spread = lax.dot_general(
            jnp.concatenate(left, axis=1),
            jnp.concatenate(right, axis=1),
            (((1,), (1,)), ((), ())),
            preferred_element_type=F32,
        )
        for s in range(steps):
            total = spread[2 * s * ROWS : (2 * s + 1) * ROWS] + spread[(2 * s + 1) * ROWS : (2 * s + 2) * ROWS]
            for x in range(halves):
                inj[s, 1, x] = total[:, x * LANES : (x + 1) * LANES]
        for s in range(steps):
            for x in range(halves):
                total = jnp.zeros((ROWS, LANES), F32)
                for i in range(n_src):
                    cell = scells[i]
                    row = lax.shift_right_logical(cell, shift_bits) - first_row
                    col = jnp.bitwise_and(cell, halves * LANES - 1) - x * LANES
                    total = total + jnp.where((sub == row) & (lane == col), swave[s, i], 0.0)
                inj[s, 0, x] = total

    halo = [
        (
            remote(send0.at[x, HI], recv0.at[x, 0], send_sem0.at[2 * x], recv_sem0.at[2 * x], peer[1]),
            remote(send0.at[x, LO], recv0.at[x, 1], send_sem0.at[2 * x + 1], recv_sem0.at[2 * x + 1], peer[-1]),
        )
        for x in range(halves)
    ]
    for x in range(halves):
        for m in range(2):
            copies[("now", m, x)].wait()
        pack(pw[0, 0, x, inner, own, :], pw[0, 1, x, inner, own, :], send0, x, pl.ds(0, zs))
        if x == 0:
            pl.semaphore_wait(barrier, len(OFFSETS))
        for copy in halo[x]:
            copy.start()

    def local_part(step):
        chunk = 4

        def part(i, carry):
            z = i * chunk
            for m in range(2):
                f = [pw[step, m, x, pl.ds(PAD + z, chunk), own, :] for x in range(halves)]
                first = [jnp.zeros_like(v) for v in f]
                second = [SECOND_COEF[0] * v for v in f]
                for k in range(1, PAD + 1):
                    up = [pltpu.roll(v, LANES - k, axis=2) for v in f] + [jnp.zeros_like(f[0])]
                    down = [jnp.zeros_like(f[0])] + [pltpu.roll(v, k, axis=2) for v in f]
                    for x in range(halves):
                        above = jnp.where(lane < LANES - k, up[x], up[x + 1])
                        below = jnp.where(lane >= k, down[x + 1], down[x])
                        second[x] = second[x] + SECOND_COEF[k] * (above + below)
                        first[x] = first[x] + FIRST_COEF[k - 1] * (above - below)
                for x in range(halves):
                    grad[m, x, pl.ds(PAD + z, chunk)] = first[x]
                    along_z = SECOND_COEF[0] * f[x]
                    for k in range(1, PAD + 1):
                        along_z = along_z + SECOND_COEF[k] * (
                            pw[step, m, x, pl.ds(PAD + z + k, chunk), own, :]
                            + pw[step, m, x, pl.ds(PAD + z - k, chunk), own, :]
                        )
                    before = qv[m, x, pl.ds(z, chunk)] if step == 0 else pw[step - 1, m, x, pl.ds(PAD + z, chunk), own, :]
                    base[m, x, pl.ds(z, chunk)] = (
                        2.0 * f[x]
                        - before
                        + a1[x, pl.ds(z, chunk)] * second[x]
                        + speed[x, pl.ds(z, chunk)] * along_z
                    )
            return carry

        lax.fori_loop(0, zs // chunk, part, 0)
        for m in range(2):
            for x in range(halves):
                base[m, x, 0] = base[m, x, 0] + inj[step, m, x]

    def halo_rows(window, x, low, high):
        window[0, x, :, pl.ds(0, ROWS), :] = turn(low)
        window[1, x, :, pl.ds(0, ROWS), :] = low
        window[0, x, :, pl.ds(2 * ROWS, ROWS), :] = high
        window[1, x, :, pl.ds(2 * ROWS, ROWS), :] = turn(high)

    part_chunk = 4

    def along_y(window, x, whole):
        def part(i, carry):
            z = i * part_chunk
            cells = pl.ds(z, part_chunk)
            for m in range(2):

                def rows(k):
                    return window[m, x, cells, pl.ds(ROWS + k, ROWS), :]

                second, first = 0.0, 0.0
                if whole:
                    second, first = SECOND_COEF[0] * rows(0), grad[m, x, pl.ds(PAD + z, part_chunk)]
                for k in range(1, PAD + 1):
                    above, below = rows(k), rows(-k)
                    second = second + SECOND_COEF[k] * (above + below)
                    first = first + FIRST_COEF[k - 1] * (above - below)
                grad[m, x, pl.ds(PAD + z, part_chunk)] = first
                base[m, x, cells] = base[m, x, cells] + a1[x, cells] * second
            return carry

        lax.fori_loop(0, zs // part_chunk, part, 0)

    def along_z(padded, member, x, z):
        mixed = jnp.zeros((part_chunk, ROWS, LANES), F32)
        for k in range(1, PAD + 1):
            mixed = mixed + FIRST_COEF[k - 1] * (
                padded[member, x, pl.ds(PAD + z + k, part_chunk)] - padded[member, x, pl.ds(PAD + z - k, part_chunk)]
            )
        return mixed

    def finish(step, x, send, whole=True):
        def part(i, carry):
            z = i * part_chunk
            cells = pl.ds(z, part_chunk)
            new = []
            for m in range(2):
                value = base[m, x, cells] + a2[x, cells] * along_z(grad, m, x, z)
                new.append(value)
                if not whole:
                    base[m, x, cells] = value
                    continue
                if step + 1 < steps:
                    pw[step + 1, m, x, pl.ds(PAD + z, part_chunk), own, :] = value
                win[step, m, x, cells, pl.ds(2 * ROWS, ROWS), :] = value.astype(BF16).astype(F32)
            pack(new[0], new[1], send, x, cells)
            return carry

        lax.fori_loop(0, zs // part_chunk, part, 0)

    def shares(x):
        def part(i, carry):
            z = i * part_chunk
            for side in range(2):
                second, first = [], []
                for m in range(2):
                    two, one = 0.0, 0.0
                    for k in range(1, PAD + 1):
                        row = ROWS - PAD + k if side == 0 else 2 * ROWS - k
                        value = pw[0, m, x, pl.ds(PAD + z, part_chunk), pl.ds(row, ROWS), :]
                        two = two + SECOND_COEF[k] * value
                        one = one + (FIRST_COEF[k - 1] if side == 0 else -FIRST_COEF[k - 1]) * value
                    second.append(two)
                    first.append(one)
                share2[side, x, pl.ds(z, part_chunk)] = jnp.where(low_rows, second[0], turn(second[1]))
                share1[side, x, pl.ds(PAD + z, part_chunk)] = jnp.where(low_rows, first[0], turn(first[1]))
            return carry

        lax.fori_loop(0, zs // part_chunk, part, 0)

    def border_rows(x):
        whole = []
        for side in range(2):
            blocks = []
            for z in range(0, zs, part_chunk):
                cells = pl.ds(z, part_chunk)
                pair = recvc[side, x, cells].astype(F32)
                flat, tilted = jnp.where(low_rows, pair, turn(pair)), jnp.where(low_rows, turn(pair), pair)
                blocks.append(
                    recvp[x, side, cells].astype(F32)
                    + flat * share2[side, x, cells]
                    + tilted * along_z(share1, side, x, z)
                )
            whole.append(jnp.concatenate(blocks, axis=0))
        halo_rows(pw.at[1, :, :, inner], x, whole[0], whole[1])

    def open_block(step, d, recv, x, z, length):
        cells = pl.ds(z, length)
        rows = pl.ds((2 + d) * ROWS, ROWS)
        slot = OFFSETS.index(d)
        low = recv[slot, x, LO, cells].astype(F32)
        high = recv[slot, x, HI, cells].astype(F32)
        win[step, 0, x, cells, rows, :] = jnp.where(low_rows, low, turn(high))
        win[step, 1, x, cells, rows, :] = jnp.where(low_rows, turn(low), high)

    chunk = 4

    def gathered(h, a, bin_ids):
        row = table[h, a]
        return jnp.stack([jnp.take_along_axis(row, ids, axis=0) for ids in bin_ids])

    def keep_weights(x):
        def part(i, carry):
            z = i * chunk
            bin_ids = [bins[x, z + j] for j in range(chunk)]
            for h in range(n_off):
                for a in range(kept):
                    cache[h, a, x, pl.ds(z, chunk)] = gathered(h, a, bin_ids)
            return carry

        lax.fori_loop(0, zs // chunk, part, 0)

    def image(step, x, start, length):
        def part(i, carry):
            z = start + i * chunk
            bin_ids = [bins[x, z + j] for j in range(chunk)]
            def lag_group(g, total):
                total = list(total)
                for j in range(GROUP):
                    h = g * GROUP + j
                    lag = lags[h]
                    product = (
                        win[step, 0, x, pl.ds(z, chunk), pl.ds(2 * ROWS - lag, ROWS), :]
                        * win[step, 1, x, pl.ds(z, chunk), pl.ds(2 * ROWS + lag, ROWS), :]
                    )
                    for a in range(n_ang):
                        weight = cache[h, a, x, pl.ds(z, chunk)] if a < kept else gathered(h, a, bin_ids)
                        total[a] = total[a] + weight * product
                return tuple(total)

            total = tuple(
                jnp.zeros((chunk, ROWS, LANES), F32) if step == 0 else acc[a, x, pl.ds(z, chunk)] for a in range(n_ang)
            )
            total = lax.fori_loop(0, n_off // GROUP, lag_group, total)
            for a in range(n_ang):
                if step + 1 < steps:
                    acc[a, x, pl.ds(z, chunk)] = total[a]
                else:
                    out[a, pl.ds(z, chunk), :, x * LANES : (x + 1) * LANES] = total[a].astype(BF16)
            return carry

        lax.fori_loop(0, length // chunk, part, 0)

    injections()
    for x in range(halves):
        copies[("speed", x)].wait()
        copies[("aniso", x)].wait()
        copies[("tilt", x)].wait()
        a1[x] = speed[x] * (1.0 + 2.0 * a1[x])
        a2[x] = speed[x] * a2[x]
        pack(a1[x], a2[x], sendc, x, pl.ds(0, zs))
    coefs = [
        remote(sendc.at[:, half], recvc.at[i], send_semc.at[i], recv_semc.at[i], peer[d])
        for i, (half, d) in enumerate(((HI, 1), (LO, -1)))
    ]
    for copy in coefs:
        copy.start()
    for m in range(2):
        for x in range(halves):
            copies[("before", m, x)].wait()
    local_part(0)
    partial = []
    for x in range(halves):
        along_y(pw.at[0, :, :, inner], x, True)
        finish(0, x, sendp, whole=False)
        partial.append(
            [
                remote(sendp.at[x, half], recvp.at[x, i], send_semp.at[2 * x + i], recv_semp.at[2 * x + i], peer[d])
                for i, (half, d) in enumerate(((HI, 1), (LO, -1)))
            ]
        )
        for copy in partial[x]:
            copy.start()
    copies["wt"].wait()
    copies["lags"].wait()
    for x in range(halves):
        copies[("bins", x)].wait()

    def direct(send, recv, send_sems, recv_sems, cells):
        for parity, here in enumerate((jnp.logical_not(odd), odd)):

            @pl.when(here)
            def _():
                for i, d in enumerate(DIRECT[parity]):
                    slot = OFFSETS.index(-d)
                    remote(send.at[cells], recv.at[(slot,) + cells], send_sems[i], recv_sems[slot], peer[d]).start()

    def passed(recv, send_sems, recv_sems, cells, index):
        here, there = (OFFSETS.index(d) for d in PASSED[index])
        return remote(recv.at[(here,) + cells], recv.at[(there,) + cells], send_sems[index], recv_sems[there], peer[-1])

    def collect(step, recv, send_sems, recv_sems, cells, x_list, z, length):
        for d in (1, -2, -1, 2):
            slot = OFFSETS.index(d)
            remote(recv.at[(slot,) + cells], recv.at[(slot,) + cells], send_sems[0], recv_sems[slot], peer[1]).wait_recv()
            for index, (source, _) in enumerate(PASSED):
                if source == d:

                    @pl.when(odd)
                    def _():
                        passed(recv, send_sems[3:], recv_sems, cells, index).start()

        for d in OFFSETS:
            for x in x_list:
                open_block(step, d, recv, x, z, length)

    def sent(send, recv, send_sems, recv_sems, cells):
        for i in range(3):
            remote(send.at[cells], recv.at[(0,) + cells], send_sems[i], recv_sems[0], peer[1]).wait_send()

        @pl.when(odd)
        def _():
            for index in range(len(PASSED)):
                passed(recv, send_sems[3:], recv_sems, cells, index).wait_send()

    first_sems = [
        ([in_sem.at[5 * x + i] for i in range(5)], [recv_sem1.at[4 * x + i] for i in range(4)]) for x in range(halves)
    ]

    for x in range(halves):
        for copy in halo[x]:
            copy.wait_recv()
        halo_rows(hw, x, recv0[x, 0].astype(F32), recv0[x, 1].astype(F32))
        along_y(hw, x, False)
        finish(0, x, send1)
        direct(send1, recv1, *first_sems[x], (x,))
    for x in range(halves):
        shares(x)
    local_part(1)
    for copy in coefs:
        copy.wait_recv()
    length = zs // PIECES
    pieces = [(x, p * length) for x in range(halves) for p in range(PIECES)]
    cells_of = [(x, slice(None), pl.ds(z, length)) for x, z in pieces]
    last_sems = [
        ([in_sem.at[5 * (halves + index) + i] for i in range(5)], [recv_sem2.at[4 * index + i] for i in range(4)])
        for index in range(len(pieces))
    ]
    for x in range(halves):
        for copy in partial[x]:
            copy.wait_recv()
        border_rows(x)
        along_y(pw.at[1, :, :, inner], x, True)
        finish(1, x, send2)
        for index, (x_of, z) in enumerate(pieces):
            if x_of == x:
                direct(send2, recv2, *last_sems[index], cells_of[index])

    by_bin = [wt[b].astype(F32) for b in range(n_bin)]
    for a in range(n_ang):
        rows = jnp.concatenate([v[a : a + 1] for v in by_bin], axis=0)
        for h in range(n_off):
            table[h, a] = jnp.broadcast_to(rows[:, h : h + 1], (n_bin, LANES))
    for x in range(halves):
        keep_weights(x)
    for x in range(halves):
        collect(0, recv1, *first_sems[x], (x,), (x,), 0, zs)
        image(0, x, 0, zs)
    for index, (x, z) in enumerate(pieces):
        collect(1, recv2, *last_sems[index], cells_of[index], (x,), z, length)
        image(1, x, z, length)

    for copy in coefs + sum([list(c) for c in halo + partial], []):
        copy.wait_send()
    for x in range(halves):
        sent(send1, recv1, *first_sems[x], (x,))
    for index in range(len(pieces)):
        sent(send2, recv2, *last_sems[index], cells_of[index])


def per_device(
    source_now, source_before, receiver_now, receiver_before, speed_term, aniso_field, tilt_field,
    angle_bins, weight_table, offset_lags, source_cells, source_wavelet, receiver_cells, receiver_traces,
):
    zs, rows, width = source_now.shape
    halves = width // LANES
    steps = source_wavelet.shape[0]
    n_off, n_bin, n_ang = weight_table.shape
    n_src = source_cells.shape[0]
    receivers = receiver_cells.shape[0]
    assert rows == ROWS and n_bin == ROWS and width & (width - 1) == 0
    half = (halves, zs, ROWS, LANES)
    block = (halves, 2, zs, ROWS, LANES)
    any_space = pl.BlockSpec(memory_space=pl.ANY)
    dma = pltpu.SemaphoreType.DMA
    in_specs = [any_space] * 14
    return pl.pallas_call(
        kernel,
        out_shape=pltpu.VMEM((n_ang, zs, rows, width), BF16),
        in_specs=in_specs,
        out_specs=pl.BlockSpec(memory_space=pltpu.VMEM),
        scratch_shapes=[
            pltpu.VMEM((steps, 2, halves, zs + 2 * PAD, 3 * ROWS, LANES), F32),
            pltpu.VMEM((2,) + half, F32),
            pltpu.VMEM(half, F32),
            pltpu.VMEM(half, F32),
            pltpu.VMEM(half, F32),
            pltpu.VMEM(half, jnp.int32),
            pltpu.VMEM((n_bin, n_ang, n_off), BF16),
            pltpu.SMEM((n_off,), jnp.int32),
            pltpu.SMEM((n_src,), jnp.int32),
            pltpu.SMEM((steps, n_src), F32),
            pltpu.VMEM((receivers // LANES, LANES), jnp.int32),
            pltpu.VMEM((steps, receivers), F32),
            pltpu.VMEM((n_off, n_ang, n_bin, LANES), F32),
            pltpu.VMEM((n_off, KEPT) + half, F32),
            pltpu.VMEM((steps, 2, halves, ROWS, LANES), F32),
            pltpu.VMEM((2,) + half, F32),
            pltpu.VMEM((2, halves, zs + 2 * PAD, ROWS, LANES), F32),
            pltpu.VMEM((2, halves, zs, 3 * ROWS, LANES), F32),
            pltpu.VMEM((2,) + half, F32),
            pltpu.VMEM((2, halves, zs + 2 * PAD, ROWS, LANES), F32),
            pltpu.VMEM(block, BF16),
            pltpu.VMEM(block, BF16),
            pltpu.VMEM(block, BF16),
            pltpu.VMEM(block, BF16),
            pltpu.VMEM(block, BF16),
            pltpu.VMEM(block, BF16),
            pltpu.VMEM((2,) + half, BF16),
            pltpu.VMEM(block, BF16),
            pltpu.VMEM((4,) + block, BF16),
            pltpu.VMEM((4,) + block, BF16),
            pltpu.VMEM((steps, 2, halves, zs, 5 * ROWS, LANES), F32),
            pltpu.VMEM((n_ang,) + half, F32),
            dma((8 * halves + 6,)),
            dma((2 * halves,)),
            dma((2 * halves,)),
            dma((2,)),
            dma((2,)),
            dma((2 * halves,)),
            dma((2 * halves,)),
            dma((4 * halves,)),
            dma((4 * halves * PIECES,)),
        ],
        compiler_params=pltpu.CompilerParams(collective_id=0, has_side_effects=True),
    )(
        source_now, source_before, receiver_now, receiver_before, speed_term, aniso_field, tilt_field,
        angle_bins, jnp.transpose(weight_table, (1, 2, 0)), offset_lags, source_cells, source_wavelet,
        receiver_cells.reshape(receivers // LANES, LANES), receiver_traces,
    )


def solution(mesh):
    return jax.shard_map(
        per_device,
        mesh=mesh,
        in_specs=(
            P("shot", "gy", None),
            P("shot", "gy", None),
            P("shot", "gy", None),
            P("shot", "gy", None),
            P(None, "gy", None),
            P(None, "gy", None),
            P(None, "gy", None),
            P(None, "gy", None),
            P(),
            P(),
            P("shot"),
            P("shot", None),
            P("shot"),
            P("shot", None),
        ),
        out_specs=P("shot", None, "gy", None),
        check_vma=False,
    )
```
